32 devices in a mesh: gx: 8 (over z, y), gy: 4 (over x, core).
Axes of the slice: x: 2, y: 2, z: 4, core: 2. Of those that a mesh axis runs over, the one named last changes fastest.
Arguments:
- positions: float32 [3, 16, 8, 256], P(None, 'gx', 'gy'), may hold values from 0 to 16, as said below
- velocities: float32 [3, 16, 8, 256], P(None, 'gx', 'gy'), may hold values from -3 to 3
- occupancy: int32 [16, 8], P('gx', 'gy'), may hold values from 64 to 256
- cot_positions: float32 [3, 16, 8, 256], P(None, 'gx', 'gy'), may hold values from -6 to 6
- cot_velocities: float32 [3, 16, 8, 256], P(None, 'gx', 'gy'), may hold values from -6 to 6
Outputs:
- grad_positions: float32 [3, 16, 8, 256], P(None, 'gx', 'gy')
- grad_velocities: float32 [3, 16, 8, 256], P(None, 'gx', 'gy')
The draws below stay inside these ranges and needn't reach their ends.
Inputs may be any that keep to these rules, and one draw needn't show every extreme that they name: `positions`: components 0 and 1 lie in [0, 1), the offset in the tile's cell; component 2 lies in [0, 16). Slots 0 to occupancy - 1 of a tile hold particles, the other slots are empty.
All inputs are finite; a program needn't handle non-finite values.
Results may differ from the reference program's by a relative error of at most 0.0003.
Values sent between devices are 32-bit elements; how exact they have to be, the bound alone decides.
No kernel may reach another device: no remote copies, remote signals or barrier semaphores. Data moves between devices by JAX's collectives and lax.ppermute only.
A program may use at most 128 MiB of HBM per device.

```python
import jax
import jax.numpy as jnp
from jax import lax

P_SIZE = 256
ZH = 16
TX = 2
STEPS = 4
TXG = 16
TYG = 8


def draw_positions(key, part):
    uniform_draw = jax.random.uniform(key, (3, TXG, TYG, P_SIZE), jnp.float32)
    scales = jnp.array([1.0, 1.0, float(ZH)], jnp.float32)[:, None, None, None]
    return uniform_draw * scales


def with_ends(values, stream_key, low, top_value):
    extent = values.shape
    spot = [jax.random.randint(jax.random.fold_in(stream_key, axis), (), 0, extent[axis]) for axis in range(len(extent))]
    values = values.at[tuple(spot)].set(low)
    longest = extent.index(max(extent))
    spot[longest] = (spot[longest] + 1) % extent[longest]
    return values.at[tuple(spot)].set(top_value)


def level_of(rng, dims, cuts, smallest, top_value):
    level = 1.0
    for axis_at, blocks in cuts:
        heights = jax.random.uniform(jax.random.fold_in(jax.random.fold_in(rng, 6), axis_at), (blocks,), jnp.float32, smallest / len(cuts), top_value / len(cuts))
        level = level * jnp.repeat(jnp.exp(heights), dims[axis_at] // blocks).reshape((-1,) + (1,) * (len(dims) - 1 - axis_at))
    return level


def gaussian(stream_key, dims, spread, bound, split=(), kind=jnp.bfloat16):
    drawn = spread * jax.random.normal(stream_key, dims, jnp.float32)
    if split:
        drawn = drawn * level_of(stream_key, dims, split, -0.22, 0.18)
    return jnp.clip(drawn, -bound, bound).astype(kind)


def setup_inputs(seed: int = 0) -> dict:
    key_of = jax.random.split(jax.random.key(seed), 6)
    return {
        "positions": draw_positions(jax.random.fold_in(key_of[5], 71), 0),
        "velocities": gaussian(key_of[1], (3, TXG, TYG, P_SIZE), 0.5, 3.0, ((1, 8), (2, 4)), jnp.float32),
        "occupancy": with_ends(jax.random.randint(key_of[2], (TXG, TYG), P_SIZE // 4, P_SIZE + 1), jax.random.fold_in(key_of[2], 1), P_SIZE // 4, P_SIZE).astype(jnp.int32),
        "cot_positions": gaussian(key_of[3], (3, TXG, TYG, P_SIZE), 1.0, 6.0, ((1, 8), (2, 4)), jnp.float32),
        "cot_velocities": gaussian(key_of[4], (3, TXG, TYG, P_SIZE), 1.0, 6.0, ((1, 8), (2, 4)), jnp.float32),
    }


time_step = 0.05
stiffness = 4.0
rest_density = 1.0
particle_mass = 0.15
viscosity = 0.5
stencil = ((-1, -1), (-1, 0), (-1, 1), (0, -1), (0, 0), (0, 1), (1, -1), (1, 0), (1, 1))

def separation(middle_tile, nearby, displace_x, displace_y):
    offsets = (float(displace_x), float(displace_y), 0.0)
    return [nearby[coord_id][..., None, :] - middle_tile[coord_id][..., :, None] + offsets[coord_id] for coord_id in range(3)]

def intersection_of(pieces):
    return jnp.maximum(1.0 - (pieces[0] * pieces[0] + pieces[1] * pieces[1] + pieces[2] * pieces[2]), 0.0)

def pairwise_density(middle_tile, nearby, displace_x, displace_y):
    intersection = intersection_of(separation(middle_tile, nearby, displace_x, displace_y))
    masses = particle_mass * nearby[3][..., None, :]
    return lax.optimization_barrier(jnp.sum(masses * intersection * intersection * intersection, axis=-1))[None]

def accel_pairs(middle_tile, nearby, displace_x, displace_y):
    pieces = separation(middle_tile, nearby, displace_x, displace_y)
    intersection = intersection_of(pieces)
    masses = particle_mass * nearby[6][..., None, :]
    pressure_push = 6.0 * masses * (middle_tile[6][..., :, None] + nearby[7][..., None, :]) * intersection * intersection
    viscous = viscosity * masses * nearby[8][..., None, :] * intersection * intersection * intersection
    components = [lax.optimization_barrier(jnp.sum(viscous * (nearby[3 + coord_id][..., None, :] - middle_tile[3 + coord_id][..., :, None]) - pressure_push * pieces[coord_id], axis=-1)) for coord_id in range(3)]
    return jnp.stack(components)

def adjacent_tiles(field, displace_x, displace_y):
    rolled = jnp.roll(field, -displace_x, axis=1)
    if displace_y == 1:
        rolled = jnp.concatenate([rolled[:, :, 1:], jnp.zeros_like(rolled[:, :, :1])], axis=2)
    if displace_y == -1:
        rolled = jnp.concatenate([jnp.zeros_like(rolled[:, :, :1]), rolled[:, :, :-1]], axis=2)
    return rolled

def grouped_by_block(pair_fn, middle_tile, nearby, displace_x, displace_y):
    nblocks = middle_tile.shape[1] // TX

    def to_blocks(field):
        return jnp.moveaxis(field.reshape(field.shape[0], nblocks, TX, field.shape[2], field.shape[3]), 1, 0)
    checked = jax.checkpoint(pair_fn, static_argnums=(2, 3))

    def block_pairs(block_args):
        return checked(block_args[0], block_args[1], displace_x, displace_y)
    result = lax.map(block_pairs, (to_blocks(middle_tile), to_blocks(nearby)))
    result = jnp.moveaxis(result, 0, 1)
    return result.reshape(result.shape[0], middle_tile.shape[1], middle_tile.shape[2], middle_tile.shape[3])

def advance(current, active_mask):
    positions = current[:3]
    payload_holder = jnp.concatenate([positions, active_mask], axis=0)
    local_density = jnp.zeros_like(active_mask)
    for displace_x, displace_y in stencil:
        local_density = local_density + grouped_by_block(pairwise_density, positions, adjacent_tiles(payload_holder, displace_x, displace_y), displace_x, displace_y)
    padded = local_density + (1.0 - active_mask)
    coefficient = stiffness * (local_density / rest_density - 1.0) / (padded * padded)
    inverse = 1.0 / padded
    middle_tile = jnp.concatenate([current, coefficient], axis=0)
    source = jnp.concatenate([current, active_mask, coefficient, inverse], axis=0)
    particle_acceleration = jnp.zeros_like(positions)
    for displace_x, displace_y in stencil:
        particle_acceleration = particle_acceleration + grouped_by_block(accel_pairs, middle_tile, adjacent_tiles(source, displace_x, displace_y), displace_x, displace_y)
    velocity = current[3:] + time_step * active_mask * particle_acceleration
    return jnp.concatenate([positions + time_step * velocity, velocity], axis=0)

def reference(positions, velocities, occupancy, cot_positions, cot_velocities):
    slot_ids = jnp.arange(P_SIZE, dtype=jnp.int32)
    active_mask = (slot_ids[None, None, :] < occupancy[:, :, None]).astype(jnp.float32)[None]
    stepper = jax.checkpoint(advance)

    def evolve(start_pos, start_vel):
        current = jnp.concatenate([start_pos, start_vel], axis=0)
        for step_id in range(STEPS):
            current = stepper(current, active_mask)
        return (current[:3], current[3:])
    outputs, pullback = jax.vjp(evolve, positions, velocities)
    grad_positions, grad_velocities = pullback((cot_positions, cot_velocities))
    return (grad_positions, grad_velocities)
```

```python
import functools

import jax
import jax.numpy as jnp
from jax import lax
from jax.experimental import pallas as pl
from jax.experimental.pallas import tpu as pltpu
from jax.sharding import PartitionSpec as P

STEPS = 4
time_step = 0.05
stiffness = 4.0
rest_density = 1.0
particle_mass = 0.15
viscosity = 0.5


FAR = 1.0e4
WALL = 1.0e5
ROWS = 16
LANES = 128
FEATS = 8


def ring_order(count):
    evens = list(range(0, count, 2))
    odds = list(range(1, count, 2))
    return evens + odds[::-1]


class Exchange:
    def __init__(self, mesh):
        self.count_x = mesh.shape["gx"]
        self.count_y = mesh.shape["gy"]
        self.order = ring_order(self.count_x)

    def permute(self, value, pairs):
        return lax.ppermute(value, ("gx", "gy"), pairs)

    def from_x(self, value, step):
        order, count = self.order, self.count_x
        pairs = [
            (order[(slot + step) % count] * self.count_y + b, order[slot] * self.count_y + b)
            for slot in range(count)
            for b in range(self.count_y)
        ]
        return self.permute(value, pairs)

    def from_y(self, value, step):
        pairs = [
            (a * self.count_y + (b + step) % self.count_y, a * self.count_y + b)
            for a in range(self.count_x)
            for b in range(self.count_y)
        ]
        return self.permute(value, pairs)

    def place(self, value):
        pairs = [
            (a * self.count_y + b, self.order[a] * self.count_y + b)
            for a in range(self.count_x)
            for b in range(self.count_y)
        ]
        return self.permute(value, pairs)

    def unplace(self, value):
        pairs = [
            (self.order[a] * self.count_y + b, a * self.count_y + b)
            for a in range(self.count_x)
            for b in range(self.count_y)
        ]
        return self.permute(value, pairs)

    def halo(self, own):
        x_low = self.from_x(own[1:2], -1)
        x_high = self.from_x(own[0:1], 1)
        upper = jnp.concatenate([x_low[:, 1:2], own[:, 1:2], x_high[:, 1:2]], axis=0)
        lower = jnp.concatenate([x_low[:, 0:1], own[:, 0:1], x_high[:, 0:1]], axis=0)
        y_low = self.from_y(upper, -1)
        y_high = self.from_y(lower, 1)
        return (own, x_low, x_high, y_low, y_high)


def region_tile(pieces, rx, ry):
    own, x_low, x_high, y_low, y_high = pieces
    if ry == 0:
        return y_low[rx, 0]
    if ry == 3:
        return y_high[rx, 0]
    if rx == 0:
        return x_low[0, ry - 1]
    if rx == 3:
        return x_high[0, ry - 1]
    return own[rx - 1, ry - 1]


def fill_region(region, pieces, wall_ref=None):
    row = lax.broadcasted_iota(jnp.int32, (FEATS, 2 * LANES), 0)
    for rx in range(4):
        for ry in range(4):
            block = region_tile(pieces, rx, ry)
            if wall_ref is not None:
                if rx in (0, 3):
                    block = jnp.where(row == 0, block + (-2.0 if rx == 0 else 2.0), block)
                if ry in (0, 3):
                    block = jnp.where(row == 1, block + wall_ref[0 if ry == 0 else 1], block)
            region[rx * 4 + ry, 0] = block[:, :LANES]
            region[rx * 4 + ry, 1] = block[:, LANES:]


def own_columns(columns, base, blocks):
    rows = 0
    for block in blocks:
        for t in range(4):
            tx, ty = t // 2, t % 2
            value = block[tx, ty]
            padded = jnp.concatenate(
                [value, jnp.zeros((LANES - FEATS, 2 * LANES), jnp.float32)], axis=0
            )
            columns[base + rows, t] = padded.T
        rows += 1


def pair_sums(n_ref, columns, sums_ref, outputs, body):
    lane = lax.broadcasted_iota(jnp.int32, (ROWS, LANES), 1)

    def tile_loop(t, carry):
        tx = t // 2
        ty = t - 2 * tx
        groups = (n_ref[t] + (ROWS - 1)) // ROWS

        def group_loop(g, carry):
            start = pl.multiple_of(g * ROWS, ROWS)

            def column(kind, feature):
                picked = columns[kind, t, pl.ds(start, ROWS), feature : feature + 1]
                return jnp.broadcast_to(picked, (ROWS, LANES))

            terms_of = body(column)

            def row_loop(dx, totals):
                totals = list(totals)
                for dy in range(3):
                    other = (tx + dx) * 4 + ty + dy
                    for lb in range(2):
                        terms = terms_of(other, lb)
                        totals = [a + b for a, b in zip(totals, terms)]
                return tuple(totals)

            zero = jnp.zeros((ROWS, LANES), jnp.float32)
            totals = lax.fori_loop(0, 3, row_loop, (zero,) * outputs)
            packed = zero
            for index, total in enumerate(totals):
                packed = jnp.where(lane == index, jnp.sum(total, axis=1, keepdims=True), packed)
            sums_ref[t, pl.ds(start, ROWS), :] = packed
            return carry

        return lax.fori_loop(0, groups, group_loop, carry)

    sums_ref[...] = jnp.zeros_like(sums_ref)
    lax.fori_loop(0, 4, tile_loop, 0)


def row_sums(sums_ref, t):
    return sums_ref[t].T


def separation(xi, region, other, lb):
    d = [region[other, lb, f : f + 1, :] - xi[f] for f in range(3)]
    q = jnp.maximum(1.0 - d[0] * d[0] - d[1] * d[1] - d[2] * d[2], 0.0)
    return d, q


def stack_rows(rows):
    width = rows[0].shape[1]
    rows = list(rows) + [jnp.zeros((1, width), jnp.float32)] * (FEATS - len(rows))
    return jnp.concatenate(rows, axis=0)


def density_kernel(n_ref, wall_ref, *refs):
    pieces, (out, region, columns, sums) = refs[:5], refs[5:]
    fill_region(region, pieces, wall_ref)
    own_columns(columns, 0, (pieces[0],))

    def body(column):
        xi = [column(0, f) for f in range(3)]

        def terms(other, lb):
            d, q = separation(xi, region, other, lb)
            return [q * q * q]

        return terms

    pair_sums(n_ref, columns, sums, 1, body)
    for t in range(4):
        live = pieces[0][t // 2, t % 2][6:7] > 0.5
        density = particle_mass * row_sums(sums, t)[0:1]
        padded = jnp.where(live, density, 1.0)
        inverse = jnp.where(live, 1.0 / padded, 0.0)
        coefficient = jnp.where(
            live, stiffness * (density / rest_density - 1.0) / (padded * padded), 0.0
        )
        out[t // 2, t % 2] = stack_rows([coefficient, inverse])


def accel_kernel(n_ref, wall_ref, *refs):
    state, press, (out, region, region_p, columns, sums) = refs[:5], refs[5:10], refs[10:]
    fill_region(region, state, wall_ref)
    fill_region(region_p, press)
    own_columns(columns, 0, (state[0], press[0]))

    def body(column):
        xi = [column(0, f) for f in range(3)]
        ci = column(1, 0)

        def terms(other, lb):
            d, q = separation(xi, region, other, lb)
            q2 = q * q
            visc = q2 * q * region_p[other, lb, 1:2, :]
            push = (ci + region_p[other, lb, 0:1, :]) * q2
            moved = [visc * region[other, lb, 3 + f : 4 + f, :] for f in range(3)]
            pushed = [push * d[f] for f in range(3)]
            return moved + [visc] + pushed

        return terms

    pair_sums(n_ref, columns, sums, 7, body)
    for t in range(4):
        own = state[0][t // 2, t % 2]
        live = own[6:7] > 0.5
        s = row_sums(sums, t)
        new_pos, new_vel = [], []
        for f in range(3):
            vel = own[3 + f : 4 + f]
            accel = particle_mass * (
                viscosity * (s[f : f + 1] - vel * s[3:4]) - 6.0 * s[4 + f : 5 + f]
            )
            vel = jnp.where(live, vel + time_step * accel, vel)
            new_vel.append(vel)
            new_pos.append(
                jnp.where(live, own[f : f + 1] + time_step * vel, own[f : f + 1])
            )
        out[t // 2, t % 2] = stack_rows(new_pos + new_vel + [own[6:7]])


def density_grad_kernel(n_ref, wall_ref, *refs):
    state, lam, press, (out, region, region_l, columns, sums) = (
        refs[:5],
        refs[5:10],
        refs[10],
        refs[11:],
    )
    fill_region(region, state, wall_ref)
    fill_region(region_l, lam)
    own_columns(columns, 0, (state[0], lam[0]))

    def body(column):
        xi = [column(0, f) for f in range(3)]
        vi = [column(0, 3 + f) for f in range(3)]
        li = [column(1, f) for f in range(3)]

        def terms(other, lb):
            d, q = separation(xi, region, other, lb)
            lj = [region_l[other, lb, f : f + 1, :] for f in range(3)]
            q2 = q * q
            along = sum((li[f] - lj[f]) * d[f] for f in range(3))
            moved = sum(lj[f] * (vi[f] - region[other, lb, 3 + f : 4 + f, :]) for f in range(3))
            return [q2 * along, q2 * q * moved]

        return terms

    pair_sums(n_ref, columns, sums, 2, body)
    for t in range(4):
        live = state[0][t // 2, t % 2][6:7] > 0.5
        s = row_sums(sums, t)
        c = press[t // 2, t % 2][0:1]
        w = press[t // 2, t % 2][1:2]
        grad_c = (-6.0 * particle_mass) * s[0:1]
        grad_w = (viscosity * particle_mass) * s[1:2]
        grad = grad_c * (stiffness * w * w - 2.0 * c * w) - grad_w * w * w
        out[t // 2, t % 2] = stack_rows([jnp.where(live, grad, 0.0)])


def main_grad_kernel(n_ref, wall_ref, *refs):
    state, press, lam = refs[:5], refs[5:10], refs[10:15]
    out, region, region_p, region_l, columns, sums = refs[15:]
    fill_region(region, state, wall_ref)
    fill_region(region_p, press)
    fill_region(region_l, lam)
    own_columns(columns, 0, (state[0], press[0], lam[0]))

    def body(column):
        xi = [column(0, f) for f in range(3)]
        vi = [column(0, 3 + f) for f in range(3)]
        ci = column(1, 0)
        wi = column(1, 1)
        li = [column(2, f) for f in range(3)]

        def terms(other, lb):
            d, q = separation(xi, region, other, lb)
            lj = [region_l[other, lb, f : f + 1, :] for f in range(3)]
            wj = region_p[other, lb, 1:2, :]
            cs = ci + region_p[other, lb, 0:1, :]
            diff = [li[f] - lj[f] for f in range(3)]
            dv = [region[other, lb, 3 + f : 4 + f, :] - vi[f] for f in range(3)]
            along = sum(diff[f] * d[f] for f in range(3))
            drag = wj * sum(li[f] * dv[f] for f in range(3)) - wi * sum(
                lj[f] * dv[f] for f in range(3)
            )
            q2 = q * q
            q3 = q2 * q
            on_d = q * (q * drag - 8.0 * (cs * along))
            on_l = cs * q2
            gx = [on_d * d[f] + (on_l * diff[f]) * 2.0 for f in range(3)]
            gv = [q3 * lj[f] for f in range(3)]
            return gx + gv + [q3 * wj]

        return terms

    pair_sums(n_ref, columns, sums, 7, body)
    for t in range(4):
        s = row_sums(sums, t)
        w = press[0][t // 2, t % 2][1:2]
        rows = [(3.0 * particle_mass) * s[f : f + 1] for f in range(3)]
        half = viscosity * particle_mass
        for f in range(3):
            mine = lam[0][t // 2, t % 2][f : f + 1]
            rows.append(half * (w * s[3 + f : 4 + f] - mine * s[6:7]))
        out[t // 2, t % 2] = stack_rows(rows)


def last_grad_kernel(n_ref, wall_ref, *refs):
    state, grads = refs[:5], refs[5:10]
    partial, carried = refs[10], refs[11]
    lam_out, carried_out, region, region_g, columns, sums = refs[12:]
    fill_region(region, state, wall_ref)
    fill_region(region_g, grads)
    own_columns(columns, 0, (state[0], grads[0]))

    def body(column):
        xi = [column(0, f) for f in range(3)]
        gi = column(1, 0)

        def terms(other, lb):
            d, q = separation(xi, region, other, lb)
            weight = (gi + region_g[other, lb, 0:1, :]) * (q * q)
            return [weight * d[f] for f in range(3)]

        return terms

    pair_sums(n_ref, columns, sums, 3, body)
    for t in range(4):
        live = state[0][t // 2, t % 2][6:7] > 0.5
        s = row_sums(sums, t)
        part = partial[t // 2, t % 2]
        old = carried[t // 2, t % 2]
        new_pos, new_vel = [], []
        for f in range(3):
            extra = part[f : f + 1] + (6.0 * particle_mass) * s[f : f + 1]
            gx = old[f : f + 1] + jnp.where(live, extra, 0.0)
            gv = old[3 + f : 4 + f] + jnp.where(live, part[3 + f : 4 + f], 0.0)
            new_pos.append(gx)
            new_vel.append(gv + time_step * gx)
        lam_out[t // 2, t % 2] = stack_rows(
            [jnp.where(live, time_step * v, 0.0) for v in new_vel]
        )
        carried_out[t // 2, t % 2] = stack_rows(new_pos + new_vel)


def run_kernel(kernel, name, n_own, walls, arrays, outputs, regions, kinds, flops):
    tiles = (2, 2, FEATS, 2 * LANES)
    shape = jax.ShapeDtypeStruct(tiles, jnp.float32)
    smem = pl.BlockSpec(memory_space=pltpu.SMEM)
    vmem = pl.BlockSpec(memory_space=pltpu.VMEM)
    result = pl.pallas_call(
        kernel,
        name=name,
        out_shape=[shape] * outputs,
        in_specs=[smem, smem] + [vmem] * len(arrays),
        out_specs=[vmem] * outputs,
        scratch_shapes=[pltpu.VMEM((16, 2, FEATS, LANES), jnp.float32)] * regions
        + [
            pltpu.VMEM((kinds, 4, 2 * LANES, LANES), jnp.float32),
            pltpu.VMEM((4, 2 * LANES, LANES), jnp.float32),
        ],
        cost_estimate=pl.CostEstimate(
            flops=flops * 36 * 65536, bytes_accessed=1 << 20, transcendentals=0
        ),
    )(n_own, walls, *arrays)
    return result[0] if outputs == 1 else result


def per_device(exchange, positions, velocities, occupancy, cot_positions, cot_velocities):
    slots = positions.shape[3]
    assert positions.shape[1:] == (2, 2, 2 * LANES)
    live = lax.broadcasted_iota(jnp.int32, occupancy.shape + (slots,), 2) < occupancy[:, :, None]
    corner = jnp.stack(
        [
            lax.broadcasted_iota(jnp.float32, live.shape, 0),
            lax.broadcasted_iota(jnp.float32, live.shape, 1),
            jnp.zeros(live.shape, jnp.float32),
        ]
    )
    placed = jnp.where(live[None], positions + corner, FAR)
    mask = live.astype(jnp.float32)[None]
    packed = jnp.concatenate(
        [placed, velocities, mask, jnp.zeros_like(mask), cot_positions, cot_velocities], axis=0
    )
    packed = jnp.moveaxis(packed, 0, 2)
    packed = exchange.place(packed)
    state = packed[:, :, :8]
    grads = packed[:, :, 8:14]
    n_own = jnp.sum(state[:, :, 6], axis=-1).astype(jnp.int32).reshape(4)
    at_y = lax.axis_index("gy")
    walls = jnp.stack(
        [
            jnp.where(at_y == 0, -WALL, -2.0),
            jnp.where(at_y == exchange.count_y - 1, WALL, 2.0),
        ]
    ).astype(jnp.float32)
    run = functools.partial(run_kernel)

    grad_pos, grad_vel = grads[:, :, :3], grads[:, :, 3:]
    grad_vel = grad_vel + time_step * grad_pos
    pad2 = jnp.zeros((2, 2, 2, slots), jnp.float32)
    carried = jnp.concatenate([grad_pos, grad_vel, pad2], axis=2)
    lam = jnp.concatenate(
        [time_step * state[:, :, 6:7] * grad_vel, jnp.zeros((2, 2, 5, slots), jnp.float32)], axis=2
    )

    states, presses = [], []
    for step in range(STEPS):
        pieces = exchange.halo(state)
        own_press = run(density_kernel, "density", n_own, walls, pieces, 1, 1, 1, 13)
        press = exchange.halo(own_press)
        states.append(pieces)
        presses.append(press)
        if step + 1 < STEPS:
            state = run(accel_kernel, "accel", n_own, walls, pieces + press, 1, 2, 2, 28)

    for step in reversed(range(STEPS)):
        lam_pieces = exchange.halo(lam)
        own_grad = run(
            density_grad_kernel,
            "density_grad",
            n_own,
            walls,
            states[step] + lam_pieces + presses[step][:1],
            1,
            2,
            2,
            30,
        )
        grad_pieces = exchange.halo(own_grad)
        partial = run(
            main_grad_kernel,
            "main_grad",
            n_own,
            walls,
            states[step] + presses[step] + lam_pieces,
            1,
            3,
            3,
            65,
        )
        lam, carried = run(
            last_grad_kernel,
            "last_grad",
            n_own,
            walls,
            states[step] + grad_pieces + (partial, carried),
            2,
            2,
            2,
            18,
        )

    result = exchange.unplace(carried[:, :, :6])
    result = jnp.moveaxis(result, 2, 0)
    return (result[:3], result[3:] - time_step * result[:3])


def solution(mesh):
    spec = P(None, "gx", "gy", None)
    exchange = Exchange(mesh)
    return jax.shard_map(
        functools.partial(per_device, exchange),
        mesh=mesh,
        in_specs=(spec, spec, P("gx", "gy"), spec, spec),
        out_specs=(spec, spec),
        check_vma=False,
    )
```

```python
import functools

import jax
import jax.numpy as jnp
from jax import lax
from jax.experimental import pallas as pl
from jax.experimental.pallas import tpu as pltpu
from jax.sharding import PartitionSpec as P

STEPS = 4
time_step = 0.05
stiffness = 4.0
rest_density = 1.0
particle_mass = 0.15
viscosity = 0.5


FAR = 1.0e4
WALL = 1.0e5
ROWS = 16
LANES = 128
FEATS = 8
VMEM_LIMIT = 16 << 20


def ring_order(count):
    evens = list(range(0, count, 2))
    odds = list(range(1, count, 2))
    return evens + odds[::-1]


class Exchange:
    def __init__(self, mesh):
        self.count_x = mesh.shape["gx"]
        self.count_y = mesh.shape["gy"]
        self.order = ring_order(self.count_x)

    def permute(self, value, pairs):
        return lax.ppermute(value, ("gx", "gy"), pairs)

    def from_x(self, value, step):
        order, count = self.order, self.count_x
        pairs = [
            (order[(slot + step) % count] * self.count_y + b, order[slot] * self.count_y + b)
            for slot in range(count)
            for b in range(self.count_y)
        ]
        return self.permute(value, pairs)

    def from_y(self, value, step):
        pairs = [
            (a * self.count_y + (b + step) % self.count_y, a * self.count_y + b)
            for a in range(self.count_x)
            for b in range(self.count_y)
        ]
        return self.permute(value, pairs)

    def place(self, value):
        pairs = [
            (a * self.count_y + b, self.order[a] * self.count_y + b)
            for a in range(self.count_x)
            for b in range(self.count_y)
        ]
        return self.permute(value, pairs)

    def unplace(self, value):
        pairs = [
            (self.order[a] * self.count_y + b, a * self.count_y + b)
            for a in range(self.count_x)
            for b in range(self.count_y)
        ]
        return self.permute(value, pairs)

    def halo(self, own):
        x_low = self.from_x(own[1:2], -1)
        x_high = self.from_x(own[0:1], 1)
        upper = jnp.concatenate([x_low[:, 1:2], own[:, 1:2], x_high[:, 1:2]], axis=0)
        lower = jnp.concatenate([x_low[:, 0:1], own[:, 0:1], x_high[:, 0:1]], axis=0)
        y_low = self.from_y(upper, -1)
        y_high = self.from_y(lower, 1)
        return (own, x_low, x_high, y_low, y_high)


def region_tile(pieces, rx, ry):
    own, x_low, x_high, y_low, y_high = pieces
    if ry == 0:
        return y_low[rx, 0]
    if ry == 3:
        return y_high[rx, 0]
    if rx == 0:
        return x_low[0, ry - 1]
    if rx == 3:
        return x_high[0, ry - 1]
    return own[rx - 1, ry - 1]


def fill_region(region, pieces, wall_ref=None):
    row = lax.broadcasted_iota(jnp.int32, (FEATS, 2 * LANES), 0)
    for rx in range(4):
        for ry in range(4):
            block = region_tile(pieces, rx, ry)
            if wall_ref is not None:
                if rx in (0, 3):
                    block = jnp.where(row == 0, block + (-2.0 if rx == 0 else 2.0), block)
                if ry in (0, 3):
                    block = jnp.where(row == 1, block + wall_ref[0 if ry == 0 else 1], block)
            region[rx * 4 + ry, 0] = block[:, :LANES]
            region[rx * 4 + ry, 1] = block[:, LANES:]


def each_tile(work):
    def step(t, carry):
        work(t, t // 2, t - 2 * (t // 2))
        return carry

    lax.fori_loop(0, 4, step, 0)


def own_columns(columns, pieces, features):
    def work(t, tx, ty):
        at = 0
        for block, chosen in zip(pieces, features):
            value = block[tx, ty]
            padded = jnp.concatenate(
                [value, jnp.zeros((LANES - FEATS, 2 * LANES), jnp.float32)], axis=0
            )
            turned = padded.T
            for index, feature in enumerate(chosen):
                columns[at + index, t] = jnp.broadcast_to(
                    turned[:, feature : feature + 1], (2 * LANES, LANES)
                )
            at += len(chosen)

    each_tile(work)


def pair_sums(n_ref, columns, sums_ref, features, outputs, body):
    def tile_loop(t, carry):
        tx = t // 2
        ty = t - 2 * tx
        groups = (n_ref[t] + (ROWS - 1)) // ROWS

        def group_loop(g, carry):
            start = pl.multiple_of(g * ROWS, ROWS)
            terms_of = body([columns[f, t, pl.ds(start, ROWS), :] for f in range(features)])

            def row_loop(dx, totals):
                totals = list(totals)
                for dy in range(3):
                    other = (tx + dx) * 4 + ty + dy
                    for lb in range(2):
                        terms = terms_of(other, lb)
                        totals = [a + b for a, b in zip(totals, terms)]
                return tuple(totals)

            zero = jnp.zeros((ROWS, LANES), jnp.float32)
            totals = lax.fori_loop(0, 3, row_loop, (zero,) * outputs)
            for index, total in enumerate(totals):
                sums_ref[index, t, pl.ds(start, ROWS), :] = total
            return carry

        return lax.fori_loop(0, groups, group_loop, carry)

    lax.fori_loop(0, 4, tile_loop, 0)


def row_sums(sums_ref, t, outputs):
    return [jnp.sum(sums_ref[index, t].T, axis=0, keepdims=True) for index in range(outputs)]


def separation(xi, region, other, lb):
    d = [region[other, lb, f : f + 1, :] - xi[f] for f in range(3)]
    q = jnp.maximum(1.0 - d[0] * d[0] - d[1] * d[1] - d[2] * d[2], 0.0)
    return d, q


def stack_rows(rows):
    width = rows[0].shape[1]
    rows = list(rows) + [jnp.zeros((1, width), jnp.float32)] * (FEATS - len(rows))
    return jnp.concatenate(rows, axis=0)


def density_kernel(n_ref, wall_ref, *refs):
    pieces, (out, region, columns, sums) = refs[:5], refs[5:]
    fill_region(region, pieces, wall_ref)
    own_columns(columns, (pieces[0],), ((0, 1, 2),))

    def body(column):
        xi = column

        def terms(other, lb):
            d, q = separation(xi, region, other, lb)
            return [q * q * q]

        return terms

    pair_sums(n_ref, columns, sums, 3, 1, body)
    def finish(t, tx, ty):
        live = pieces[0][tx, ty][6:7] > 0.5
        density = particle_mass * row_sums(sums, t, 1)[0]
        padded = jnp.where(live, density, 1.0)
        inverse = jnp.where(live, 1.0 / padded, 0.0)
        coefficient = jnp.where(
            live, stiffness * (density / rest_density - 1.0) / (padded * padded), 0.0
        )
        out[tx, ty] = stack_rows([coefficient, inverse])

    each_tile(finish)


def accel_kernel(n_ref, wall_ref, *refs):
    state, press, (out, region, region_p, columns, sums) = refs[:5], refs[5:10], refs[10:]
    fill_region(region, state, wall_ref)
    fill_region(region_p, press)
    own_columns(columns, (state[0], press[0]), ((0, 1, 2), (0,)))

    def body(column):
        xi, ci = column[:3], column[3]

        def terms(other, lb):
            d, q = separation(xi, region, other, lb)
            q2 = q * q
            visc = q2 * q * region_p[other, lb, 1:2, :]
            push = (ci + region_p[other, lb, 0:1, :]) * q2
            moved = [visc * region[other, lb, 3 + f : 4 + f, :] for f in range(3)]
            pushed = [push * d[f] for f in range(3)]
            return moved + [visc] + pushed

        return terms

    pair_sums(n_ref, columns, sums, 4, 7, body)
    def finish(t, tx, ty):
        own = state[0][tx, ty]
        live = own[6:7] > 0.5
        s = row_sums(sums, t, 7)
        new_pos, new_vel = [], []
        for f in range(3):
            vel = own[3 + f : 4 + f]
            accel = particle_mass * (
                viscosity * (s[f] - vel * s[3]) - 6.0 * s[4 + f]
            )
            vel = jnp.where(live, vel + time_step * accel, vel)
            new_vel.append(vel)
            new_pos.append(
                jnp.where(live, own[f : f + 1] + time_step * vel, own[f : f + 1])
            )
        out[tx, ty] = stack_rows(new_pos + new_vel + [own[6:7]])

    each_tile(finish)


def density_grad_kernel(n_ref, wall_ref, *refs):
    state, lam, press, (out, region, region_l, columns, sums) = (
        refs[:5],
        refs[5:10],
        refs[10],
        refs[11:],
    )
    fill_region(region, state, wall_ref)
    fill_region(region_l, lam)
    own_columns(columns, (state[0], lam[0]), ((0, 1, 2, 3, 4, 5), (0, 1, 2)))

    def body(column):
        xi, vi, li = column[:3], column[3:6], column[6:]

        def terms(other, lb):
            d, q = separation(xi, region, other, lb)
            lj = [region_l[other, lb, f : f + 1, :] for f in range(3)]
            q2 = q * q
            along = sum((li[f] - lj[f]) * d[f] for f in range(3))
            moved = sum(lj[f] * (vi[f] - region[other, lb, 3 + f : 4 + f, :]) for f in range(3))
            return [q2 * along, q2 * q * moved]

        return terms

    pair_sums(n_ref, columns, sums, 9, 2, body)
    def finish(t, tx, ty):
        live = state[0][tx, ty][6:7] > 0.5
        s = row_sums(sums, t, 2)
        c = press[tx, ty][0:1]
        w = press[tx, ty][1:2]
        grad_c = (-6.0 * particle_mass) * s[0]
        grad_w = (viscosity * particle_mass) * s[1]
        grad = grad_c * (stiffness * w * w - 2.0 * c * w) - grad_w * w * w
        out[tx, ty] = stack_rows([jnp.where(live, grad, 0.0)])

    each_tile(finish)


def main_grad_kernel(n_ref, wall_ref, *refs):
    state, press, lam = refs[:5], refs[5:10], refs[10:15]
    out, region, region_p, region_l, columns, sums = refs[15:]
    fill_region(region, state, wall_ref)
    fill_region(region_p, press)
    fill_region(region_l, lam)
    own_columns(
        columns, (state[0], press[0], lam[0]), ((0, 1, 2, 3, 4, 5), (0, 1), (0, 1, 2))
    )

    def body(column):
        xi, vi, li = column[:3], column[3:6], column[8:]
        ci, wi = column[6:8]

        def terms(other, lb):
            d, q = separation(xi, region, other, lb)
            lj = [region_l[other, lb, f : f + 1, :] for f in range(3)]
            wj = region_p[other, lb, 1:2, :]
            cs = ci + region_p[other, lb, 0:1, :]
            diff = [li[f] - lj[f] for f in range(3)]
            dv = [region[other, lb, 3 + f : 4 + f, :] - vi[f] for f in range(3)]
            along = sum(diff[f] * d[f] for f in range(3))
            drag = wj * sum(li[f] * dv[f] for f in range(3)) - wi * sum(
                lj[f] * dv[f] for f in range(3)
            )
            q2 = q * q
            q3 = q2 * q
            on_d = q * (q * drag - 8.0 * (cs * along))
            on_l = cs * q2
            gx = [on_d * d[f] + (on_l * diff[f]) * 2.0 for f in range(3)]
            gv = [q3 * lj[f] for f in range(3)]
            return gx + gv + [q3 * wj]

        return terms

    pair_sums(n_ref, columns, sums, 11, 7, body)
    def finish(t, tx, ty):
        s = row_sums(sums, t, 7)
        w = press[0][tx, ty][1:2]
        rows = [(3.0 * particle_mass) * s[f] for f in range(3)]
        half = viscosity * particle_mass
        for f in range(3):
            mine = lam[0][tx, ty][f : f + 1]
            rows.append(half * (w * s[3 + f] - mine * s[6]))
        out[tx, ty] = stack_rows(rows)

    each_tile(finish)


def last_grad_kernel(n_ref, wall_ref, *refs):
    state, grads = refs[:5], refs[5:10]
    partial, carried = refs[10], refs[11]
    lam_out, carried_out, region, region_g, columns, sums = refs[12:]
    fill_region(region, state, wall_ref)
    fill_region(region_g, grads)
    own_columns(columns, (state[0], grads[0]), ((0, 1, 2), (0,)))

    def body(column):
        xi, gi = column[:3], column[3]

        def terms(other, lb):
            d, q = separation(xi, region, other, lb)
            weight = (gi + region_g[other, lb, 0:1, :]) * (q * q)
            return [weight * d[f] for f in range(3)]

        return terms

    pair_sums(n_ref, columns, sums, 4, 3, body)
    def finish(t, tx, ty):
        live = state[0][tx, ty][6:7] > 0.5
        s = row_sums(sums, t, 3)
        part = partial[tx, ty]
        old = carried[tx, ty]
        new_pos, new_vel = [], []
        for f in range(3):
            extra = part[f : f + 1] + (6.0 * particle_mass) * s[f]
            gx = old[f : f + 1] + jnp.where(live, extra, 0.0)
            gv = old[3 + f : 4 + f] + jnp.where(live, part[3 + f : 4 + f], 0.0)
            new_pos.append(gx)
            new_vel.append(gv + time_step * gx)
        lam_out[tx, ty] = stack_rows(
            [jnp.where(live, time_step * v, 0.0) for v in new_vel]
        )
        carried_out[tx, ty] = stack_rows(new_pos + new_vel)

    each_tile(finish)


def run_kernel(kernel, name, n_own, walls, arrays, outputs, regions, features, totals, flops):
    tiles = (2, 2, FEATS, 2 * LANES)
    shape = jax.ShapeDtypeStruct(tiles, jnp.float32)
    smem = pl.BlockSpec(memory_space=pltpu.SMEM)
    vmem = pl.BlockSpec(memory_space=pltpu.VMEM)
    result = pl.pallas_call(
        kernel,
        name=name,
        out_shape=[shape] * outputs,
        in_specs=[smem, smem] + [vmem] * len(arrays),
        out_specs=[vmem] * outputs,
        scratch_shapes=[pltpu.VMEM((16, 2, FEATS, LANES), jnp.float32)] * regions
        + [
            pltpu.VMEM((features, 4, 2 * LANES, LANES), jnp.float32),
            pltpu.VMEM((totals, 4, 2 * LANES, LANES), jnp.float32),
        ],
        compiler_params=pltpu.CompilerParams(vmem_limit_bytes=VMEM_LIMIT),
        cost_estimate=pl.CostEstimate(
            flops=flops * 36 * 65536, bytes_accessed=1 << 20, transcendentals=0
        ),
    )(n_own, walls, *arrays)
    return result[0] if outputs == 1 else result


def per_device(exchange, positions, velocities, occupancy, cot_positions, cot_velocities):
    slots = positions.shape[3]
    assert positions.shape[1:] == (2, 2, 2 * LANES)
    live = lax.broadcasted_iota(jnp.int32, occupancy.shape + (slots,), 2) < occupancy[:, :, None]
    corner = jnp.stack(
        [
            lax.broadcasted_iota(jnp.float32, live.shape, 0),
            lax.broadcasted_iota(jnp.float32, live.shape, 1),
            jnp.zeros(live.shape, jnp.float32),
        ]
    )
    placed = jnp.where(live[None], positions + corner, FAR)
    mask = live.astype(jnp.float32)[None]
    packed = jnp.concatenate(
        [placed, velocities, mask, jnp.zeros_like(mask), cot_positions, cot_velocities], axis=0
    )
    packed = jnp.moveaxis(packed, 0, 2)
    packed = exchange.place(packed)
    state = packed[:, :, :8]
    grads = packed[:, :, 8:14]
    n_own = jnp.sum(state[:, :, 6], axis=-1).astype(jnp.int32).reshape(4)
    at_y = lax.axis_index("gy")
    walls = jnp.stack(
        [
            jnp.where(at_y == 0, -WALL, -2.0),
            jnp.where(at_y == exchange.count_y - 1, WALL, 2.0),
        ]
    ).astype(jnp.float32)
    run = functools.partial(run_kernel)

    grad_pos, grad_vel = grads[:, :, :3], grads[:, :, 3:]
    grad_vel = grad_vel + time_step * grad_pos
    pad2 = jnp.zeros((2, 2, 2, slots), jnp.float32)
    carried = jnp.concatenate([grad_pos, grad_vel, pad2], axis=2)
    lam = jnp.concatenate(
        [time_step * state[:, :, 6:7] * grad_vel, jnp.zeros((2, 2, 5, slots), jnp.float32)], axis=2
    )

    states, presses = [], []
    for step in range(STEPS):
        pieces = exchange.halo(state)
        own_press = run(density_kernel, "density", n_own, walls, pieces, 1, 1, 3, 1, 13)
        press = exchange.halo(own_press)
        states.append(pieces)
        presses.append(press)
        if step + 1 < STEPS:
            state = run(accel_kernel, "accel", n_own, walls, pieces + press, 1, 2, 4, 7, 28)

    for step in reversed(range(STEPS)):
        lam_pieces = exchange.halo(lam)
        own_grad = run(
            density_grad_kernel,
            "density_grad",
            n_own,
            walls,
            states[step] + lam_pieces + presses[step][:1],
            1,
            2,
            9,
            2,
            30,
        )
        grad_pieces = exchange.halo(own_grad)
        partial = run(
            main_grad_kernel,
            "main_grad",
            n_own,
            walls,
            states[step] + presses[step] + lam_pieces,
            1,
            3,
            11,
            7,
            65,
        )
        lam, carried = run(
            last_grad_kernel,
            "last_grad",
            n_own,
            walls,
            states[step] + grad_pieces + (partial, carried),
            2,
            2,
            4,
            3,
            18,
        )

    result = exchange.unplace(carried[:, :, :6])
    result = jnp.moveaxis(result, 2, 0)
    return (result[:3], result[3:] - time_step * result[:3])


def solution(mesh):
    spec = P(None, "gx", "gy", None)
    exchange = Exchange(mesh)
    return jax.shard_map(
        functools.partial(per_device, exchange),
        mesh=mesh,
        in_specs=(spec, spec, P("gx", "gy"), spec, spec),
        out_specs=(spec, spec),
        check_vma=False,
    )
```

```python
import functools

import jax
import jax.numpy as jnp
from jax import lax
from jax.experimental import pallas as pl
from jax.experimental.pallas import tpu as pltpu
from jax.sharding import PartitionSpec as P

STEPS = 4
time_step = 0.05
stiffness = 4.0
rest_density = 1.0
particle_mass = 0.15
viscosity = 0.5


FAR = 1.0e4
WALL = 1.0e5
ROWS = 16
LANES = 128
FEATS = 8
VMEM_LIMIT = 16 << 20
BLOCKS = 32
PAD = 4
MERGE = 4
REACH = 1.001
NEVER = 1.0e30


def ring_order(count):
    evens = list(range(0, count, 2))
    odds = list(range(1, count, 2))
    return evens + odds[::-1]


class Exchange:
    def __init__(self, mesh):
        self.count_x = mesh.shape["gx"]
        self.count_y = mesh.shape["gy"]
        self.order = ring_order(self.count_x)

    def permute(self, value, pairs):
        return lax.ppermute(value, ("gx", "gy"), pairs)

    def from_x(self, value, step):
        order, count = self.order, self.count_x
        pairs = [
            (order[(slot + step) % count] * self.count_y + b, order[slot] * self.count_y + b)
            for slot in range(count)
            for b in range(self.count_y)
        ]
        return self.permute(value, pairs)

    def from_y(self, value, step):
        pairs = [
            (a * self.count_y + (b + step) % self.count_y, a * self.count_y + b)
            for a in range(self.count_x)
            for b in range(self.count_y)
        ]
        return self.permute(value, pairs)

    def place(self, value):
        pairs = [
            (a * self.count_y + b, self.order[a] * self.count_y + b)
            for a in range(self.count_x)
            for b in range(self.count_y)
        ]
        return self.permute(value, pairs)

    def unplace(self, value):
        pairs = [
            (self.order[a] * self.count_y + b, a * self.count_y + b)
            for a in range(self.count_x)
            for b in range(self.count_y)
        ]
        return self.permute(value, pairs)

    def halo(self, own):
        x_low = self.from_x(own[1:2], -1)
        x_high = self.from_x(own[0:1], 1)
        upper = jnp.concatenate([x_low[:, 1:2], own[:, 1:2], x_high[:, 1:2]], axis=0)
        lower = jnp.concatenate([x_low[:, 0:1], own[:, 0:1], x_high[:, 0:1]], axis=0)
        y_low = self.from_y(upper, -1)
        y_high = self.from_y(lower, 1)
        return (own, x_low, x_high, y_low, y_high)


def region_tile(pieces, rx, ry):
    own, x_low, x_high, y_low, y_high = pieces
    if ry == 0:
        return y_low[rx, 0]
    if ry == 3:
        return y_high[rx, 0]
    if rx == 0:
        return x_low[0, ry - 1]
    if rx == 3:
        return x_high[0, ry - 1]
    return own[rx - 1, ry - 1]


def fill_region(region, pieces, wall_ref=None):
    row = lax.broadcasted_iota(jnp.int32, (FEATS, 2 * LANES), 0)
    for rx in range(4):
        for ry in range(4):
            block = region_tile(pieces, rx, ry)
            if wall_ref is not None:
                if rx in (0, 3):
                    block = jnp.where(row == 0, block + (-2.0 if rx == 0 else 2.0), block)
                if ry in (0, 3):
                    block = jnp.where(row == 1, block + wall_ref[0 if ry == 0 else 1], block)
            region[rx * 4 + ry, 0] = block[:, :LANES]
            region[rx * 4 + ry, 1] = block[:, LANES:]


def each_tile(work):
    def step(t, carry):
        work(t, t // 2, t - 2 * (t // 2))
        return carry

    lax.fori_loop(0, 4, step, 0)


def own_columns(columns, pieces, features):
    def work(t, tx, ty):
        at = 0
        for block, chosen in zip(pieces, features):
            value = block[tx, ty]
            padded = jnp.concatenate(
                [value, jnp.zeros((LANES - FEATS, 2 * LANES), jnp.float32)], axis=0
            )
            turned = padded.T
            for index, feature in enumerate(chosen):
                columns[at + index, t] = jnp.broadcast_to(
                    turned[:, feature : feature + 1], (2 * LANES, LANES)
                )
            at += len(chosen)

    each_tile(work)


def take_lanes(sources, row):
    lane = jnp.broadcast_to(row % LANES, (FEATS, LANES))
    block = jnp.broadcast_to(row // LANES, (FEATS, LANES))
    picked = jnp.zeros((FEATS, LANES), jnp.float32)
    for at, source in enumerate(sources):
        picked = jnp.where(block == at, jnp.take_along_axis(source, lane, axis=1), picked)
    return picked


def merge_region(merged, region, order_ref, counts_ref):
    for at in range(BLOCKS + PAD):
        merged[at] = jnp.zeros((FEATS, LANES), jnp.float32)
    used = (counts_ref[4] + (LANES - 1)) // LANES

    def step(index, carry):
        for near in range(MERGE):
            at = index * MERGE + near
            sources = [region[s // 2, s % 2] for s in range(BLOCKS)]
            merged[at] = take_lanes(sources, order_ref[at])
        return carry

    lax.fori_loop(0, (used + (MERGE - 1)) // MERGE, step, 0)


def block_ranges(ranges, merged, own, counts_ref):
    depth = merged[:BLOCKS, 2, :]
    rank = lax.broadcasted_iota(jnp.int32, (BLOCKS, LANES), 0) * LANES
    rank = rank + lax.broadcasted_iota(jnp.int32, (BLOCKS, LANES), 1)
    held = rank < counts_ref[4]
    least = jnp.min(jnp.where(held, depth, WALL), axis=1, keepdims=True)
    most = jnp.max(jnp.where(held, depth, -WALL), axis=1, keepdims=True)
    rows, limits = [], []
    for t in range(4):
        for lb in range(2):
            rows.append(own[t // 2, t % 2][2:3, lb * LANES : (lb + 1) * LANES])
            lane = lax.broadcasted_iota(jnp.int32, (1, LANES), 1) + lb * LANES
            limits.append((lane < counts_ref[t]).astype(jnp.float32))
    mine = jnp.concatenate(rows, axis=0)
    inside = jnp.concatenate(limits, axis=0) > 0.5
    low = jnp.where(inside, mine, WALL)
    high = jnp.where(inside, mine, -WALL)
    reach = 1
    while reach < ROWS:
        low = jnp.minimum(low, pltpu.roll(low, LANES - reach, 1))
        high = jnp.maximum(high, pltpu.roll(high, LANES - reach, 1))
        reach *= 2
    low = low - REACH
    high = high + REACH
    first = jnp.full((FEATS, LANES), BLOCKS, jnp.int32)
    past = jnp.zeros((FEATS, LANES), jnp.int32)
    for at in range(BLOCKS):
        near = (jnp.broadcast_to(most[at : at + 1], (FEATS, LANES)) >= low) & (
            jnp.broadcast_to(least[at : at + 1], (FEATS, LANES)) <= high
        )
        first = jnp.where(near, jnp.minimum(first, at), first)
        past = jnp.where(near, at + 1, past)
    ranges[0] = first
    ranges[1] = past


def pair_sums(counts_ref, range_ref, columns, sums_ref, features, outputs, together, body):
    per_block = LANES // ROWS

    def tile_loop(t, carry):
        groups = (counts_ref[t] + (ROWS - 1)) // ROWS

        def group_loop(g, carry):
            start = pl.multiple_of(g * ROWS, ROWS)
            terms_of = body([columns[f, t, pl.ds(start, ROWS), :] for f in range(features)], t)
            line = t * 2 + g // per_block
            lane = (g % per_block) * ROWS
            first = jnp.clip(range_ref[0, line, lane], 0, BLOCKS)
            past = jnp.clip(range_ref[1, line, lane], 0, BLOCKS)
            trips = (jnp.maximum(past - first, 0) + (together - 1)) // together

            def block_loop(index, totals):
                totals = list(totals)
                for near in range(together):
                    terms = terms_of(first + index * together + near)
                    totals = [a + b for a, b in zip(totals, terms)]
                return tuple(totals)

            zero = jnp.zeros((ROWS, LANES), jnp.float32)
            totals = lax.fori_loop(0, trips, block_loop, (zero,) * outputs)
            for index, total in enumerate(totals):
                sums_ref[index, t, pl.ds(start, ROWS), :] = total
            return carry

        return lax.fori_loop(0, groups, group_loop, carry)

    lax.fori_loop(0, 4, tile_loop, 0)


def row_sums(sums_ref, t, outputs):
    return [jnp.sum(sums_ref[index, t].T, axis=0, keepdims=True) for index in range(outputs)]


def separation(xi, merged, bias_ref, t, block):
    d = [merged[block, f : f + 1, :] - xi[f] for f in range(3)]
    bias = bias_ref[t, block]
    q = jnp.maximum(bias - d[0] * d[0] - d[1] * d[1] - d[2] * d[2], 0.0)
    return d, q


def stack_rows(rows):
    width = rows[0].shape[1]
    rows = list(rows) + [jnp.zeros((1, width), jnp.float32)] * (FEATS - len(rows))
    return jnp.concatenate(rows, axis=0)


def sort_kernel(order_ref, packed_ref, out):
    for tx, ty in ((0, 0), (0, 1), (1, 0), (1, 1)):
        for part in range(packed_ref.shape[2] // FEATS):
            value = packed_ref[tx, ty, part * FEATS : (part + 1) * FEATS]
            sources = [value[:, :LANES], value[:, LANES:]]
            halves = [
                take_lanes(sources, order_ref[tx, ty : ty + 1, lb * LANES : (lb + 1) * LANES])
                for lb in range(2)
            ]
            out[tx, ty, part * FEATS : (part + 1) * FEATS] = jnp.concatenate(halves, axis=1)


def merge_kernel(counts_ref, order_ref, *refs):
    pieces, (merged, region) = refs[:5], refs[5:]
    fill_region(region, pieces)
    merge_region(merged, region, order_ref, counts_ref)


def density_kernel(counts_ref, wall_ref, order_ref, bias_ref, *refs):
    pieces = refs[:5]
    out, merged, ranges, region, columns, sums, range_ref, sem = refs[5:]
    fill_region(region, pieces, wall_ref)
    merge_region(merged, region, order_ref, counts_ref)
    block_ranges(ranges, merged, pieces[0], counts_ref)
    own_columns(columns, (pieces[0],), ((0, 1, 2),))
    copy = pltpu.make_async_copy(ranges, range_ref, sem)
    copy.start()
    copy.wait()

    def body(column, t):
        def terms(block):
            d, q = separation(column, merged, bias_ref, t, block)
            return [q * q * q]

        return terms

    pair_sums(counts_ref, range_ref, columns, sums, 3, 1, 4, body)

    def finish(t, tx, ty):
        live = pieces[0][tx, ty][6:7] > 0.5
        density = particle_mass * row_sums(sums, t, 1)[0]
        padded = jnp.where(live, density, 1.0)
        inverse = jnp.where(live, 1.0 / padded, 0.0)
        coefficient = jnp.where(
            live, stiffness * (density / rest_density - 1.0) / (padded * padded), 0.0
        )
        out[tx, ty] = stack_rows([coefficient, inverse])

    each_tile(finish)


def accel_kernel(counts_ref, range_ref, order_ref, bias_ref, merged, state, *refs):
    press, (out, merged_p, region, columns, sums) = refs[:5], refs[5:]
    fill_region(region, press)
    merge_region(merged_p, region, order_ref, counts_ref)
    own_columns(columns, (state, press[0]), ((0, 1, 2), (0,)))

    def body(column, t):
        xi, ci = column[:3], column[3]

        def terms(block):
            d, q = separation(xi, merged, bias_ref, t, block)
            q2 = q * q
            visc = q2 * q * merged_p[block, 1:2, :]
            push = (ci + merged_p[block, 0:1, :]) * q2
            moved = [visc * merged[block, 3 + f : 4 + f, :] for f in range(3)]
            pushed = [push * d[f] for f in range(3)]
            return moved + [visc] + pushed

        return terms

    pair_sums(counts_ref, range_ref, columns, sums, 4, 7, 3, body)

    def finish(t, tx, ty):
        own = state[tx, ty]
        live = own[6:7] > 0.5
        s = row_sums(sums, t, 7)
        new_pos, new_vel = [], []
        for f in range(3):
            vel = own[3 + f : 4 + f]
            accel = particle_mass * (viscosity * (s[f] - vel * s[3]) - 6.0 * s[4 + f])
            vel = jnp.where(live, vel + time_step * accel, vel)
            new_vel.append(vel)
            new_pos.append(
                jnp.where(live, own[f : f + 1] + time_step * vel, own[f : f + 1])
            )
        out[tx, ty] = stack_rows(new_pos + new_vel + [own[6:7]])

    each_tile(finish)


def density_grad_kernel(counts_ref, range_ref, order_ref, bias_ref, merged, state, press, *refs):
    lam, (out, merged_l, region, columns, sums) = refs[:5], refs[5:]
    fill_region(region, lam)
    merge_region(merged_l, region, order_ref, counts_ref)
    own_columns(columns, (state, lam[0]), ((0, 1, 2, 3, 4, 5), (0, 1, 2)))

    def body(column, t):
        xi, vi, li = column[:3], column[3:6], column[6:]

        def terms(block):
            d, q = separation(xi, merged, bias_ref, t, block)
            lj = [merged_l[block, f : f + 1, :] for f in range(3)]
            q2 = q * q
            along = sum((li[f] - lj[f]) * d[f] for f in range(3))
            moved = sum(lj[f] * (vi[f] - merged[block, 3 + f : 4 + f, :]) for f in range(3))
            return [q2 * along, q2 * q * moved]

        return terms

    pair_sums(counts_ref, range_ref, columns, sums, 9, 2, 3, body)

    def finish(t, tx, ty):
        live = state[tx, ty][6:7] > 0.5
        s = row_sums(sums, t, 2)
        c = press[tx, ty][0:1]
        w = press[tx, ty][1:2]
        grad_c = (-6.0 * particle_mass) * s[0]
        grad_w = (viscosity * particle_mass) * s[1]
        grad = grad_c * (stiffness * w * w - 2.0 * c * w) - grad_w * w * w
        out[tx, ty] = stack_rows([jnp.where(live, grad, 0.0)])

    each_tile(finish)


def main_grad_kernel(counts_ref, range_ref, bias_ref, merged, merged_p, merged_l, *refs):
    state, press, lam, out, columns, sums = refs
    own_columns(columns, (state, press, lam), ((0, 1, 2, 3, 4, 5), (0, 1), (0, 1, 2)))

    def body(column, t):
        xi, vi, li = column[:3], column[3:6], column[8:]
        ci, wi = column[6:8]

        def terms(block):
            d, q = separation(xi, merged, bias_ref, t, block)
            lj = [merged_l[block, f : f + 1, :] for f in range(3)]
            wj = merged_p[block, 1:2, :]
            cs = ci + merged_p[block, 0:1, :]
            diff = [li[f] - lj[f] for f in range(3)]
            dv = [merged[block, 3 + f : 4 + f, :] - vi[f] for f in range(3)]
            along = sum(diff[f] * d[f] for f in range(3))
            drag = wj * sum(li[f] * dv[f] for f in range(3)) - wi * sum(
                lj[f] * dv[f] for f in range(3)
            )
            q2 = q * q
            q3 = q2 * q
            on_d = q * (q * drag - 8.0 * (cs * along))
            on_l = (cs * q2) * 2.0
            gx = [on_d * d[f] + on_l * diff[f] for f in range(3)]
            gv = [q3 * lj[f] for f in range(3)]
            return gx + gv + [q3 * wj]

        return terms

    pair_sums(counts_ref, range_ref, columns, sums, 11, 7, 2, body)

    def finish(t, tx, ty):
        s = row_sums(sums, t, 7)
        w = press[tx, ty][1:2]
        rows = [(3.0 * particle_mass) * s[f] for f in range(3)]
        half = viscosity * particle_mass
        for f in range(3):
            mine = lam[tx, ty][f : f + 1]
            rows.append(half * (w * s[3 + f] - mine * s[6]))
        out[tx, ty] = stack_rows(rows)

    each_tile(finish)


def last_grad_kernel(counts_ref, range_ref, order_ref, bias_ref, merged, state, *refs):
    grads, partial, carried = refs[:5], refs[5], refs[6]
    lam_out, carried_out, region, merged_g, columns, sums = refs[7:]
    fill_region(region, grads)
    merge_region(merged_g, region, order_ref, counts_ref)
    own_columns(columns, (state, grads[0]), ((0, 1, 2), (0,)))

    def body(column, t):
        xi, gi = column[:3], column[3]

        def terms(block):
            d, q = separation(xi, merged, bias_ref, t, block)
            weight = (gi + merged_g[block, 0:1, :]) * (q * q)
            return [weight * d[f] for f in range(3)]

        return terms

    pair_sums(counts_ref, range_ref, columns, sums, 4, 3, 4, body)

    def finish(t, tx, ty):
        live = state[tx, ty][6:7] > 0.5
        s = row_sums(sums, t, 3)
        part = partial[tx, ty]
        old = carried[tx, ty]
        new_pos, new_vel = [], []
        for f in range(3):
            extra = part[f : f + 1] + (6.0 * particle_mass) * s[f]
            gx = old[f : f + 1] + jnp.where(live, extra, 0.0)
            gv = old[3 + f : 4 + f] + jnp.where(live, part[3 + f : 4 + f], 0.0)
            new_pos.append(gx)
            new_vel.append(gv + time_step * gx)
        lam_out[tx, ty] = stack_rows([jnp.where(live, time_step * v, 0.0) for v in new_vel])
        carried_out[tx, ty] = stack_rows(new_pos + new_vel)

    each_tile(finish)


TILES = jax.ShapeDtypeStruct((2, 2, FEATS, 2 * LANES), jnp.float32)
MERGED = jax.ShapeDtypeStruct((BLOCKS + PAD, FEATS, LANES), jnp.float32)
RANGES = jax.ShapeDtypeStruct((2, FEATS, LANES), jnp.int32)
REGION = pltpu.VMEM((16, 2, FEATS, LANES), jnp.float32)


def per_pair(features, outputs):
    tile = (4, 2 * LANES, LANES)
    return [pltpu.VMEM((features,) + tile, jnp.float32), pltpu.VMEM((outputs,) + tile, jnp.float32)]


def run_kernel(kernel, name, scalars, arrays, out_shape, scratch, cycles):
    smem = pl.BlockSpec(memory_space=pltpu.SMEM)
    vmem = pl.BlockSpec(memory_space=pltpu.VMEM)
    result = pl.pallas_call(
        kernel,
        name=name,
        out_shape=out_shape,
        in_specs=[smem] * len(scalars) + [vmem] * len(arrays),
        out_specs=[vmem] * len(out_shape),
        scratch_shapes=scratch,
        compiler_params=pltpu.CompilerParams(vmem_limit_bytes=VMEM_LIMIT),
        cost_estimate=pl.CostEstimate(
            flops=cycles * 4096, bytes_accessed=1 << 18, transcendentals=0
        ),
    )(*scalars, *arrays)
    return result


def per_device(exchange, positions, velocities, occupancy, cot_positions, cot_velocities):
    slots = positions.shape[3]
    assert positions.shape[1:] == (2, 2, 2 * LANES)
    live = lax.broadcasted_iota(jnp.int32, occupancy.shape + (slots,), 2) < occupancy[:, :, None]
    corner = jnp.stack(
        [
            lax.broadcasted_iota(jnp.float32, live.shape, 0),
            lax.broadcasted_iota(jnp.float32, live.shape, 1),
            jnp.zeros(live.shape, jnp.float32),
        ]
    )
    placed = jnp.where(live[None], positions + corner, FAR)
    mask = live.astype(jnp.float32)[None]
    spare = jnp.zeros_like(mask)
    packed = jnp.concatenate(
        [placed, velocities, mask, spare, cot_positions, cot_velocities, spare, spare], axis=0
    )
    packed = jnp.moveaxis(packed, 0, 2)
    depth_key = jnp.where(live, positions[2], WALL)
    slot = lax.broadcasted_iota(jnp.int32, live.shape, 2)
    by_depth = lax.sort((depth_key, slot), dimension=2, num_keys=1)[1]
    back = lax.sort((by_depth, slot), dimension=2, num_keys=1)[1]
    (packed,) = run_kernel(
        sort_kernel,
        "sort_own",
        (),
        (by_depth, packed),
        [jax.ShapeDtypeStruct(packed.shape, jnp.float32)],
        [],
        500,
    )
    packed = exchange.place(packed)
    state = packed[:, :, :8]
    grads = packed[:, :, 8:14]
    n_own = jnp.sum(state[:, :, 6], axis=-1).astype(jnp.int32).reshape(4)
    at_y = lax.axis_index("gy")
    at_low = at_y == 0
    at_high = at_y == exchange.count_y - 1
    walls = jnp.stack([jnp.where(at_low, -WALL, -2.0), jnp.where(at_high, WALL, 2.0)])
    walls = walls.astype(jnp.float32)

    grad_pos, grad_vel = grads[:, :, :3], grads[:, :, 3:]
    grad_vel = grad_vel + time_step * grad_pos
    pad2 = jnp.zeros((2, 2, 2, slots), jnp.float32)
    carried = jnp.concatenate([grad_pos, grad_vel, pad2], axis=2)
    lam = jnp.concatenate(
        [time_step * state[:, :, 6:7] * grad_vel, jnp.zeros((2, 2, 5, slots), jnp.float32)], axis=2
    )

    pieces = exchange.halo(state)
    own, x_low, x_high, y_low, y_high = [piece[:, :, (2, 6)] for piece in pieces]
    wide = jnp.concatenate([x_low, own, x_high], axis=0)
    wide = jnp.concatenate([y_low, wide, y_high], axis=1)
    row_y = lax.broadcasted_iota(jnp.int32, (4, 4, slots), 1)
    beyond = ((row_y == 0) & at_low) | ((row_y == 3) & at_high)
    present = (wide[:, :, 1] > 0.5) & ~beyond
    key = jnp.where(present, wide[:, :, 0], WALL).reshape(-1)
    place = lax.broadcasted_iota(jnp.int32, key.shape, 0)
    order = lax.sort((key, place), dimension=0, num_keys=1)[1]
    total = jnp.sum(present.astype(jnp.int32))
    counts = jnp.concatenate([n_own, total[None]])
    tile_x = order // (4 * slots)
    tile_y = (order // slots) % 4
    bias = []
    for t in range(4):
        by_x = (tile_x >= t // 2) & (tile_x <= t // 2 + 2)
        by_y = (tile_y >= t % 2) & (tile_y <= t % 2 + 2)
        bias.append(jnp.where(by_x & by_y & (place < total), 1.0, -NEVER))
    bias = jnp.stack(bias).reshape(4, BLOCKS, 1, LANES)
    bias = jnp.pad(bias, ((0, 0), (0, PAD), (0, 0), (0, 0)), constant_values=-NEVER)
    order = order.reshape(BLOCKS, 1, LANES)

    saved = []
    for step in range(STEPS):
        if step > 0:
            pieces = exchange.halo(state)
        own_press, merged, ranges = run_kernel(
            density_kernel,
            "density",
            (counts, walls),
            (order, bias) + pieces,
            [TILES, MERGED, RANGES],
            [REGION] + per_pair(3, 1) + [pltpu.SMEM(RANGES.shape, jnp.int32), pltpu.SemaphoreType.DMA],
            8000,
        )
        press = exchange.halo(own_press)
        if step + 1 < STEPS:
            new_state, merged_p = run_kernel(
                accel_kernel,
                "accel",
                (counts, ranges),
                (order, bias, merged, state) + press,
                [TILES, MERGED],
                [REGION] + per_pair(4, 7),
                10000,
            )
        else:
            new_state = state
            (merged_p,) = run_kernel(
                merge_kernel, "merge", (counts,), (order,) + press, [MERGED], [REGION], 2000
            )
        saved.append((state, own_press, ranges, merged, merged_p))
        state = new_state

    for step in reversed(range(STEPS)):
        state, own_press, ranges, merged, merged_p = saved[step]
        lam_pieces = exchange.halo(lam)
        own_grad, merged_l = run_kernel(
            density_grad_kernel,
            "density_grad",
            (counts, ranges),
            (order, bias, merged, state, own_press) + lam_pieces,
            [TILES, MERGED],
            [REGION] + per_pair(9, 2),
            10000,
        )
        grad_pieces = exchange.halo(own_grad)
        (partial,) = run_kernel(
            main_grad_kernel,
            "main_grad",
            (counts, ranges),
            (bias, merged, merged_p, merged_l, state, own_press, lam),
            [TILES],
            per_pair(11, 7),
            20000,
        )
        lam, carried = run_kernel(
            last_grad_kernel,
            "last_grad",
            (counts, ranges),
            (order, bias, merged, state) + grad_pieces + (partial, carried),
            [TILES, TILES],
            [REGION, pltpu.VMEM(MERGED.shape, jnp.float32)] + per_pair(4, 3),
            8000,
        )

    result = exchange.unplace(carried)
    (result,) = run_kernel(sort_kernel, "unsort_own", (), (back, result), [TILES], [], 500)
    result = jnp.moveaxis(result[:, :, :6], 2, 0)
    return (result[:3], result[3:] - time_step * result[:3])


def solution(mesh):
    spec = P(None, "gx", "gy", None)
    exchange = Exchange(mesh)
    return jax.shard_map(
        functools.partial(per_device, exchange),
        mesh=mesh,
        in_specs=(spec, spec, P("gx", "gy"), spec, spec),
        out_specs=(spec, spec),
        check_vma=False,
    )
```

```python
import functools

import jax
import jax.numpy as jnp
from jax import lax
from jax.experimental import pallas as pl
from jax.experimental.pallas import tpu as pltpu
from jax.sharding import PartitionSpec as P

STEPS = 4
time_step = 0.05
stiffness = 4.0
rest_density = 1.0
particle_mass = 0.15
viscosity = 0.5


FAR = 1.0e4
WALL = 1.0e5
ROWS = 16
LANES = 128
FEATS = 8
LANE_BITS = LANES.bit_length() - 1
VMEM_LIMIT = 12 << 20
BLOCKS = 32
PAD = 4
MERGE = 4
REACH = 1.001
NEVER = 1.0e30


def ring_order(count):
    evens = list(range(0, count, 2))
    odds = list(range(1, count, 2))
    return evens + odds[::-1]


class Exchange:
    def __init__(self, mesh):
        self.count_x = mesh.shape["gx"]
        self.count_y = mesh.shape["gy"]
        self.order = ring_order(self.count_x)

    def permute(self, value, pairs):
        return lax.ppermute(value, ("gx", "gy"), pairs)

    def from_x(self, value, step):
        order, count = self.order, self.count_x
        pairs = [
            (order[(slot + step) % count] * self.count_y + b, order[slot] * self.count_y + b)
            for slot in range(count)
            for b in range(self.count_y)
        ]
        return self.permute(value, pairs)

    def from_y(self, value, step):
        pairs = [
            (a * self.count_y + (b + step) % self.count_y, a * self.count_y + b)
            for a in range(self.count_x)
            for b in range(self.count_y)
        ]
        return self.permute(value, pairs)

    def place(self, value):
        pairs = [
            (a * self.count_y + b, self.order[a] * self.count_y + b)
            for a in range(self.count_x)
            for b in range(self.count_y)
        ]
        return self.permute(value, pairs)

    def unplace(self, value):
        pairs = [
            (self.order[a] * self.count_y + b, a * self.count_y + b)
            for a in range(self.count_x)
            for b in range(self.count_y)
        ]
        return self.permute(value, pairs)

    def halo(self, own, beside=None):
        x_low = self.from_x(own[1:2], -1)
        x_high = self.from_x(own[0:1], 1)
        if beside is not None:
            x_low, x_high, beside = lax.optimization_barrier((x_low, x_high, beside))
        upper = jnp.concatenate([x_low[:, 1:2], own[:, 1:2], x_high[:, 1:2]], axis=0)
        lower = jnp.concatenate([x_low[:, 0:1], own[:, 0:1], x_high[:, 0:1]], axis=0)
        y_low = self.from_y(upper, -1)
        y_high = self.from_y(lower, 1)
        pieces = (own, x_low, x_high, y_low, y_high)
        return pieces if beside is None else (pieces, beside)


def region_tile(pieces, rx, ry):
    own, x_low, x_high, y_low, y_high = pieces
    if ry == 0:
        return y_low[rx, 0]
    if ry == 3:
        return y_high[rx, 0]
    if rx == 0:
        return x_low[0, ry - 1]
    if rx == 3:
        return x_high[0, ry - 1]
    return own[rx - 1, ry - 1]


def fill_region(region, pieces, pack, wall_ref=None):
    kept = FEATS // pack
    row = lax.broadcasted_iota(jnp.int32, (FEATS, 2 * LANES), 0)
    for rx in range(4):
        for ry in range(4):
            block = region_tile(pieces, rx, ry)
            if wall_ref is not None:
                if rx in (0, 3):
                    block = jnp.where(row == 0, block + (-2.0 if rx == 0 else 2.0), block)
                if ry in (0, 3):
                    block = jnp.where(row == 1, block + wall_ref[0 if ry == 0 else 1], block)
            for lb in range(2):
                at = (rx * 4 + ry) * 2 + lb
                inside = (at % pack) * kept
                region[at // pack, inside : inside + kept] = block[
                    :kept, lb * LANES : (lb + 1) * LANES
                ]


def each_tile(work, tiles=4, unroll=False):
    if unroll:
        for t in range(tiles):
            work(t, t // 2, t % 2)
        return

    def step(t, carry):
        work(t, t // 2, t - 2 * (t // 2))
        return carry

    lax.fori_loop(0, tiles, step, 0)


def spread_columns(columns, t, values):
    at = 0
    for block, chosen in values:
        padded = jnp.concatenate(
            [block, jnp.zeros((LANES - FEATS, 2 * LANES), jnp.float32)], axis=0
        )
        turned = padded.T
        for index, feature in enumerate(chosen):
            columns[at + index, t] = jnp.broadcast_to(
                turned[:, feature : feature + 1], (2 * LANES, LANES)
            )
        at += len(chosen)


def take_lanes(sources, row, pack=1):
    shape = (FEATS, LANES)
    lane = jnp.broadcast_to(row & (LANES - 1), shape)
    block = jnp.broadcast_to(row >> LANE_BITS, shape)
    vector = block // pack if pack > 1 else block
    picked = jnp.zeros(shape, jnp.float32)
    for at, source in enumerate(sources):
        picked = jnp.where(vector == at, jnp.take_along_axis(source, lane, axis=1), picked)
    if pack == 1:
        return picked
    inside = block & (pack - 1)
    result = picked
    for at in range(1, pack):
        shifted = pltpu.roll(picked, FEATS - at * (FEATS // pack), 0)
        result = jnp.where(inside == at, shifted, result)
    return result


def merge_region(merged, region, order_ref, counts_ref, pack):
    for at in range(BLOCKS + PAD):
        merged[at] = jnp.zeros((FEATS, LANES), jnp.float32)
    used = (counts_ref[4] + (LANES - 1)) >> LANE_BITS

    def step(index, carry):
        for near in range(MERGE):
            at = index * MERGE + near
            sources = [region[s] for s in range(BLOCKS // pack)]
            merged[at] = take_lanes(sources, order_ref[at], pack)
        return carry

    lax.fori_loop(0, (used + (MERGE - 1)) // MERGE, step, 0)


def block_ranges(ranges, merged, own, counts_ref):
    depth = merged[:BLOCKS, 2, :]
    rank = lax.broadcasted_iota(jnp.int32, (BLOCKS, LANES), 0) * LANES
    rank = rank + lax.broadcasted_iota(jnp.int32, (BLOCKS, LANES), 1)
    held = rank < counts_ref[4]
    least = jnp.min(jnp.where(held, depth, WALL), axis=1, keepdims=True)
    most = jnp.max(jnp.where(held, depth, -WALL), axis=1, keepdims=True)
    rows, limits = [], []
    for t in range(4):
        for lb in range(2):
            rows.append(own[t // 2, t % 2][2:3, lb * LANES : (lb + 1) * LANES])
            lane = lax.broadcasted_iota(jnp.int32, (1, LANES), 1) + lb * LANES
            limits.append((lane < counts_ref[t]).astype(jnp.float32))
    mine = jnp.concatenate(rows, axis=0)
    inside = jnp.concatenate(limits, axis=0) > 0.5
    low = jnp.where(inside, mine, WALL)
    high = jnp.where(inside, mine, -WALL)
    reach = 1
    while reach < ROWS:
        low = jnp.minimum(low, pltpu.roll(low, LANES - reach, 1))
        high = jnp.maximum(high, pltpu.roll(high, LANES - reach, 1))
        reach *= 2
    low = low - REACH
    high = high + REACH
    first = jnp.full((FEATS, LANES), BLOCKS, jnp.int32)
    past = jnp.zeros((FEATS, LANES), jnp.int32)
    for at in range(BLOCKS):
        near = (jnp.broadcast_to(most[at : at + 1], (FEATS, LANES)) >= low) & (
            jnp.broadcast_to(least[at : at + 1], (FEATS, LANES)) <= high
        )
        first = jnp.where(near, jnp.minimum(first, at), first)
        past = jnp.where(near, at + 1, past)
    ranges[0] = first
    ranges[1] = jnp.maximum(past - first, 0)


def pair_sums(counts_ref, range_ref, columns, sums_ref, outputs, together, body, tiles=(0, 4)):
    row_bits = ROWS.bit_length() - 1
    line_bits = LANE_BITS - row_bits

    def tile_loop(t, carry):
        groups = (counts_ref[t] + (ROWS - 1)) >> row_bits

        def group_loop(g, carry):
            start = pl.multiple_of(g << row_bits, ROWS)
            terms_of = body([ref[f, t, pl.ds(start, ROWS), :] for ref, f in columns], t)
            line = (t << 1) + (g >> line_bits)
            lane = (g & ((1 << line_bits) - 1)) << row_bits
            first = range_ref[0, line, lane]
            length = jnp.minimum(range_ref[1, line, lane], BLOCKS - first)
            trips = (length + (together - 1)) // together

            def block_loop(index, totals):
                totals = list(totals)
                for near in range(together):
                    terms = terms_of(first + index * together + near)
                    totals = [a + b for a, b in zip(totals, terms)]
                return tuple(totals)

            zero = jnp.zeros((ROWS, LANES), jnp.float32)
            totals = lax.fori_loop(0, trips, block_loop, (zero,) * outputs)
            for index, total in enumerate(totals):
                sums_ref[index, t - tiles[0], pl.ds(start, ROWS), :] = total
            return carry

        return lax.fori_loop(0, groups, group_loop, carry)

    lax.fori_loop(*tiles, tile_loop, 0)


def row_sums(sums_ref, t, outputs):
    return [jnp.sum(sums_ref[index, t].T, axis=0, keepdims=True) for index in range(outputs)]


def separation(xi, merged, bias_ref, t, block):
    d = [merged[block, f : f + 1, :] - xi[f] for f in range(3)]
    bias = bias_ref[t, block]
    q = jnp.maximum(bias - d[0] * d[0] - d[1] * d[1] - d[2] * d[2], 0.0)
    return d, q


def stack_rows(rows):
    width = rows[0].shape[1]
    rows = list(rows) + [jnp.zeros((1, width), jnp.float32)] * (FEATS - len(rows))
    return jnp.concatenate(rows, axis=0)


def sort_kernel(order_ref, packed_ref, out):
    for tx, ty in ((0, 0), (0, 1), (1, 0), (1, 1)):
        for part in range(packed_ref.shape[2] // FEATS):
            value = packed_ref[tx, ty, part * FEATS : (part + 1) * FEATS]
            sources = [value[:, :LANES], value[:, LANES:]]
            halves = [
                take_lanes(sources, order_ref[tx, ty : ty + 1, lb * LANES : (lb + 1) * LANES])
                for lb in range(2)
            ]
            out[tx, ty, part * FEATS : (part + 1) * FEATS] = jnp.concatenate(halves, axis=1)


def merge_kernel(pack, counts_ref, order_ref, *refs):
    pieces, (merged, region) = refs[:5], refs[5:]
    fill_region(region, pieces, pack)
    merge_region(merged, region, order_ref, counts_ref, pack)


def density_kernel(counts_ref, wall_ref, order_ref, bias_ref, *refs):
    pieces = refs[:5]
    out, merged, ranges, columns, region, sums, range_ref, sem = refs[5:]
    fill_region(region, pieces, 1, wall_ref)
    merge_region(merged, region, order_ref, counts_ref, 1)
    block_ranges(ranges, merged, pieces[0], counts_ref)
    copy = pltpu.make_async_copy(ranges, range_ref, sem)
    for t in range(4):
        if t == 2:
            copy.start()
        spread_columns(columns, t, ((pieces[0][t // 2, t % 2], (0, 1, 2)),))
    copy.wait()

    def body(column, t):
        def terms(block):
            d, q = separation(column, merged, bias_ref, t, block)
            return [q * q * q]

        return terms

    own = [(columns, f) for f in range(3)]
    pair_sums(counts_ref, range_ref, own, sums, 1, 4, body)

    def finish(t, tx, ty):
        live = pieces[0][tx, ty][6:7] > 0.5
        density = particle_mass * row_sums(sums, t, 1)[0]
        padded = jnp.where(live, density, 1.0)
        inverse = jnp.where(live, 1.0 / padded, 0.0)
        coefficient = jnp.where(
            live, stiffness * (density / rest_density - 1.0) / (padded * padded), 0.0
        )
        out[tx, ty] = stack_rows([coefficient, inverse])

    each_tile(finish, unroll=True)


def accel_kernel(counts_ref, range_ref, order_ref, bias_ref, merged, places, state, *refs):
    press, (out, merged_p, region, columns, sums) = refs[:5], refs[5:]
    fill_region(region, press, 4)
    merge_region(merged_p, region, order_ref, counts_ref, 4)
    each_tile(
        lambda t, tx, ty: spread_columns(columns, t, ((press[0][tx, ty], (0,)),)), unroll=True
    )

    def body(column, t):
        xi, ci = column[:3], column[3]

        def terms(block):
            d, q = separation(xi, merged, bias_ref, t, block)
            q2 = q * q
            visc = q2 * q * merged_p[block, 1:2, :]
            push = (ci + merged_p[block, 0:1, :]) * q2
            moved = [visc * merged[block, 3 + f : 4 + f, :] for f in range(3)]
            pushed = [push * d[f] for f in range(3)]
            return moved + [visc] + pushed

        return terms

    own = [(places, f) for f in range(3)] + [(columns, 0)]
    pair_sums(counts_ref, range_ref, own, sums, 7, 3, body)

    def finish(t, tx, ty):
        own = state[tx, ty]
        live = own[6:7] > 0.5
        s = row_sums(sums, t, 7)
        new_pos, new_vel = [], []
        for f in range(3):
            vel = own[3 + f : 4 + f]
            accel = particle_mass * (viscosity * (s[f] - vel * s[3]) - 6.0 * s[4 + f])
            vel = jnp.where(live, vel + time_step * accel, vel)
            new_vel.append(vel)
            new_pos.append(
                jnp.where(live, own[f : f + 1] + time_step * vel, own[f : f + 1])
            )
        out[tx, ty] = stack_rows(new_pos + new_vel + [own[6:7]])

    each_tile(finish)


def density_grad_kernel(
    counts_ref, range_ref, order_ref, bias_ref, merged, places, state, press, *refs
):
    lam, (out, merged_l, columns, region, sums) = refs[:5], refs[5:]
    fill_region(region, lam, 2)
    merge_region(merged_l, region, order_ref, counts_ref, 2)
    each_tile(
        lambda t, tx, ty: spread_columns(
            columns, t, ((state[tx, ty], (3, 4, 5)), (lam[0][tx, ty], (0, 1, 2)))
        )
    )

    def body(column, t):
        xi, vi, li = column[:3], column[3:6], column[6:]

        def terms(block):
            d, q = separation(xi, merged, bias_ref, t, block)
            lj = [merged_l[block, f : f + 1, :] for f in range(3)]
            q2 = q * q
            along = sum((li[f] - lj[f]) * d[f] for f in range(3))
            moved = sum(lj[f] * (vi[f] - merged[block, 3 + f : 4 + f, :]) for f in range(3))
            return [q2 * along, q2 * q * moved]

        return terms

    own = [(places, f) for f in range(3)] + [(columns, f) for f in range(6)]
    pair_sums(counts_ref, range_ref, own, sums, 2, 3, body)

    def finish(t, tx, ty):
        live = state[tx, ty][6:7] > 0.5
        s = row_sums(sums, t, 2)
        c = press[tx, ty][0:1]
        w = press[tx, ty][1:2]
        grad_c = (-6.0 * particle_mass) * s[0]
        grad_w = (viscosity * particle_mass) * s[1]
        grad = grad_c * (stiffness * w * w - 2.0 * c * w) - grad_w * w * w
        out[tx, ty] = stack_rows([jnp.where(live, grad, 0.0)])

    each_tile(finish, unroll=True)


def main_grad_kernel(half, counts_ref, range_ref, bias_ref, merged, merged_p, merged_l, *refs):
    places, moves, press, lam, out, columns, sums = refs
    for ty in range(2):
        spread_columns(columns, 2 * half + ty, ((press[half, ty], (0, 1)),))

    def body(column, t):
        xi, vi, li = column[:3], column[3:6], column[6:9]
        ci, wi = column[9:]

        def terms(block):
            d, q = separation(xi, merged, bias_ref, t, block)
            lj = [merged_l[block, f : f + 1, :] for f in range(3)]
            wj = merged_p[block, 1:2, :]
            cs = ci + merged_p[block, 0:1, :]
            diff = [li[f] - lj[f] for f in range(3)]
            dv = [merged[block, 3 + f : 4 + f, :] - vi[f] for f in range(3)]
            along = sum(diff[f] * d[f] for f in range(3))
            drag = wj * sum(li[f] * dv[f] for f in range(3)) - wi * sum(
                lj[f] * dv[f] for f in range(3)
            )
            q2 = q * q
            q3 = q2 * q
            on_d = q * (q * drag - 8.0 * (cs * along))
            on_l = (cs * q2) * 2.0
            gx = [on_d * d[f] + on_l * diff[f] for f in range(3)]
            gv = [q3 * lj[f] for f in range(3)]
            return gx + gv + [q3 * wj]

        return terms

    own = [(places, f) for f in range(3)] + [(moves, f) for f in range(6)]
    own += [(columns, f) for f in range(2)]
    pair_sums(
        counts_ref, range_ref, own, sums, 7, 2, body, tiles=(2 * half, 2 * half + 2)
    )

    def finish(t, tx, ty):
        s = row_sums(sums, t, 7)
        w = press[half, t][1:2]
        rows = [(3.0 * particle_mass) * s[f] for f in range(3)]
        scale = viscosity * particle_mass
        for f in range(3):
            mine = lam[half, t][f : f + 1]
            rows.append(scale * (w * s[3 + f] - mine * s[6]))
        out[0, t] = stack_rows(rows)

    each_tile(finish, tiles=2)


def last_grad_kernel(counts_ref, range_ref, order_ref, bias_ref, merged, places, state, *refs):
    grads, partials, carried = refs[:5], refs[5:7], refs[7]
    lam_out, carried_out, region, merged_g, columns, sums = refs[8:]
    fill_region(region, grads, 8)
    merge_region(merged_g, region, order_ref, counts_ref, 8)
    each_tile(
        lambda t, tx, ty: spread_columns(columns, t, ((grads[0][tx, ty], (0,)),)), unroll=True
    )

    def body(column, t):
        xi, gi = column[:3], column[3]

        def terms(block):
            d, q = separation(xi, merged, bias_ref, t, block)
            weight = (gi + merged_g[block, 0:1, :]) * (q * q)
            return [weight * d[f] for f in range(3)]

        return terms

    own = [(places, f) for f in range(3)] + [(columns, 0)]
    pair_sums(counts_ref, range_ref, own, sums, 3, 4, body)

    def finish(t, tx, ty):
        live = state[tx, ty][6:7] > 0.5
        s = row_sums(sums, t, 3)
        part = partials[tx][0, ty]
        old = carried[tx, ty]
        new_pos, new_vel = [], []
        for f in range(3):
            extra = part[f : f + 1] + (6.0 * particle_mass) * s[f]
            gx = old[f : f + 1] + jnp.where(live, extra, 0.0)
            gv = old[3 + f : 4 + f] + jnp.where(live, part[3 + f : 4 + f], 0.0)
            new_pos.append(gx)
            new_vel.append(gv + time_step * gx)
        lam_out[tx, ty] = stack_rows([jnp.where(live, time_step * v, 0.0) for v in new_vel])
        carried_out[tx, ty] = stack_rows(new_pos + new_vel)

    each_tile(finish, unroll=True)


TILES = jax.ShapeDtypeStruct((2, 2, FEATS, 2 * LANES), jnp.float32)
MERGED = jax.ShapeDtypeStruct((BLOCKS + PAD, FEATS, LANES), jnp.float32)
RANGES = jax.ShapeDtypeStruct((2, FEATS, LANES), jnp.int32)
HALF = jax.ShapeDtypeStruct((1, 2, FEATS, 2 * LANES), jnp.float32)


def wide(count, tiles=4):
    return jax.ShapeDtypeStruct((count, tiles, 2 * LANES, LANES), jnp.float32)


def vmem_like(shape):
    return pltpu.VMEM(shape.shape, shape.dtype)


def packed_region(pack):
    return pltpu.VMEM((BLOCKS // pack, FEATS, LANES), jnp.float32)


def run_kernel(kernel, name, scalars, arrays, out_shape, scratch, cycles):
    smem = pl.BlockSpec(memory_space=pltpu.SMEM)
    vmem = pl.BlockSpec(memory_space=pltpu.VMEM)
    result = pl.pallas_call(
        kernel,
        name=name,
        out_shape=out_shape,
        in_specs=[smem] * len(scalars) + [vmem] * len(arrays),
        out_specs=[vmem] * len(out_shape),
        scratch_shapes=scratch,
        compiler_params=pltpu.CompilerParams(vmem_limit_bytes=VMEM_LIMIT),
        cost_estimate=pl.CostEstimate(
            flops=cycles * 65536, bytes_accessed=1 << 18, transcendentals=0
        ),
    )(*scalars, *arrays)
    return result


def per_device(exchange, positions, velocities, occupancy, cot_positions, cot_velocities):
    slots = positions.shape[3]
    assert positions.shape[1:] == (2, 2, 2 * LANES)
    live = lax.broadcasted_iota(jnp.int32, occupancy.shape + (slots,), 2) < occupancy[:, :, None]
    corner = jnp.stack(
        [
            lax.broadcasted_iota(jnp.float32, live.shape, 0),
            lax.broadcasted_iota(jnp.float32, live.shape, 1),
            jnp.zeros(live.shape, jnp.float32),
        ]
    )
    placed = jnp.where(live[None], positions + corner, FAR)
    mask = live.astype(jnp.float32)[None]
    spare = jnp.zeros_like(mask)
    packed = jnp.concatenate(
        [placed, velocities, mask, spare, cot_positions, cot_velocities, spare, spare], axis=0
    )
    packed = jnp.moveaxis(packed, 0, 2)
    depth_key = jnp.where(live, positions[2], WALL)
    slot = lax.broadcasted_iota(jnp.int32, live.shape, 2)
    by_depth = lax.sort((depth_key, slot), dimension=2, num_keys=1)[1]
    back = lax.sort((by_depth, slot), dimension=2, num_keys=1)[1]
    (packed,) = run_kernel(
        sort_kernel,
        "sort_own",
        (),
        (by_depth, packed),
        [jax.ShapeDtypeStruct(packed.shape, jnp.float32)],
        [],
        500,
    )
    packed = exchange.place(packed)
    state = packed[:, :, :8]
    grads = packed[:, :, 8:14]
    n_own = jnp.sum(state[:, :, 6], axis=-1).astype(jnp.int32).reshape(4)
    at_y = lax.axis_index("gy")
    at_low = at_y == 0
    at_high = at_y == exchange.count_y - 1
    walls = jnp.stack([jnp.where(at_low, -WALL, -2.0), jnp.where(at_high, WALL, 2.0)])
    walls = walls.astype(jnp.float32)

    grad_pos, grad_vel = grads[:, :, :3], grads[:, :, 3:]
    grad_vel = grad_vel + time_step * grad_pos
    pad2 = jnp.zeros((2, 2, 2, slots), jnp.float32)
    carried = jnp.concatenate([grad_pos, grad_vel, pad2], axis=2)
    lam = jnp.concatenate(
        [time_step * state[:, :, 6:7] * grad_vel, jnp.zeros((2, 2, 5, slots), jnp.float32)], axis=2
    )

    pieces = exchange.halo(state)
    own, x_low, x_high, y_low, y_high = pieces
    around = jnp.concatenate([x_low, own, x_high], axis=0)
    around = jnp.concatenate([y_low, around, y_high], axis=1)
    row_y = lax.broadcasted_iota(jnp.int32, (4, 4, slots), 1)
    beyond = ((row_y == 0) & at_low) | ((row_y == 3) & at_high)
    present = (around[:, :, 6] > 0.5) & ~beyond
    key = jnp.where(present, around[:, :, 2], WALL).reshape(-1)
    place = lax.broadcasted_iota(jnp.int32, key.shape, 0)
    order = lax.sort((key, place), dimension=0, num_keys=1)[1]
    total = jnp.sum(present.astype(jnp.int32))
    counts = jnp.concatenate([n_own, total[None]])
    tile_x = order // (4 * slots)
    tile_y = (order // slots) % 4
    bias = []
    for t in range(4):
        by_x = (tile_x >= t // 2) & (tile_x <= t // 2 + 2)
        by_y = (tile_y >= t % 2) & (tile_y <= t % 2 + 2)
        bias.append(jnp.where(by_x & by_y & (place < total), 1.0, -NEVER))
    bias = jnp.stack(bias).reshape(4, BLOCKS, 1, LANES)
    bias = jnp.pad(bias, ((0, 0), (0, PAD), (0, 0), (0, 0)), constant_values=-NEVER)
    order = order.reshape(BLOCKS, 1, LANES)

    saved = []
    for step in range(STEPS):
        if step > 0:
            pieces = exchange.halo(state)
        own_press, merged, ranges, places = run_kernel(
            density_kernel,
            "density",
            (counts, walls),
            (order, bias) + pieces,
            [TILES, MERGED, RANGES, wide(3)],
            [
                packed_region(1),
                vmem_like(wide(1)),
                pltpu.SMEM(RANGES.shape, jnp.int32),
                pltpu.SemaphoreType.DMA,
            ],
            8000,
        )
        press = exchange.halo(own_press)
        if step + 1 < STEPS:
            new_state, merged_p = run_kernel(
                accel_kernel,
                "accel",
                (counts, ranges),
                (order, bias, merged, places, state) + press,
                [TILES, MERGED],
                [packed_region(4), vmem_like(wide(1)), vmem_like(wide(7))],
                10000,
            )
        else:
            new_state = state
            (merged_p,) = run_kernel(
                functools.partial(merge_kernel, 4),
                "merge",
                (counts,),
                (order,) + press,
                [MERGED],
                [packed_region(4)],
                2000,
            )
        saved.append((state, own_press, ranges, merged, merged_p, places))
        state = new_state

    for step in reversed(range(STEPS)):
        state, own_press, ranges, merged, merged_p, places = saved[step]
        lam_pieces = exchange.halo(lam)
        own_grad, merged_l, moves = run_kernel(
            density_grad_kernel,
            "density_grad",
            (counts, ranges),
            (order, bias, merged, places, state, own_press) + lam_pieces,
            [TILES, MERGED, wide(6)],
            [packed_region(2), vmem_like(wide(2))],
            10000,
        )
        halves = [
            run_kernel(
                functools.partial(main_grad_kernel, half),
                "main_grad_%d" % half,
                (counts, ranges),
                (bias, merged, merged_p, merged_l, places, moves, own_press, lam),
                [HALF],
                [vmem_like(wide(2)), vmem_like(wide(7, 2))],
                10000,
            )[0]
            for half in range(2)
        ]
        if step == 0:
            halves[0], back = lax.optimization_barrier((halves[0], back))
        grad_pieces, halves[0] = exchange.halo(own_grad, beside=halves[0])
        lam, carried = run_kernel(
            last_grad_kernel,
            "last_grad",
            (counts, ranges),
            (order, bias, merged, places, state) + grad_pieces + tuple(halves) + (carried,),
            [TILES, TILES],
            [packed_region(8), vmem_like(MERGED), vmem_like(wide(1)), vmem_like(wide(3))],
            8000,
        )

    result = exchange.unplace(carried)
    (result,) = run_kernel(sort_kernel, "unsort_own", (), (back, result), [TILES], [], 500)
    result = jnp.moveaxis(result[:, :, :6], 2, 0)
    return (result[:3], result[3:] - time_step * result[:3])


def solution(mesh):
    spec = P(None, "gx", "gy", None)
    exchange = Exchange(mesh)
    return jax.shard_map(
        functools.partial(per_device, exchange),
        mesh=mesh,
        in_specs=(spec, spec, P("gx", "gy"), spec, spec),
        out_specs=(spec, spec),
        check_vma=False,
    )
```

```python
import functools

import jax
import jax.numpy as jnp
from jax import lax
from jax.experimental import pallas as pl
from jax.experimental.pallas import tpu as pltpu
from jax.sharding import PartitionSpec as P

STEPS = 4
time_step = 0.05
stiffness = 4.0
rest_density = 1.0
particle_mass = 0.15
viscosity = 0.5


FAR = 1.0e4
BEYOND = 1.0e5
ROWS = 16
LANES = 128
FEATS = 8
LANE_BITS = LANES.bit_length() - 1
PRESS_ROWS = 2
LAM_ROWS = 4
VMEM_LIMIT = 12 << 20
BLOCKS = 30
PAD = 4
MERGE = 4
REACH = 1.001
NEVER = 1.0e30


def path_order(count):
    evens = list(range(0, count, 2))
    odds = list(range(1, count, 2))
    return evens + odds[::-1]


class Exchange:
    def __init__(self, mesh):
        self.count_x = mesh.shape["gx"]
        self.count_y = mesh.shape["gy"]
        assert self.count_y == 4
        path = path_order(self.count_x)
        self.ring = [(a, 0) for a in path] + [(a, 1) for a in path[::-1]]
        column_of = {}
        for column in range(len(self.ring)):
            for half in range(2):
                column_of[self.device(column, half)] = column
        self.odd = [column_of[d] % 2 for d in range(self.count_x * self.count_y)]

    def device(self, column, half):
        a, line = self.ring[column % len(self.ring)]
        return a * self.count_y + line * 2 + half

    def permute(self, value, pairs):
        return lax.ppermute(value, ("gx", "gy"), pairs)

    def at_odd(self):
        flat = lax.axis_index("gx") * self.count_y + lax.axis_index("gy")
        return jnp.array(self.odd, jnp.int32)[flat] == 1

    def at_low(self):
        return lax.axis_index("gy") % 2 == 0

    def from_ring(self, value, step):
        pairs = [
            (self.device(column + step, half), self.device(column, half))
            for column in range(len(self.ring))
            for half in range(2)
        ]
        return self.permute(value, pairs)

    def from_other_half(self, value):
        pairs = [
            (self.device(column, 1 - half), self.device(column, half))
            for column in range(len(self.ring))
            for half in range(2)
        ]
        return self.permute(value, pairs)

    def routes(self, flip):
        return [
            (a * self.count_y + b, self.device(2 * a + (b + flip) % 2, b // 2))
            for a in range(self.count_x)
            for b in range(self.count_y)
        ]

    def place(self, blocks):
        odd_b = lax.axis_index("gy") % 2 == 1
        parts = [
            self.permute(jnp.where(odd_b, blocks[1 - flip], blocks[flip]), self.routes(flip))
            for flip in range(2)
        ]
        odd = self.at_odd()
        lower = jnp.where(odd, parts[1], parts[0])
        upper = jnp.where(odd, parts[0], parts[1])
        return jnp.concatenate([lower, upper], axis=0)

    def unplace(self, tiles):
        odd = self.at_odd()
        lower, upper = tiles[:2], tiles[2:]
        parts = [
            self.permute(
                jnp.where(odd, upper, lower) if flip == 0 else jnp.where(odd, lower, upper),
                [(target, source) for source, target in self.routes(flip)],
            )
            for flip in range(2)
        ]
        odd_b = lax.axis_index("gy") % 2 == 1
        return jnp.stack(
            [jnp.where(odd_b, parts[1], parts[0]), jnp.where(odd_b, parts[0], parts[1])]
        )

    def halo(self, own, beside=None):
        x_low = self.from_ring(own, -1)
        x_high = self.from_ring(own, 1)
        if beside is not None:
            x_low, x_high, beside = lax.optimization_barrier((x_low, x_high, beside))
        at_low = self.at_low()
        edges = jnp.stack([jnp.where(at_low, part[3], part[0]) for part in (x_low, own, x_high)])
        pieces = (own, x_low, x_high, self.from_other_half(edges))
        return pieces if beside is None else (pieces, beside)


def fill_region(region, pieces, pack, shift_ref=None):
    own, x_low, x_high, far = pieces
    kept = FEATS // pack
    row = lax.broadcasted_iota(jnp.int32, (FEATS, 2 * LANES), 0)
    for rx in range(3):
        for ry in range(5):
            block = far[rx] if ry == 4 else (x_low, own, x_high)[rx][ry]
            if shift_ref is not None:
                if rx != 1:
                    block = jnp.where(row == 0, block + (rx - 1.0), block)
                if ry == 4:
                    block = jnp.where(row == 1, block + shift_ref[0], block)
            for lb in range(2):
                at = (rx * 5 + ry) * 2 + lb
                inside = (at % pack) * kept
                region[at // pack, inside : inside + kept] = block[
                    :kept, lb * LANES : (lb + 1) * LANES
                ]


def each_tile(work, tiles=4, unroll=False):
    if unroll:
        for t in range(tiles):
            work(t)
        return

    def step(t, carry):
        work(t)
        return carry

    lax.fori_loop(0, tiles, step, 0)


def spread_columns(columns, t, values):
    at = 0
    for block, chosen in values:
        padded = jnp.concatenate(
            [block, jnp.zeros((LANES - block.shape[0], 2 * LANES), jnp.float32)], axis=0
        )
        turned = padded.T
        for index, feature in enumerate(chosen):
            columns[at + index, t] = jnp.broadcast_to(
                turned[:, feature : feature + 1], (2 * LANES, LANES)
            )
        at += len(chosen)


def take_lanes(sources, row, pack=1):
    shape = (FEATS, LANES)
    lane = jnp.broadcast_to(row & (LANES - 1), shape)
    block = jnp.broadcast_to(row >> LANE_BITS, shape)
    vector = block // pack if pack > 1 else block
    picked = jnp.zeros(shape, jnp.float32)
    for at, source in enumerate(sources):
        picked = jnp.where(vector == at, jnp.take_along_axis(source, lane, axis=1), picked)
    if pack == 1:
        return picked
    inside = block & (pack - 1)
    result = picked
    for at in range(1, pack):
        shifted = pltpu.roll(picked, FEATS - at * (FEATS // pack), 0)
        result = jnp.where(inside == at, shifted, result)
    return result


def merge_region(merged, region, order_ref, counts_ref, pack):
    for at in range(BLOCKS + PAD):
        merged[at] = jnp.zeros((FEATS, LANES), jnp.float32)
    used = (counts_ref[4] + (LANES - 1)) >> LANE_BITS

    def step(index, carry):
        for near in range(MERGE):
            at = index * MERGE + near
            sources = [region[s] for s in range(-(-BLOCKS // pack))]
            merged[at] = take_lanes(sources, order_ref[at], pack)
        return carry

    lax.fori_loop(0, (used + (MERGE - 1)) // MERGE, step, 0)


def block_ranges(ranges, merged, own, counts_ref):
    depth = merged[:BLOCKS, 2, :]
    rank = lax.broadcasted_iota(jnp.int32, (BLOCKS, LANES), 0) * LANES
    rank = rank + lax.broadcasted_iota(jnp.int32, (BLOCKS, LANES), 1)
    held = rank < counts_ref[4]
    least = jnp.min(jnp.where(held, depth, BEYOND), axis=1, keepdims=True)
    most = jnp.max(jnp.where(held, depth, -BEYOND), axis=1, keepdims=True)
    rows, limits = [], []
    for t in range(4):
        for lb in range(2):
            rows.append(own[t][2:3, lb * LANES : (lb + 1) * LANES])
            lane = lax.broadcasted_iota(jnp.int32, (1, LANES), 1) + lb * LANES
            limits.append((lane < counts_ref[t]).astype(jnp.float32))
    mine = jnp.concatenate(rows, axis=0)
    inside = jnp.concatenate(limits, axis=0) > 0.5
    low = jnp.where(inside, mine, BEYOND)
    high = jnp.where(inside, mine, -BEYOND)
    reach = 1
    while reach < ROWS:
        low = jnp.minimum(low, pltpu.roll(low, LANES - reach, 1))
        high = jnp.maximum(high, pltpu.roll(high, LANES - reach, 1))
        reach *= 2
    low = low - REACH
    high = high + REACH
    first = jnp.full((FEATS, LANES), BLOCKS, jnp.int32)
    past = jnp.zeros((FEATS, LANES), jnp.int32)
    for at in range(BLOCKS):
        near = (jnp.broadcast_to(most[at : at + 1], (FEATS, LANES)) >= low) & (
            jnp.broadcast_to(least[at : at + 1], (FEATS, LANES)) <= high
        )
        first = jnp.where(near, jnp.minimum(first, at), first)
        past = jnp.where(near, at + 1, past)
    ranges[0] = first
    ranges[1] = jnp.maximum(past - first, 0)


def pair_sums(counts_ref, range_ref, columns, sums_ref, outputs, together, body, tiles=(0, 4)):
    row_bits = ROWS.bit_length() - 1
    line_bits = LANE_BITS - row_bits

    def tile_loop(t, carry):
        groups = (counts_ref[t] + (ROWS - 1)) >> row_bits

        def group_loop(g, carry):
            start = pl.multiple_of(g << row_bits, ROWS)
            terms_of = body([ref[f, t, pl.ds(start, ROWS), :] for ref, f in columns], t)
            line = (t << 1) + (g >> line_bits)
            lane = (g & ((1 << line_bits) - 1)) << row_bits
            first = range_ref[0, line, lane]
            length = jnp.minimum(range_ref[1, line, lane], BLOCKS - first)
            trips = (length + (together - 1)) // together

            def block_loop(index, totals):
                totals = list(totals)
                for near in range(together):
                    terms = terms_of(first + index * together + near)
                    totals = [a + b for a, b in zip(totals, terms)]
                return tuple(totals)

            zero = jnp.zeros((ROWS, LANES), jnp.float32)
            totals = lax.fori_loop(0, trips, block_loop, (zero,) * outputs)
            for index, total in enumerate(totals):
                sums_ref[index, t - tiles[0], pl.ds(start, ROWS), :] = total
            return carry

        return lax.fori_loop(0, groups, group_loop, carry)

    lax.fori_loop(*tiles, tile_loop, 0)


def row_sums(sums_ref, t, outputs):
    return [jnp.sum(sums_ref[index, t].T, axis=0, keepdims=True) for index in range(outputs)]


def separation(xi, merged, bias_ref, t, block):
    d = [merged[block, f : f + 1, :] - xi[f] for f in range(3)]
    bias = bias_ref[t, block]
    q = jnp.maximum(bias - d[0] * d[0] - d[1] * d[1] - d[2] * d[2], 0.0)
    return d, q


def stack_rows(rows, height=FEATS):
    width = rows[0].shape[1]
    rows = list(rows) + [jnp.zeros((1, width), jnp.float32)] * (height - len(rows))
    return jnp.concatenate(rows, axis=0)


def sort_kernel(order_ref, packed_ref, out):
    for tx, ty in ((0, 0), (0, 1), (1, 0), (1, 1)):
        for part in range(packed_ref.shape[2] // FEATS):
            value = packed_ref[tx, ty, part * FEATS : (part + 1) * FEATS]
            sources = [value[:, :LANES], value[:, LANES:]]
            halves = [
                take_lanes(sources, order_ref[tx, ty : ty + 1, lb * LANES : (lb + 1) * LANES])
                for lb in range(2)
            ]
            out[tx, ty, part * FEATS : (part + 1) * FEATS] = jnp.concatenate(halves, axis=1)


def merge_kernel(pack, counts_ref, order_ref, *refs):
    pieces, (merged, region) = refs[:4], refs[4:]
    fill_region(region, pieces, pack)
    merge_region(merged, region, order_ref, counts_ref, pack)


def density_kernel(counts_ref, shift_ref, order_ref, bias_ref, *refs):
    pieces = refs[:4]
    out, merged, ranges, columns, region, sums, range_ref, sem = refs[4:]
    fill_region(region, pieces, 1, shift_ref)
    merge_region(merged, region, order_ref, counts_ref, 1)
    block_ranges(ranges, merged, pieces[0], counts_ref)
    copy = pltpu.make_async_copy(ranges, range_ref, sem)
    for t in range(4):
        if t == 2:
            copy.start()
        spread_columns(columns, t, ((pieces[0][t], (0, 1, 2)),))
    copy.wait()

    def body(column, t):
        def terms(block):
            d, q = separation(column, merged, bias_ref, t, block)
            return [q * q * q]

        return terms

    own = [(columns, f) for f in range(3)]
    pair_sums(counts_ref, range_ref, own, sums, 1, 4, body)

    def finish(t):
        live = pieces[0][t][6:7] > 0.5
        density = particle_mass * row_sums(sums, t, 1)[0]
        padded = jnp.where(live, density, 1.0)
        inverse = jnp.where(live, 1.0 / padded, 0.0)
        coefficient = jnp.where(
            live, stiffness * (density / rest_density - 1.0) / (padded * padded), 0.0
        )
        out[t] = stack_rows([coefficient, inverse], PRESS_ROWS)

    each_tile(finish, unroll=True)


def accel_kernel(counts_ref, range_ref, order_ref, bias_ref, merged, places, state, *refs):
    press, (out, merged_p, region, columns, sums) = refs[:4], refs[4:]
    fill_region(region, press, 4)
    merge_region(merged_p, region, order_ref, counts_ref, 4)
    each_tile(
        lambda t: spread_columns(columns, t, ((press[0][t], (0,)),)), unroll=True
    )

    def body(column, t):
        xi, ci = column[:3], column[3]

        def terms(block):
            d, q = separation(xi, merged, bias_ref, t, block)
            q2 = q * q
            visc = q2 * q * merged_p[block, 1:2, :]
            push = (ci + merged_p[block, 0:1, :]) * q2
            moved = [visc * merged[block, 3 + f : 4 + f, :] for f in range(3)]
            pushed = [push * d[f] for f in range(3)]
            return moved + [visc] + pushed

        return terms

    own = [(places, f) for f in range(3)] + [(columns, 0)]
    pair_sums(counts_ref, range_ref, own, sums, 7, 3, body)

    def finish(t):
        own = state[t]
        live = own[6:7] > 0.5
        s = row_sums(sums, t, 7)
        new_pos, new_vel = [], []
        for f in range(3):
            vel = own[3 + f : 4 + f]
            accel = particle_mass * (viscosity * (s[f] - vel * s[3]) - 6.0 * s[4 + f])
            vel = jnp.where(live, vel + time_step * accel, vel)
            new_vel.append(vel)
            new_pos.append(
                jnp.where(live, own[f : f + 1] + time_step * vel, own[f : f + 1])
            )
        out[t] = stack_rows(new_pos + new_vel + [own[6:7]])

    each_tile(finish)


def density_grad_kernel(
    counts_ref, range_ref, order_ref, bias_ref, merged, places, state, press, *refs
):
    lam, (out, merged_l, columns, region, sums) = refs[:4], refs[4:]
    fill_region(region, lam, 2)
    merge_region(merged_l, region, order_ref, counts_ref, 2)
    each_tile(
        lambda t: spread_columns(columns, t, ((state[t], (3, 4, 5)), (lam[0][t], (0, 1, 2))))
    )

    def body(column, t):
        xi, vi, li = column[:3], column[3:6], column[6:]

        def terms(block):
            d, q = separation(xi, merged, bias_ref, t, block)
            lj = [merged_l[block, f : f + 1, :] for f in range(3)]
            q2 = q * q
            along = sum((li[f] - lj[f]) * d[f] for f in range(3))
            moved = sum(lj[f] * (vi[f] - merged[block, 3 + f : 4 + f, :]) for f in range(3))
            return [q2 * along, q2 * q * moved]

        return terms

    own = [(places, f) for f in range(3)] + [(columns, f) for f in range(6)]
    pair_sums(counts_ref, range_ref, own, sums, 2, 3, body)

    def finish(t):
        live = state[t][6:7] > 0.5
        s = row_sums(sums, t, 2)
        c = press[t][0:1]
        w = press[t][1:2]
        grad_c = (-6.0 * particle_mass) * s[0]
        grad_w = (viscosity * particle_mass) * s[1]
        grad = grad_c * (stiffness * w * w - 2.0 * c * w) - grad_w * w * w
        out[t] = jnp.where(live, grad, 0.0)

    each_tile(finish, unroll=True)


def main_grad_kernel(half, counts_ref, range_ref, bias_ref, merged, merged_p, merged_l, *refs):
    places, moves, press, lam, out, columns, sums = refs
    for t in range(2 * half, 2 * half + 2):
        spread_columns(columns, t, ((press[t], (0, 1)),))

    def body(column, t):
        xi, vi, li = column[:3], column[3:6], column[6:9]
        ci, wi = column[9:]

        def terms(block):
            d, q = separation(xi, merged, bias_ref, t, block)
            lj = [merged_l[block, f : f + 1, :] for f in range(3)]
            wj = merged_p[block, 1:2, :]
            cs = ci + merged_p[block, 0:1, :]
            diff = [li[f] - lj[f] for f in range(3)]
            dv = [merged[block, 3 + f : 4 + f, :] - vi[f] for f in range(3)]
            along = sum(diff[f] * d[f] for f in range(3))
            drag = wj * sum(li[f] * dv[f] for f in range(3)) - wi * sum(
                lj[f] * dv[f] for f in range(3)
            )
            q2 = q * q
            q3 = q2 * q
            on_d = q * (q * drag - 8.0 * (cs * along))
            on_l = (cs * q2) * 2.0
            gx = [on_d * d[f] + on_l * diff[f] for f in range(3)]
            gv = [q3 * lj[f] for f in range(3)]
            return gx + gv + [q3 * wj]

        return terms

    own = [(places, f) for f in range(3)] + [(moves, f) for f in range(6)]
    own += [(columns, f) for f in range(2)]
    pair_sums(
        counts_ref, range_ref, own, sums, 7, 2, body, tiles=(2 * half, 2 * half + 2)
    )

    def finish(t):
        s = row_sums(sums, t, 7)
        w = press[2 * half + t][1:2]
        rows = [(3.0 * particle_mass) * s[f] for f in range(3)]
        scale = viscosity * particle_mass
        for f in range(3):
            mine = lam[2 * half + t][f : f + 1]
            rows.append(scale * (w * s[3 + f] - mine * s[6]))
        out[t] = stack_rows(rows)

    each_tile(finish, tiles=2)


def last_grad_kernel(counts_ref, range_ref, order_ref, bias_ref, merged, places, state, *refs):
    grads, partials, carried = refs[:4], refs[4:6], refs[6]
    lam_out, carried_out, region, merged_g, columns, sums = refs[7:]
    fill_region(region, grads, 8)
    merge_region(merged_g, region, order_ref, counts_ref, 8)
    each_tile(
        lambda t: spread_columns(columns, t, ((grads[0][t], (0,)),)), unroll=True
    )

    def body(column, t):
        xi, gi = column[:3], column[3]

        def terms(block):
            d, q = separation(xi, merged, bias_ref, t, block)
            weight = (gi + merged_g[block, 0:1, :]) * (q * q)
            return [weight * d[f] for f in range(3)]

        return terms

    own = [(places, f) for f in range(3)] + [(columns, 0)]
    pair_sums(counts_ref, range_ref, own, sums, 3, 4, body)

    def finish(t):
        live = state[t][6:7] > 0.5
        s = row_sums(sums, t, 3)
        part = partials[t // 2][t % 2]
        old = carried[t]
        new_pos, new_vel = [], []
        for f in range(3):
            extra = part[f : f + 1] + (6.0 * particle_mass) * s[f]
            gx = old[f : f + 1] + jnp.where(live, extra, 0.0)
            gv = old[3 + f : 4 + f] + jnp.where(live, part[3 + f : 4 + f], 0.0)
            new_pos.append(gx)
            new_vel.append(gv + time_step * gx)
        lam_out[t] = stack_rows([jnp.where(live, time_step * v, 0.0) for v in new_vel], LAM_ROWS)
        carried_out[t] = stack_rows(new_pos + new_vel)

    each_tile(finish, unroll=True)


def tiles_of(rows, tiles=4):
    return jax.ShapeDtypeStruct((tiles, rows, 2 * LANES), jnp.float32)


TILES = tiles_of(FEATS)
MERGED = jax.ShapeDtypeStruct((BLOCKS + PAD, FEATS, LANES), jnp.float32)
RANGES = jax.ShapeDtypeStruct((2, FEATS, LANES), jnp.int32)


def wide(count, tiles=4):
    return jax.ShapeDtypeStruct((count, tiles, 2 * LANES, LANES), jnp.float32)


def vmem_like(shape):
    return pltpu.VMEM(shape.shape, shape.dtype)


def packed_region(pack):
    return pltpu.VMEM((-(-BLOCKS // pack), FEATS, LANES), jnp.float32)


def run_kernel(kernel, name, scalars, arrays, out_shape, scratch, cycles):
    smem = pl.BlockSpec(memory_space=pltpu.SMEM)
    vmem = pl.BlockSpec(memory_space=pltpu.VMEM)
    result = pl.pallas_call(
        kernel,
        name=name,
        out_shape=out_shape,
        in_specs=[smem] * len(scalars) + [vmem] * len(arrays),
        out_specs=[vmem] * len(out_shape),
        scratch_shapes=scratch,
        compiler_params=pltpu.CompilerParams(vmem_limit_bytes=VMEM_LIMIT),
        cost_estimate=pl.CostEstimate(
            flops=cycles * 65536, bytes_accessed=1 << 18, transcendentals=0
        ),
    )(*scalars, *arrays)
    return result


def per_device(exchange, positions, velocities, occupancy, cot_positions, cot_velocities):
    slots = positions.shape[3]
    assert positions.shape[1:] == (2, 2, 2 * LANES)
    live = lax.broadcasted_iota(jnp.int32, occupancy.shape + (slots,), 2) < occupancy[:, :, None]
    placed = jnp.where(live[None], positions, FAR)
    mask = live.astype(jnp.float32)[None]
    spare = jnp.zeros_like(mask)
    packed = jnp.concatenate(
        [placed, velocities, mask, spare, cot_positions, cot_velocities, spare, spare], axis=0
    )
    packed = jnp.moveaxis(packed, 0, 2)
    depth_key = jnp.where(live, positions[2], BEYOND)
    slot = lax.broadcasted_iota(jnp.int32, live.shape, 2)
    by_depth = lax.sort((depth_key, slot), dimension=2, num_keys=1)[1]
    back = lax.sort((by_depth, slot), dimension=2, num_keys=1)[1]
    (packed,) = run_kernel(
        sort_kernel,
        "sort_own",
        (),
        (by_depth, packed),
        [jax.ShapeDtypeStruct(packed.shape, jnp.float32)],
        [],
        500,
    )
    packed = exchange.place(packed)
    row_y = lax.broadcasted_iota(jnp.float32, (4, slots), 0)
    state = packed[:, :8].at[:, 1].add(row_y)
    grad_pos, grad_vel = packed[:, 8:11], packed[:, 11:14]
    n_own = jnp.sum(state[:, 6], axis=-1).astype(jnp.int32)
    at_low = exchange.at_low()
    shift = jnp.where(at_low, 4.0, -4.0).astype(jnp.float32).reshape(1)

    grad_vel = grad_vel + time_step * grad_pos
    pad2 = jnp.zeros((4, 2, slots), jnp.float32)
    carried = jnp.concatenate([grad_pos, grad_vel, pad2], axis=1)
    lam = jnp.concatenate(
        [
            time_step * state[:, 6:7] * grad_vel,
            jnp.zeros((4, LAM_ROWS - 3, slots), jnp.float32),
        ],
        axis=1,
    )

    pieces = exchange.halo(state)
    own, x_low, x_high, far = [piece[:, 2:7:4] for piece in pieces]
    around = jnp.stack([x_low, own, x_high])
    around = jnp.concatenate([around, far[:, None]], axis=1)
    present = around[:, :, 1] > 0.5
    key = jnp.where(present, around[:, :, 0], BEYOND).reshape(-1)
    place = lax.broadcasted_iota(jnp.int32, key.shape, 0)
    order = lax.sort((key, place), dimension=0, num_keys=1)[1]
    total = jnp.sum(present.astype(jnp.int32))
    counts = jnp.concatenate([n_own, total[None]])
    tile_y = (order // slots) % 5
    tile_y = jnp.where(tile_y == 4, jnp.where(at_low, 4, -1), tile_y)
    bias = [
        jnp.where((tile_y >= t - 1) & (tile_y <= t + 1) & (place < total), 1.0, -NEVER)
        for t in range(4)
    ]
    bias = jnp.stack(bias).reshape(4, BLOCKS, 1, LANES)
    bias = jnp.pad(bias, ((0, 0), (0, PAD), (0, 0), (0, 0)), constant_values=-NEVER)
    order = jnp.pad(order.reshape(BLOCKS, 1, LANES), ((0, PAD), (0, 0), (0, 0)))

    saved = []
    for step in range(STEPS):
        if step > 0:
            pieces = exchange.halo(state)
        own_press, merged, ranges, places = run_kernel(
            density_kernel,
            "density",
            (counts, shift),
            (order, bias) + pieces,
            [tiles_of(PRESS_ROWS), MERGED, RANGES, wide(3)],
            [
                packed_region(1),
                vmem_like(wide(1)),
                pltpu.SMEM(RANGES.shape, jnp.int32),
                pltpu.SemaphoreType.DMA,
            ],
            8000,
        )
        press = exchange.halo(own_press)
        if step + 1 < STEPS:
            new_state, merged_p = run_kernel(
                accel_kernel,
                "accel",
                (counts, ranges),
                (order, bias, merged, places, state) + press,
                [TILES, MERGED],
                [packed_region(4), vmem_like(wide(1)), vmem_like(wide(7))],
                10000,
            )
        else:
            new_state = state
            (merged_p,) = run_kernel(
                functools.partial(merge_kernel, 4),
                "merge",
                (counts,),
                (order,) + press,
                [MERGED],
                [packed_region(4)],
                2000,
            )
        saved.append((state, own_press, ranges, merged, merged_p, places))
        state = new_state

    for step in reversed(range(STEPS)):
        state, own_press, ranges, merged, merged_p, places = saved[step]
        lam_pieces = exchange.halo(lam)
        own_grad, merged_l, moves = run_kernel(
            density_grad_kernel,
            "density_grad",
            (counts, ranges),
            (order, bias, merged, places, state, own_press) + lam_pieces,
            [tiles_of(1), MERGED, wide(6)],
            [packed_region(2), vmem_like(wide(2))],
            10000,
        )
        halves = [
            run_kernel(
                functools.partial(main_grad_kernel, half),
                "main_grad_%d" % half,
                (counts, ranges),
                (bias, merged, merged_p, merged_l, places, moves, own_press, lam),
                [tiles_of(FEATS, 2)],
                [vmem_like(wide(2)), vmem_like(wide(7, 2))],
                10000,
            )[0]
            for half in range(2)
        ]
        if step == 0:
            halves[0], back = lax.optimization_barrier((halves[0], back))
        grad_pieces, halves[0] = exchange.halo(own_grad, beside=halves[0])
        lam, carried = run_kernel(
            last_grad_kernel,
            "last_grad",
            (counts, ranges),
            (order, bias, merged, places, state) + grad_pieces + tuple(halves) + (carried,),
            [tiles_of(LAM_ROWS), TILES],
            [packed_region(8), vmem_like(MERGED), vmem_like(wide(1)), vmem_like(wide(3))],
            8000,
        )

    result = exchange.unplace(carried)
    square = jax.ShapeDtypeStruct(result.shape, jnp.float32)
    (result,) = run_kernel(sort_kernel, "unsort_own", (), (back, result), [square], [], 500)
    result = jnp.moveaxis(result[:, :, :6], 2, 0)
    return (result[:3], result[3:] - time_step * result[:3])


def solution(mesh):
    spec = P(None, "gx", "gy", None)
    exchange = Exchange(mesh)
    return jax.shard_map(
        functools.partial(per_device, exchange),
        mesh=mesh,
        in_specs=(spec, spec, P("gx", "gy"), spec, spec),
        out_specs=(spec, spec),
        check_vma=False,
    )
```

```python
import functools

import jax
import jax.numpy as jnp
from jax import lax
from jax.experimental import pallas as pl
from jax.experimental.pallas import tpu as pltpu
from jax.sharding import PartitionSpec as P

STEPS = 4
time_step = 0.05
stiffness = 4.0
rest_density = 1.0
particle_mass = 0.15
viscosity = 0.5


FAR = 1.0e4
BEYOND = 1.0e5
ROWS = 16
LANES = 128
FEATS = 8
LANE_BITS = LANES.bit_length() - 1
PRESS_ROWS = 2
LAM_ROWS = 4
VMEM_LIMIT = 12 << 20
BLOCKS = 30
PAD = 4
MERGE = 4
REACH = 1.001
NEVER = 1.0e30


def path_order(count):
    evens = list(range(0, count, 2))
    odds = list(range(1, count, 2))
    return evens + odds[::-1]


class Exchange:
    def __init__(self, mesh):
        self.count_x = mesh.shape["gx"]
        self.count_y = mesh.shape["gy"]
        assert self.count_y == 4
        path = path_order(self.count_x)
        self.ring = [(a, 0) for a in path] + [(a, 1) for a in path[::-1]]

    def device(self, column, half):
        a, line = self.ring[column % len(self.ring)]
        return a * self.count_y + line * 2 + half

    def permute(self, value, pairs):
        return lax.ppermute(value, ("gx", "gy"), pairs)

    def at_odd(self):
        a, b = lax.axis_index("gx"), lax.axis_index("gy")
        place = jnp.where(a % 2 == 0, a // 2, self.count_x - 1 - a // 2)
        column = jnp.where(b < 2, place, 2 * self.count_x - 1 - place)
        return column % 2 == 1

    def at_low(self):
        return lax.axis_index("gy") % 2 == 0

    def from_ring(self, value, step):
        pairs = [
            (self.device(column + step, half), self.device(column, half))
            for column in range(len(self.ring))
            for half in range(2)
        ]
        return self.permute(value, pairs)

    def from_other_half(self, value):
        pairs = [
            (self.device(column, 1 - half), self.device(column, half))
            for column in range(len(self.ring))
            for half in range(2)
        ]
        return self.permute(value, pairs)

    def routes(self, flip):
        return [
            (a * self.count_y + b, self.device(2 * a + (b + flip) % 2, b // 2))
            for a in range(self.count_x)
            for b in range(self.count_y)
        ]

    def place(self, parts):
        return [self.permute(part, self.routes(flip)) for flip, part in enumerate(parts)]

    def unplace(self, parts):
        return [
            self.permute(part, [(target, source) for source, target in self.routes(flip)])
            for flip, part in enumerate(parts)
        ]

    def halo(self, own, beside=None):
        x_low = self.from_ring(own, -1)
        x_high = self.from_ring(own, 1)
        if beside is not None:
            x_low, x_high, beside = lax.optimization_barrier((x_low, x_high, beside))
        at_low = self.at_low()
        edges = jnp.stack([jnp.where(at_low, part[3], part[0]) for part in (x_low, own, x_high)])
        pieces = (own, x_low, x_high, self.from_other_half(edges))
        return pieces if beside is None else (pieces, beside)


def fill_region(region, pieces, pack, shift_ref=None):
    own, x_low, x_high, far = pieces
    kept = FEATS // pack
    row = lax.broadcasted_iota(jnp.int32, (FEATS, 2 * LANES), 0)
    for rx in range(3):
        for ry in range(5):
            block = far[rx] if ry == 4 else (x_low, own, x_high)[rx][ry]
            if shift_ref is not None:
                if rx != 1:
                    block = jnp.where(row == 0, block + (rx - 1.0), block)
                if ry == 4:
                    block = jnp.where(row == 1, block + shift_ref[0], block)
            for lb in range(2):
                at = (rx * 5 + ry) * 2 + lb
                inside = (at % pack) * kept
                region[at // pack, inside : inside + kept] = block[
                    :kept, lb * LANES : (lb + 1) * LANES
                ]


def each_tile(work, tiles=4, unroll=False):
    if unroll:
        for t in range(tiles):
            work(t)
        return

    def step(t, carry):
        work(t)
        return carry

    lax.fori_loop(0, tiles, step, 0)


def spread_columns(columns, t, values):
    at = 0
    for block, chosen in values:
        padded = jnp.concatenate(
            [block, jnp.zeros((LANES - block.shape[0], 2 * LANES), jnp.float32)], axis=0
        )
        turned = padded.T
        for index, feature in enumerate(chosen):
            columns[at + index, t] = jnp.broadcast_to(
                turned[:, feature : feature + 1], (2 * LANES, LANES)
            )
        at += len(chosen)


def take_lanes(sources, row, pack=1):
    shape = (FEATS, LANES)
    lane = jnp.broadcast_to(row & (LANES - 1), shape)
    block = jnp.broadcast_to(row >> LANE_BITS, shape)
    vector = block // pack if pack > 1 else block
    picked = jnp.zeros(shape, jnp.float32)
    for at, source in enumerate(sources):
        picked = jnp.where(vector == at, jnp.take_along_axis(source, lane, axis=1), picked)
    if pack == 1:
        return picked
    inside = block & (pack - 1)
    result = picked
    for at in range(1, pack):
        shifted = pltpu.roll(picked, FEATS - at * (FEATS // pack), 0)
        result = jnp.where(inside == at, shifted, result)
    return result


def merge_region(merged, region, order_ref, counts_ref, pack):
    for at in range(BLOCKS + PAD):
        merged[at] = jnp.zeros((FEATS, LANES), jnp.float32)
    used = (counts_ref[4] + (LANES - 1)) >> LANE_BITS

    def step(index, carry):
        for near in range(MERGE):
            at = index * MERGE + near
            sources = [region[s] for s in range(-(-BLOCKS // pack))]
            merged[at] = take_lanes(sources, order_ref[at], pack)
        return carry

    lax.fori_loop(0, (used + (MERGE - 1)) // MERGE, step, 0)


def block_ranges(ranges, merged, own, counts_ref):
    depth = merged[:BLOCKS, 2, :]
    rank = lax.broadcasted_iota(jnp.int32, (BLOCKS, LANES), 0) * LANES
    rank = rank + lax.broadcasted_iota(jnp.int32, (BLOCKS, LANES), 1)
    held = rank < counts_ref[4]
    least = jnp.min(jnp.where(held, depth, BEYOND), axis=1, keepdims=True)
    most = jnp.max(jnp.where(held, depth, -BEYOND), axis=1, keepdims=True)
    rows, limits = [], []
    for t in range(4):
        for lb in range(2):
            rows.append(own[t][2:3, lb * LANES : (lb + 1) * LANES])
            lane = lax.broadcasted_iota(jnp.int32, (1, LANES), 1) + lb * LANES
            limits.append((lane < counts_ref[t]).astype(jnp.float32))
    mine = jnp.concatenate(rows, axis=0)
    inside = jnp.concatenate(limits, axis=0) > 0.5
    low = jnp.where(inside, mine, BEYOND)
    high = jnp.where(inside, mine, -BEYOND)
    reach = 1
    while reach < ROWS:
        low = jnp.minimum(low, pltpu.roll(low, LANES - reach, 1))
        high = jnp.maximum(high, pltpu.roll(high, LANES - reach, 1))
        reach *= 2
    low = low - REACH
    high = high + REACH
    first = jnp.full((FEATS, LANES), BLOCKS, jnp.int32)
    past = jnp.zeros((FEATS, LANES), jnp.int32)
    for at in range(BLOCKS):
        near = (jnp.broadcast_to(most[at : at + 1], (FEATS, LANES)) >= low) & (
            jnp.broadcast_to(least[at : at + 1], (FEATS, LANES)) <= high
        )
        first = jnp.where(near, jnp.minimum(first, at), first)
        past = jnp.where(near, at + 1, past)
    length = jnp.maximum(past - first, 0)
    ranges[0] = jnp.minimum(first, BLOCKS - 1)
    for together in range(1, RANGES.shape[0]):
        trips = jnp.zeros((FEATS, LANES), jnp.int32)
        for least_length in range(1, BLOCKS + 1, together):
            trips = jnp.where(length >= least_length, trips + 1, trips)
        ranges[together] = trips


def pair_sums(
    counts_ref, range_ref, columns, sums_ref, outputs, together, body, tiles=(0, 4), spans=1
):
    rows = ROWS * spans
    row_bits = rows.bit_length() - 1
    line_bits = LANE_BITS - row_bits

    def tile_loop(t, carry):
        groups = (counts_ref[t] + (rows - 1)) >> row_bits

        def group_loop(g, carry):
            start = pl.multiple_of(g << row_bits, rows)
            terms_of = body([ref[f, t, pl.ds(start, rows), :] for ref, f in columns], t)
            line = (t << 1) + (g >> line_bits)
            lane = (g & ((1 << line_bits) - 1)) << row_bits
            first = range_ref[0, line, lane]
            trips = range_ref[together, line, lane]

            def block_loop(index, totals):
                totals = list(totals)
                for near in range(together):
                    terms = terms_of(first + index * together + near)
                    totals = [a + b for a, b in zip(totals, terms)]
                return tuple(totals)

            zero = jnp.zeros((rows, LANES), jnp.float32)
            totals = lax.fori_loop(0, trips, block_loop, (zero,) * outputs)
            for index, total in enumerate(totals):
                sums_ref[index, t - tiles[0], pl.ds(start, rows), :] = total
            return carry

        return lax.fori_loop(0, groups, group_loop, carry)

    lax.fori_loop(*tiles, tile_loop, 0)


def row_sums(sums_ref, t, outputs):
    return [jnp.sum(sums_ref[index, t].T, axis=0, keepdims=True) for index in range(outputs)]


def separation(xi, merged, bias_ref, t, block):
    d = [merged[block, f : f + 1, :] - xi[f] for f in range(3)]
    bias = bias_ref[t, block]
    q = jnp.maximum(bias - d[0] * d[0] - d[1] * d[1] - d[2] * d[2], 0.0)
    return d, q


def stack_rows(rows, height=FEATS):
    width = rows[0].shape[1]
    rows = list(rows) + [jnp.zeros((1, width), jnp.float32)] * (height - len(rows))
    return jnp.concatenate(rows, axis=0)


def pack_kernel(flag_ref, held_ref, pos, vel, cot_pos, cot_vel, *parts):
    lane = lax.broadcasted_iota(jnp.int32, (1, 2 * LANES), 1)
    none = jnp.zeros((1, 2 * LANES), jnp.float32)
    swap = flag_ref[0] == 1
    for ty in range(2):
        columns = []
        for tx in range(2):
            live = lane < held_ref[tx, ty]
            rows = [jnp.where(live, pos[f, tx, ty : ty + 1], FAR) for f in range(3)]
            rows += [vel[f, tx, ty : ty + 1] for f in range(3)]
            rows += [jnp.where(live, 1.0, 0.0), none]
            rows += [cot_pos[f, tx, ty : ty + 1] for f in range(3)]
            rows += [cot_vel[f, tx, ty : ty + 1] for f in range(3)]
            columns.append(jnp.concatenate(rows + [none, none], axis=0))
        parts[0][ty] = jnp.where(swap, columns[1], columns[0])
        parts[1][ty] = jnp.where(swap, columns[0], columns[1])


def spread_row(row):
    padded = jnp.concatenate([row, jnp.zeros((LANES - 1, 2 * LANES), jnp.float32)], axis=0)
    return jnp.broadcast_to(padded.T[:, 0:1], (2 * LANES, LANES))


def prepare_kernel(flag_ref, first, second, state, carried, lam, rank_ref):
    shape = (2 * LANES, LANES)
    slot = lax.broadcasted_iota(jnp.int32, shape, 0)
    lane = lax.broadcasted_iota(jnp.int32, shape, 1)
    swap = flag_ref[1] == 1
    for t in range(4):
        near, other = (first, second) if t < 2 else (second, first)
        value = jnp.where(swap, other[t % 2], near[t % 2])
        key = jnp.where(value[6:7] > 0.5, value[2:3], BEYOND)
        keys = spread_row(key)
        ranks = []
        for lb in range(2):
            mine = key[:, lb * LANES : (lb + 1) * LANES]
            ahead = (keys < mine) | ((keys == mine) & (slot < lane + lb * LANES))
            ranks.append(jnp.sum(jnp.where(ahead, 1.0, 0.0), axis=0, keepdims=True))
        rank = jnp.concatenate(ranks, axis=1)
        rank_ref[t] = rank.astype(jnp.int32)
        went = spread_row(rank)
        turned = [[], []]
        for lb in range(2):
            hit = went == (lane + lb * LANES).astype(jnp.float32)
            source = jnp.sum(
                jnp.where(hit, slot.astype(jnp.float32), 0.0), axis=0, keepdims=True
            ).astype(jnp.int32)
            for part in range(2):
                rows = value[part * FEATS : (part + 1) * FEATS]
                turned[part].append(take_lanes([rows[:, :LANES], rows[:, LANES:]], source))
        own, cots = [jnp.concatenate(halves, axis=1) for halves in turned]
        row = lax.broadcasted_iota(jnp.int32, own.shape, 0)
        state[t] = jnp.where(row == 1, own + float(t), own)
        grad_pos = [cots[f : f + 1] for f in range(3)]
        grad_vel = [cots[3 + f : 4 + f] + time_step * cots[f : f + 1] for f in range(3)]
        carried[t] = stack_rows(grad_pos + grad_vel)
        lam[t] = stack_rows([time_step * own[6:7] * g for g in grad_vel], LAM_ROWS)


def restore_kernel(flag_ref, rank_ref, carried, *parts):
    swap = flag_ref[1] == 1
    tiles = []
    for t in range(4):
        value = carried[t]
        halves = [
            take_lanes(
                [value[:, :LANES], value[:, LANES:]], rank_ref[t, :, lb * LANES : (lb + 1) * LANES]
            )
            for lb in range(2)
        ]
        value = jnp.concatenate(halves, axis=1)
        rows = [value[f : f + 1] for f in range(3)]
        rows += [value[3 + f : 4 + f] - time_step * value[f : f + 1] for f in range(3)]
        tiles.append(stack_rows(rows))
    for ty in range(2):
        parts[0][ty] = jnp.where(swap, tiles[2 + ty], tiles[ty])
        parts[1][ty] = jnp.where(swap, tiles[ty], tiles[2 + ty])


def plan_kernel(flag_ref, order, *refs):
    pieces, (counts, padded, bias) = refs[:4], refs[4:]
    total = jnp.float32(0)
    for kind, piece in enumerate(pieces):
        for t in range(piece.shape[0]):
            held = jnp.sum(piece[t][6:7])
            total = total + held
            if kind == 0:
                counts[t] = held.astype(jnp.int32)
    total = total.astype(jnp.int32)
    counts[4] = total
    far_row = jnp.where(flag_ref[2] == 1, 4, -1)
    lane = lax.broadcasted_iota(jnp.int32, (1, LANES), 1)
    for at in range(BLOCKS + PAD):
        if at >= BLOCKS:
            padded[at] = jnp.zeros((1, LANES), jnp.int32)
            for t in range(4):
                bias[t, at] = jnp.full((1, LANES), -NEVER, jnp.float32)
            continue
        places = order[at]
        padded[at] = places
        tile = places >> (LANE_BITS + 1)
        row_y = jnp.where(tile >= 10, tile - 10, jnp.where(tile >= 5, tile - 5, tile))
        row_y = jnp.where(row_y == 4, far_row, row_y)
        held = lane + at * LANES < total
        for t in range(4):
            near = (row_y >= t - 1) & (row_y <= t + 1) & held
            bias[t, at] = jnp.where(near, 1.0, -NEVER)


def merge_kernel(pack, counts_ref, order_ref, *refs):
    pieces, (merged, region) = refs[:4], refs[4:]
    fill_region(region, pieces, pack)
    merge_region(merged, region, order_ref, counts_ref, pack)


def density_kernel(counts_ref, shift_ref, order_ref, bias_ref, *refs):
    pieces = refs[:4]
    out, merged, ranges, columns, region, sums, range_ref, sem = refs[4:]
    fill_region(region, pieces, 1, shift_ref)
    merge_region(merged, region, order_ref, counts_ref, 1)
    block_ranges(ranges, merged, pieces[0], counts_ref)
    copy = pltpu.make_async_copy(ranges, range_ref, sem)
    for t in range(4):
        if t == 2:
            copy.start()
        spread_columns(columns, t, ((pieces[0][t], (0, 1, 2)),))
    copy.wait()

    def body(column, t):
        def terms(block):
            d, q = separation(column, merged, bias_ref, t, block)
            return [q * q * q]

        return terms

    own = [(columns, f) for f in range(3)]
    pair_sums(counts_ref, range_ref, own, sums, 1, 4, body)

    def finish(t):
        live = pieces[0][t][6:7] > 0.5
        density = particle_mass * row_sums(sums, t, 1)[0]
        padded = jnp.where(live, density, 1.0)
        inverse = jnp.where(live, 1.0 / padded, 0.0)
        coefficient = jnp.where(
            live, stiffness * (density / rest_density - 1.0) / (padded * padded), 0.0
        )
        out[t] = stack_rows([coefficient, inverse], PRESS_ROWS)

    each_tile(finish, unroll=True)


def accel_kernel(counts_ref, range_ref, order_ref, bias_ref, merged, places, state, *refs):
    press, (out, merged_p, region, columns, sums) = refs[:4], refs[4:]
    fill_region(region, press, 4)
    merge_region(merged_p, region, order_ref, counts_ref, 4)
    each_tile(
        lambda t: spread_columns(columns, t, ((press[0][t], (0,)),)), unroll=True
    )

    def body(column, t):
        xi, ci = column[:3], column[3]

        def terms(block):
            d, q = separation(xi, merged, bias_ref, t, block)
            q2 = q * q
            visc = q2 * q * merged_p[block, 1:2, :]
            push = (ci + merged_p[block, 0:1, :]) * q2
            moved = [visc * merged[block, 3 + f : 4 + f, :] for f in range(3)]
            pushed = [push * d[f] for f in range(3)]
            return moved + [visc] + pushed

        return terms

    own = [(places, f) for f in range(3)] + [(columns, 0)]
    pair_sums(counts_ref, range_ref, own, sums, 7, 3, body)

    def finish(t):
        own = state[t]
        live = own[6:7] > 0.5
        s = row_sums(sums, t, 7)
        new_pos, new_vel = [], []
        for f in range(3):
            vel = own[3 + f : 4 + f]
            accel = particle_mass * (viscosity * (s[f] - vel * s[3]) - 6.0 * s[4 + f])
            vel = jnp.where(live, vel + time_step * accel, vel)
            new_vel.append(vel)
            new_pos.append(
                jnp.where(live, own[f : f + 1] + time_step * vel, own[f : f + 1])
            )
        out[t] = stack_rows(new_pos + new_vel + [own[6:7]])

    each_tile(finish)


def density_grad_kernel(
    counts_ref, range_ref, order_ref, bias_ref, merged, places, state, press, *refs
):
    lam, (out, merged_l, columns, region, sums) = refs[:4], refs[4:]
    fill_region(region, lam, 2)
    merge_region(merged_l, region, order_ref, counts_ref, 2)
    each_tile(
        lambda t: spread_columns(columns, t, ((state[t], (3, 4, 5)), (lam[0][t], (0, 1, 2))))
    )

    def body(column, t):
        xi, vi, li = column[:3], column[3:6], column[6:]

        def terms(block):
            d, q = separation(xi, merged, bias_ref, t, block)
            lj = [merged_l[block, f : f + 1, :] for f in range(3)]
            q2 = q * q
            along = sum((li[f] - lj[f]) * d[f] for f in range(3))
            moved = sum(lj[f] * (vi[f] - merged[block, 3 + f : 4 + f, :]) for f in range(3))
            return [q2 * along, q2 * q * moved]

        return terms

    own = [(places, f) for f in range(3)] + [(columns, f) for f in range(6)]
    pair_sums(counts_ref, range_ref, own, sums, 2, 3, body)

    def finish(t):
        live = state[t][6:7] > 0.5
        s = row_sums(sums, t, 2)
        c = press[t][0:1]
        w = press[t][1:2]
        grad_c = (-6.0 * particle_mass) * s[0]
        grad_w = (viscosity * particle_mass) * s[1]
        grad = grad_c * (stiffness * w * w - 2.0 * c * w) - grad_w * w * w
        out[t] = jnp.where(live, grad, 0.0)

    each_tile(finish, unroll=True)


def main_grad_kernel(half, counts_ref, range_ref, bias_ref, merged, merged_p, merged_l, *refs):
    places, moves, press, lam, out, columns, sums = refs
    for t in range(2 * half, 2 * half + 2):
        spread_columns(columns, t, ((press[t], (0, 1)),))

    def body(column, t):
        xi, vi, li = column[:3], column[3:6], column[6:9]
        ci, wi = column[9:]

        def terms(block):
            d, q = separation(xi, merged, bias_ref, t, block)
            lj = [merged_l[block, f : f + 1, :] for f in range(3)]
            wj = merged_p[block, 1:2, :]
            cs = ci + merged_p[block, 0:1, :]
            diff = [li[f] - lj[f] for f in range(3)]
            dv = [merged[block, 3 + f : 4 + f, :] - vi[f] for f in range(3)]
            along = sum(diff[f] * d[f] for f in range(3))
            drag = wj * sum(li[f] * dv[f] for f in range(3)) - wi * sum(
                lj[f] * dv[f] for f in range(3)
            )
            q2 = q * q
            q3 = q2 * q
            on_d = q * (q * drag - 8.0 * (cs * along))
            on_l = (cs * q2) * 2.0
            gx = [on_d * d[f] + on_l * diff[f] for f in range(3)]
            gv = [q3 * lj[f] for f in range(3)]
            return gx + gv + [q3 * wj]

        return terms

    own = [(places, f) for f in range(3)] + [(moves, f) for f in range(6)]
    own += [(columns, f) for f in range(2)]
    pair_sums(
        counts_ref, range_ref, own, sums, 7, 2, body, tiles=(2 * half, 2 * half + 2)
    )

    def finish(t):
        s = row_sums(sums, t, 7)
        w = press[2 * half + t][1:2]
        rows = [(3.0 * particle_mass) * s[f] for f in range(3)]
        scale = viscosity * particle_mass
        for f in range(3):
            mine = lam[2 * half + t][f : f + 1]
            rows.append(scale * (w * s[3 + f] - mine * s[6]))
        out[t] = stack_rows(rows)

    each_tile(finish, tiles=2)


def last_grad_kernel(counts_ref, range_ref, order_ref, bias_ref, merged, places, state, *refs):
    grads, partials, carried = refs[:4], refs[4:6], refs[6]
    lam_out, carried_out, region, merged_g, columns, sums = refs[7:]
    fill_region(region, grads, 8)
    merge_region(merged_g, region, order_ref, counts_ref, 8)
    each_tile(
        lambda t: spread_columns(columns, t, ((grads[0][t], (0,)),)), unroll=True
    )

    def body(column, t):
        xi, gi = column[:3], column[3]

        def terms(block):
            d, q = separation(xi, merged, bias_ref, t, block)
            weight = (gi + merged_g[block, 0:1, :]) * (q * q)
            return [weight * d[f] for f in range(3)]

        return terms

    own = [(places, f) for f in range(3)] + [(columns, 0)]
    pair_sums(counts_ref, range_ref, own, sums, 3, 4, body)

    def finish(t):
        live = state[t][6:7] > 0.5
        s = row_sums(sums, t, 3)
        part = partials[t // 2][t % 2]
        old = carried[t]
        new_pos, new_vel = [], []
        for f in range(3):
            extra = part[f : f + 1] + (6.0 * particle_mass) * s[f]
            gx = old[f : f + 1] + jnp.where(live, extra, 0.0)
            gv = old[3 + f : 4 + f] + jnp.where(live, part[3 + f : 4 + f], 0.0)
            new_pos.append(gx)
            new_vel.append(gv + time_step * gx)
        lam_out[t] = stack_rows([jnp.where(live, time_step * v, 0.0) for v in new_vel], LAM_ROWS)
        carried_out[t] = stack_rows(new_pos + new_vel)

    each_tile(finish, unroll=True)


def tiles_of(rows, tiles=4):
    return jax.ShapeDtypeStruct((tiles, rows, 2 * LANES), jnp.float32)


TILES = tiles_of(FEATS)
MERGED = jax.ShapeDtypeStruct((BLOCKS + PAD, FEATS, LANES), jnp.float32)
RANGES = jax.ShapeDtypeStruct((5, FEATS, LANES), jnp.int32)


def wide(count, tiles=4):
    return jax.ShapeDtypeStruct((count, tiles, 2 * LANES, LANES), jnp.float32)


def vmem_like(shape):
    return pltpu.VMEM(shape.shape, shape.dtype)


def packed_region(pack):
    return pltpu.VMEM((-(-BLOCKS // pack), FEATS, LANES), jnp.float32)


def run_kernel(kernel, name, scalars, arrays, out_shape, scratch, cycles, scalar_outputs=0):
    smem = pl.BlockSpec(memory_space=pltpu.SMEM)
    vmem = pl.BlockSpec(memory_space=pltpu.VMEM)
    result = pl.pallas_call(
        kernel,
        name=name,
        out_shape=out_shape,
        in_specs=[smem] * len(scalars) + [vmem] * len(arrays),
        out_specs=[smem] * scalar_outputs + [vmem] * (len(out_shape) - scalar_outputs),
        scratch_shapes=scratch,
        compiler_params=pltpu.CompilerParams(vmem_limit_bytes=VMEM_LIMIT),
        cost_estimate=pl.CostEstimate(
            flops=cycles * 65536, bytes_accessed=1 << 18, transcendentals=0
        ),
    )(*scalars, *arrays)
    return result


def per_device(exchange, positions, velocities, occupancy, cot_positions, cot_velocities):
    slots = positions.shape[3]
    assert positions.shape[1:] == (2, 2, 2 * LANES)
    at_low = exchange.at_low()
    flags = jnp.stack([lax.axis_index("gy") % 2 == 1, exchange.at_odd(), at_low]).astype(jnp.int32)
    shift = jnp.where(at_low, 4.0, -4.0).astype(jnp.float32).reshape(1)
    parts = run_kernel(
        pack_kernel,
        "pack",
        (flags, occupancy),
        (positions, velocities, cot_positions, cot_velocities),
        [tiles_of(2 * FEATS, 2)] * 2,
        [],
        500,
    )
    parts = exchange.place(parts)
    state, carried, lam, rank = run_kernel(
        prepare_kernel,
        "prepare",
        (flags,),
        tuple(parts),
        [TILES, TILES, tiles_of(LAM_ROWS), jax.ShapeDtypeStruct((4, 1, slots), jnp.int32)],
        [],
        1000,
    )

    pieces = exchange.halo(state)
    own, x_low, x_high, far = [piece[:, 2:7:4] for piece in pieces]
    around = jnp.stack([x_low, own, x_high])
    around = jnp.concatenate([around, far[:, None]], axis=1)
    present = around[:, :, 1] > 0.5
    key = jnp.where(present, around[:, :, 0], BEYOND).reshape(-1)
    place = lax.broadcasted_iota(jnp.int32, key.shape, 0)
    order = lax.sort((key, place), dimension=0, num_keys=1)[1]
    counts, order, bias = run_kernel(
        plan_kernel,
        "plan",
        (flags,),
        (order.reshape(BLOCKS, 1, LANES),) + pieces,
        [
            jax.ShapeDtypeStruct((8,), jnp.int32),
            jax.ShapeDtypeStruct((BLOCKS + PAD, 1, LANES), jnp.int32),
            jax.ShapeDtypeStruct((4, BLOCKS + PAD, 1, LANES), jnp.float32),
        ],
        [],
        500,
        scalar_outputs=1,
    )

    saved = []
    for step in range(STEPS):
        if step > 0:
            pieces = exchange.halo(state)
        own_press, merged, ranges, places = run_kernel(
            density_kernel,
            "density",
            (counts, shift),
            (order, bias) + pieces,
            [tiles_of(PRESS_ROWS), MERGED, RANGES, wide(3)],
            [
                packed_region(1),
                vmem_like(wide(1)),
                pltpu.SMEM(RANGES.shape, jnp.int32),
                pltpu.SemaphoreType.DMA,
            ],
            8000,
        )
        press = exchange.halo(own_press)
        if step + 1 < STEPS:
            new_state, merged_p = run_kernel(
                accel_kernel,
                "accel",
                (counts, ranges),
                (order, bias, merged, places, state) + press,
                [TILES, MERGED],
                [packed_region(4), vmem_like(wide(1)), vmem_like(wide(7))],
                10000,
            )
        else:
            new_state = state
            (merged_p,) = run_kernel(
                functools.partial(merge_kernel, 4),
                "merge",
                (counts,),
                (order,) + press,
                [MERGED],
                [packed_region(4)],
                2000,
            )
        saved.append((state, own_press, ranges, merged, merged_p, places))
        state = new_state

    for step in reversed(range(STEPS)):
        state, own_press, ranges, merged, merged_p, places = saved[step]
        lam_pieces = exchange.halo(lam)
        own_grad, merged_l, moves = run_kernel(
            density_grad_kernel,
            "density_grad",
            (counts, ranges),
            (order, bias, merged, places, state, own_press) + lam_pieces,
            [tiles_of(1), MERGED, wide(6)],
            [packed_region(2), vmem_like(wide(2))],
            10000,
        )
        halves = [
            run_kernel(
                functools.partial(main_grad_kernel, half),
                "main_grad_%d" % half,
                (counts, ranges),
                (bias, merged, merged_p, merged_l, places, moves, own_press, lam),
                [tiles_of(FEATS, 2)],
                [vmem_like(wide(2)), vmem_like(wide(7, 2))],
                10000,
            )[0]
            for half in range(2)
        ]
        grad_pieces, halves[0] = exchange.halo(own_grad, beside=halves[0])
        lam, carried = run_kernel(
            last_grad_kernel,
            "last_grad",
            (counts, ranges),
            (order, bias, merged, places, state) + grad_pieces + tuple(halves) + (carried,),
            [tiles_of(LAM_ROWS), TILES],
            [packed_region(8), vmem_like(MERGED), vmem_like(wide(1)), vmem_like(wide(3))],
            8000,
        )

    parts = run_kernel(
        restore_kernel, "restore", (flags,), (rank, carried), [tiles_of(FEATS, 2)] * 2, [], 500
    )
    parts = exchange.unplace(parts)
    swap = lax.axis_index("gy") % 2 == 1
    grads = jnp.stack([jnp.where(swap, parts[1], parts[0]), jnp.where(swap, parts[0], parts[1])])
    grads = jnp.moveaxis(grads, 2, 0)
    return (grads[:3], grads[3:6])


def solution(mesh):
    spec = P(None, "gx", "gy", None)
    exchange = Exchange(mesh)
    return jax.shard_map(
        functools.partial(per_device, exchange),
        mesh=mesh,
        in_specs=(spec, spec, P("gx", "gy"), spec, spec),
        out_specs=(spec, spec),
        check_vma=False,
    )
```

```python
import functools

import jax
import jax.numpy as jnp
from jax import lax
from jax.experimental import pallas as pl
from jax.experimental.pallas import tpu as pltpu
from jax.sharding import PartitionSpec as P

STEPS = 4
time_step = 0.05
stiffness = 4.0
rest_density = 1.0
particle_mass = 0.15
viscosity = 0.5


FAR = 1.0e4
BEYOND = 1.0e5
ROWS = 16
LANES = 128
FEATS = 8
LANE_BITS = LANES.bit_length() - 1
PRESS_ROWS = 2
COUNTS_AT = 64
LAM_ROWS = 4
VMEM_LIMIT = 12 << 20
BLOCKS = 30
PAD = 4
MERGE = 4
REACH = 1.001
NEVER = 1.0e30


def closed_ring(count):
    assert count % 2 == 0
    levels = count // 2
    up = []
    for level in range(levels):
        three = [(2 * level, 0), (2 * level, 1), (2 * level + 1, 1)]
        up += three if level % 2 == 0 else three[::-1]
    down = [(2 * level + 1, 0) for level in range(levels)][::-1]
    return down[-1:] + up + down[:-1]


class Exchange:
    def __init__(self, mesh):
        self.count_x = mesh.shape["gx"]
        self.count_y = mesh.shape["gy"]
        assert self.count_y == 4
        self.ring = closed_ring(self.count_x)

    def device(self, column, half):
        a, line = self.ring[column % len(self.ring)]
        return a * self.count_y + line * 2 + half

    def permute(self, value, pairs):
        return lax.ppermute(value, ("gx", "gy"), pairs)

    def at_odd(self):
        a, b = lax.axis_index("gx"), lax.axis_index("gy")
        odd = jnp.bool_(False)
        for column, (level, line) in enumerate(self.ring):
            if column % 2 == 1:
                odd = odd | ((a == level) & (b // 2 == line))
        return odd

    def at_low(self):
        return lax.axis_index("gy") % 2 == 0

    def from_ring(self, value, step):
        pairs = [
            (self.device(column + step, half), self.device(column, half))
            for column in range(len(self.ring))
            for half in range(2)
        ]
        return self.permute(value, pairs)

    def from_other_half(self, value):
        pairs = [
            (self.device(column, 1 - half), self.device(column, half))
            for column in range(len(self.ring))
            for half in range(2)
        ]
        return self.permute(value, pairs)

    def routes(self, flip):
        return [
            (a * self.count_y + b, self.device(2 * a + (b + flip) % 2, b // 2))
            for a in range(self.count_x)
            for b in range(self.count_y)
        ]

    def place(self, parts):
        return [self.permute(part, self.routes(flip)) for flip, part in enumerate(parts)]

    def unplace(self, parts):
        return [
            self.permute(part, [(target, source) for source, target in self.routes(flip)])
            for flip, part in enumerate(parts)
        ]

    def halo(self, own, beside=None):
        x_low = self.from_ring(own, -1)
        x_high = self.from_ring(own, 1)
        if beside is not None:
            x_low, x_high, beside = lax.optimization_barrier((x_low, x_high, beside))
        at_low = self.at_low()
        edges = jnp.stack([jnp.where(at_low, part[3], part[0]) for part in (x_low, own, x_high)])
        pieces = (own, x_low, x_high, self.from_other_half(edges))
        return pieces if beside is None else (pieces, beside)


def fill_region(region, pieces, pack, shift_ref=None):
    own, x_low, x_high, far = pieces
    kept = FEATS // pack
    row = lax.broadcasted_iota(jnp.int32, (FEATS, 2 * LANES), 0)
    for rx in range(3):
        for ry in range(5):
            block = far[rx] if ry == 4 else (x_low, own, x_high)[rx][ry]
            if shift_ref is not None:
                if rx != 1:
                    block = jnp.where(row == 0, block + (rx - 1.0), block)
                if ry == 4:
                    block = jnp.where(row == 1, block + shift_ref[0], block)
            for lb in range(2):
                at = (rx * 5 + ry) * 2 + lb
                inside = (at % pack) * kept
                region[at // pack, inside : inside + kept] = block[
                    :kept, lb * LANES : (lb + 1) * LANES
                ]


def each_tile(work, tiles=4, unroll=False):
    if unroll:
        for t in range(tiles):
            work(t)
        return

    def step(t, carry):
        work(t)
        return carry

    lax.fori_loop(0, tiles, step, 0)


def spread_columns(columns, t, values):
    at = 0
    for block, chosen in values:
        padded = jnp.concatenate(
            [block, jnp.zeros((LANES - block.shape[0], 2 * LANES), jnp.float32)], axis=0
        )
        turned = padded.T
        for index, feature in enumerate(chosen):
            columns[at + index, t] = jnp.broadcast_to(
                turned[:, feature : feature + 1], (2 * LANES, LANES)
            )
        at += len(chosen)


def take_lanes(sources, row, pack=1):
    shape = (FEATS, LANES)
    lane = jnp.broadcast_to(row & (LANES - 1), shape)
    block = jnp.broadcast_to(row >> LANE_BITS, shape)
    vector = block // pack if pack > 1 else block
    picked = jnp.zeros(shape, jnp.float32)
    for at, source in enumerate(sources):
        picked = jnp.where(vector == at, jnp.take_along_axis(source, lane, axis=1), picked)
    if pack == 1:
        return picked
    inside = block & (pack - 1)
    result = picked
    for at in range(1, pack):
        shifted = pltpu.roll(picked, FEATS - at * (FEATS // pack), 0)
        result = jnp.where(inside == at, shifted, result)
    return result


def merge_region(merged, region, order_ref, total, pack):
    for at in range(BLOCKS + PAD):
        merged[at] = jnp.zeros((FEATS, LANES), jnp.float32)
    used = (total + (LANES - 1)) >> LANE_BITS

    def step(index, carry):
        for near in range(MERGE):
            at = index * MERGE + near
            sources = [region[s] for s in range(-(-BLOCKS // pack))]
            merged[at] = take_lanes(sources, order_ref[at], pack)
        return carry

    lax.fori_loop(0, (used + (MERGE - 1)) // MERGE, step, 0)


def block_ranges(table, merged, own, counts_ref):
    depth = merged[:BLOCKS, 2, :]
    rank = lax.broadcasted_iota(jnp.int32, (BLOCKS, LANES), 0) * LANES
    rank = rank + lax.broadcasted_iota(jnp.int32, (BLOCKS, LANES), 1)
    held = rank < counts_ref[4]
    least = jnp.min(jnp.where(held, depth, BEYOND), axis=1, keepdims=True)
    most = jnp.max(jnp.where(held, depth, -BEYOND), axis=1, keepdims=True)
    rows, limits = [], []
    for t in range(4):
        for lb in range(2):
            rows.append(own[t][2:3, lb * LANES : (lb + 1) * LANES])
            lane = lax.broadcasted_iota(jnp.int32, (1, LANES), 1) + lb * LANES
            limits.append((lane < counts_ref[t]).astype(jnp.float32))
    mine = jnp.concatenate(rows, axis=0)
    inside = jnp.concatenate(limits, axis=0) > 0.5
    low = jnp.where(inside, mine, BEYOND)
    high = jnp.where(inside, mine, -BEYOND)
    reach = 1
    while reach < ROWS:
        low = jnp.minimum(low, pltpu.roll(low, LANES - reach, 1))
        high = jnp.maximum(high, pltpu.roll(high, LANES - reach, 1))
        reach *= 2
    low = low - REACH
    high = high + REACH
    first = jnp.full((FEATS, LANES), BLOCKS, jnp.int32)
    past = jnp.zeros((FEATS, LANES), jnp.int32)
    for at in range(BLOCKS):
        near = (jnp.broadcast_to(most[at : at + 1], (FEATS, LANES)) >= low) & (
            jnp.broadcast_to(least[at : at + 1], (FEATS, LANES)) <= high
        )
        first = jnp.where(near, jnp.minimum(first, at), first)
        past = jnp.where(near, at + 1, past)
    length = jnp.maximum(past - first, 0)
    word = jnp.minimum(first, BLOCKS - 1)
    for together in range(2, 5):
        trips = jnp.zeros((FEATS, LANES), jnp.int32)
        for least_length in range(1, BLOCKS + 1, together):
            trips = jnp.where(length >= least_length, trips + 1, trips)
        word = word | (trips << (8 * (together - 1)))
    per_line = LANES // ROWS
    lane = lax.broadcasted_iota(jnp.int32, (FEATS, LANES), 1)
    line = lax.broadcasted_iota(jnp.int32, (FEATS, LANES), 0)
    word = jnp.take_along_axis(word, (lane & (per_line - 1)) * ROWS, axis=1)
    word = jnp.where(lane // per_line == line, word, 0)
    for shift in (4, 2, 1):
        word = word + pltpu.roll(word, shift, 0)
    for index in range(5):
        word = jnp.where(lane == COUNTS_AT + index, counts_ref[index], word)
    table[...] = word[0:1]


def pair_sums(table_ref, columns, sums_ref, outputs, together, body, tiles=(0, 4)):
    row_bits = ROWS.bit_length() - 1
    per_tile = 2 * LANES // ROWS

    def tile_loop(t, carry):
        groups = (table_ref[0, COUNTS_AT + t] + (ROWS - 1)) >> row_bits

        def group_loop(g, carry):
            start = pl.multiple_of(g << row_bits, ROWS)
            terms_of = body([ref[f, t, pl.ds(start, ROWS), :] for ref, f in columns], t)
            word = table_ref[0, t * per_tile + g]
            first = word & 31
            trips = (word >> (8 * (together - 1))) & 31

            def block_loop(index, totals):
                totals = list(totals)
                for near in range(together):
                    terms = terms_of(first + index * together + near)
                    totals = [a + b for a, b in zip(totals, terms)]
                return tuple(totals)

            zero = jnp.zeros((ROWS, LANES), jnp.float32)
            totals = lax.fori_loop(0, trips, block_loop, (zero,) * outputs)
            for index, total in enumerate(totals):
                sums_ref[index, t - tiles[0], pl.ds(start, ROWS), :] = total
            return carry

        return lax.fori_loop(0, groups, group_loop, carry)

    lax.fori_loop(*tiles, tile_loop, 0)


def row_sums(sums_ref, t, outputs):
    return [jnp.sum(sums_ref[index, t].T, axis=0, keepdims=True) for index in range(outputs)]


def separation(xi, merged, bias_ref, t, block):
    d = [merged[block, f : f + 1, :] - xi[f] for f in range(3)]
    bias = bias_ref[t, block]
    q = jnp.maximum(bias - d[0] * d[0] - d[1] * d[1] - d[2] * d[2], 0.0)
    return d, q


def stack_rows(rows, height=FEATS):
    width = rows[0].shape[1]
    rows = list(rows) + [jnp.zeros((1, width), jnp.float32)] * (height - len(rows))
    return jnp.concatenate(rows, axis=0)


def pack_kernel(flag_ref, held_ref, pos, vel, cot_pos, cot_vel, *parts):
    lane = lax.broadcasted_iota(jnp.int32, (1, 2 * LANES), 1)
    none = jnp.zeros((1, 2 * LANES), jnp.float32)
    swap = flag_ref[0] == 1
    for ty in range(2):
        columns = []
        for tx in range(2):
            live = lane < held_ref[tx, ty]
            rows = [jnp.where(live, pos[f, tx, ty : ty + 1], FAR) for f in range(3)]
            rows += [vel[f, tx, ty : ty + 1] for f in range(3)]
            rows += [jnp.where(live, 1.0, 0.0), none]
            rows += [cot_pos[f, tx, ty : ty + 1] for f in range(3)]
            rows += [cot_vel[f, tx, ty : ty + 1] for f in range(3)]
            columns.append(jnp.concatenate(rows + [none, none], axis=0))
        parts[0][ty] = jnp.where(swap, columns[1], columns[0])
        parts[1][ty] = jnp.where(swap, columns[0], columns[1])


def spread_row(row):
    padded = jnp.concatenate([row, jnp.zeros((LANES - 1, 2 * LANES), jnp.float32)], axis=0)
    return jnp.broadcast_to(padded.T[:, 0:1], (2 * LANES, LANES))


def prepare_kernel(flag_ref, first, second, state, carried, lam, rank_ref):
    shape = (2 * LANES, LANES)
    slot = lax.broadcasted_iota(jnp.int32, shape, 0)
    lane = lax.broadcasted_iota(jnp.int32, shape, 1)
    swap = flag_ref[1] == 1
    for t in range(4):
        near, other = (first, second) if t < 2 else (second, first)
        value = jnp.where(swap, other[t % 2], near[t % 2])
        key = jnp.where(value[6:7] > 0.5, value[2:3], BEYOND)
        keys = spread_row(key)
        ranks = []
        for lb in range(2):
            mine = key[:, lb * LANES : (lb + 1) * LANES]
            ahead = (keys < mine) | ((keys == mine) & (slot < lane + lb * LANES))
            ranks.append(jnp.sum(jnp.where(ahead, 1.0, 0.0), axis=0, keepdims=True))
        rank = jnp.concatenate(ranks, axis=1)
        rank_ref[t] = rank.astype(jnp.int32)
        went = spread_row(rank)
        turned = [[], []]
        for lb in range(2):
            hit = went == (lane + lb * LANES).astype(jnp.float32)
            source = jnp.sum(
                jnp.where(hit, slot.astype(jnp.float32), 0.0), axis=0, keepdims=True
            ).astype(jnp.int32)
            for part in range(2):
                rows = value[part * FEATS : (part + 1) * FEATS]
                turned[part].append(take_lanes([rows[:, :LANES], rows[:, LANES:]], source))
        own, cots = [jnp.concatenate(halves, axis=1) for halves in turned]
        row = lax.broadcasted_iota(jnp.int32, own.shape, 0)
        state[t] = jnp.where(row == 1, own + float(t), own)
        grad_pos = [cots[f : f + 1] for f in range(3)]
        grad_vel = [cots[3 + f : 4 + f] + time_step * cots[f : f + 1] for f in range(3)]
        carried[t] = stack_rows(grad_pos + grad_vel)
        lam[t] = stack_rows([time_step * own[6:7] * g for g in grad_vel], LAM_ROWS)


def restore_kernel(flag_ref, rank_ref, carried, *parts):
    swap = flag_ref[1] == 1
    tiles = []
    for t in range(4):
        value = carried[t]
        halves = [
            take_lanes(
                [value[:, :LANES], value[:, LANES:]], rank_ref[t, :, lb * LANES : (lb + 1) * LANES]
            )
            for lb in range(2)
        ]
        value = jnp.concatenate(halves, axis=1)
        rows = [value[f : f + 1] for f in range(3)]
        rows += [value[3 + f : 4 + f] - time_step * value[f : f + 1] for f in range(3)]
        tiles.append(stack_rows(rows))
    for ty in range(2):
        parts[0][ty] = jnp.where(swap, tiles[2 + ty], tiles[ty])
        parts[1][ty] = jnp.where(swap, tiles[ty], tiles[2 + ty])


def plan_kernel(flag_ref, order, *refs):
    pieces, (counts, padded, bias) = refs[:4], refs[4:]
    total = jnp.float32(0)
    for kind, piece in enumerate(pieces):
        for t in range(piece.shape[0]):
            held = jnp.sum(piece[t][6:7])
            total = total + held
            if kind == 0:
                counts[t] = held.astype(jnp.int32)
    total = total.astype(jnp.int32)
    counts[4] = total
    far_row = jnp.where(flag_ref[2] == 1, 4, -1)
    lane = lax.broadcasted_iota(jnp.int32, (1, LANES), 1)
    for at in range(BLOCKS + PAD):
        if at >= BLOCKS:
            padded[at] = jnp.zeros((1, LANES), jnp.int32)
            for t in range(4):
                bias[t, at] = jnp.full((1, LANES), -NEVER, jnp.float32)
            continue
        places = order[at]
        padded[at] = places
        tile = places >> (LANE_BITS + 1)
        row_y = jnp.where(tile >= 10, tile - 10, jnp.where(tile >= 5, tile - 5, tile))
        row_y = jnp.where(row_y == 4, far_row, row_y)
        held = lane + at * LANES < total
        for t in range(4):
            near = (row_y >= t - 1) & (row_y <= t + 1) & held
            bias[t, at] = jnp.where(near, 1.0, -NEVER)


def spread_kernel(features, block, columns):
    each_tile(lambda t: spread_columns(columns, t, ((block[t], tuple(range(features))),)))


def merge_kernel(pack, table_ref, order_ref, *refs):
    pieces, (merged, region) = refs[:4], refs[4:]
    fill_region(region, pieces, pack)
    merge_region(merged, region, order_ref, table_ref[0, COUNTS_AT + 4], pack)


def density_kernel(counts_ref, shift_ref, order_ref, bias_ref, *refs):
    columns, pieces = refs[0], refs[1:5]
    out, merged, table, region, sums, table_ref, sem = refs[5:]
    fill_region(region, pieces, 1, shift_ref)
    merge_region(merged, region, order_ref, counts_ref[4], 1)
    block_ranges(table, merged, pieces[0], counts_ref)
    copy = pltpu.make_async_copy(table, table_ref, sem)
    copy.start()
    copy.wait()

    def body(column, t):
        def terms(block):
            d, q = separation(column, merged, bias_ref, t, block)
            return [q * q * q]

        return terms

    own = [(columns, f) for f in range(3)]
    pair_sums(table_ref, own, sums, 1, 4, body)

    def finish(t):
        live = pieces[0][t][6:7] > 0.5
        density = particle_mass * row_sums(sums, t, 1)[0]
        padded = jnp.where(live, density, 1.0)
        inverse = jnp.where(live, 1.0 / padded, 0.0)
        coefficient = jnp.where(
            live, stiffness * (density / rest_density - 1.0) / (padded * padded), 0.0
        )
        out[t] = stack_rows([coefficient, inverse], PRESS_ROWS)

    each_tile(finish, unroll=True)


def accel_kernel(table_ref, order_ref, bias_ref, merged, columns, press_columns, state, *refs):
    press, (out, merged_p, region, sums) = refs[:4], refs[4:]
    fill_region(region, press, 4)
    merge_region(merged_p, region, order_ref, table_ref[0, COUNTS_AT + 4], 4)

    def body(column, t):
        xi, ci = column[:3], column[3]

        def terms(block):
            d, q = separation(xi, merged, bias_ref, t, block)
            q2 = q * q
            visc = q2 * q * merged_p[block, 1:2, :]
            push = (ci + merged_p[block, 0:1, :]) * q2
            moved = [visc * merged[block, 3 + f : 4 + f, :] for f in range(3)]
            pushed = [push * d[f] for f in range(3)]
            return moved + [visc] + pushed

        return terms

    own = [(columns, f) for f in range(3)] + [(press_columns, 0)]
    pair_sums(table_ref, own, sums, 7, 3, body)

    def finish(t):
        own = state[t]
        live = own[6:7] > 0.5
        s = row_sums(sums, t, 7)
        new_pos, new_vel = [], []
        for f in range(3):
            vel = own[3 + f : 4 + f]
            accel = particle_mass * (viscosity * (s[f] - vel * s[3]) - 6.0 * s[4 + f])
            vel = jnp.where(live, vel + time_step * accel, vel)
            new_vel.append(vel)
            new_pos.append(
                jnp.where(live, own[f : f + 1] + time_step * vel, own[f : f + 1])
            )
        out[t] = stack_rows(new_pos + new_vel + [own[6:7]])

    each_tile(finish)


def density_grad_kernel(
    table_ref, order_ref, bias_ref, merged, columns, lam_columns, state, press, *refs
):
    lam, (out, merged_l, region, sums) = refs[:4], refs[4:]
    fill_region(region, lam, 2)
    merge_region(merged_l, region, order_ref, table_ref[0, COUNTS_AT + 4], 2)

    def body(column, t):
        xi, vi, li = column[:3], column[3:6], column[6:]

        def terms(block):
            d, q = separation(xi, merged, bias_ref, t, block)
            lj = [merged_l[block, f : f + 1, :] for f in range(3)]
            q2 = q * q
            along = sum((li[f] - lj[f]) * d[f] for f in range(3))
            moved = sum(lj[f] * (vi[f] - merged[block, 3 + f : 4 + f, :]) for f in range(3))
            return [q2 * along, q2 * q * moved]

        return terms

    own = [(columns, f) for f in range(6)] + [(lam_columns, f) for f in range(3)]
    pair_sums(table_ref, own, sums, 2, 3, body)

    def finish(t):
        live = state[t][6:7] > 0.5
        s = row_sums(sums, t, 2)
        c = press[t][0:1]
        w = press[t][1:2]
        grad_c = (-6.0 * particle_mass) * s[0]
        grad_w = (viscosity * particle_mass) * s[1]
        grad = grad_c * (stiffness * w * w - 2.0 * c * w) - grad_w * w * w
        out[t] = jnp.where(live, grad, 0.0)

    each_tile(finish, unroll=True)


def main_grad_kernel(half, table_ref, bias_ref, merged, merged_p, merged_l, *refs):
    columns, lam_columns, press_columns, press, lam, out, sums = refs

    def body(column, t):
        xi, vi, li = column[:3], column[3:6], column[6:9]
        ci, wi = column[9:]

        def terms(block):
            d, q = separation(xi, merged, bias_ref, t, block)
            lj = [merged_l[block, f : f + 1, :] for f in range(3)]
            wj = merged_p[block, 1:2, :]
            cs = ci + merged_p[block, 0:1, :]
            diff = [li[f] - lj[f] for f in range(3)]
            dv = [merged[block, 3 + f : 4 + f, :] - vi[f] for f in range(3)]
            along = sum(diff[f] * d[f] for f in range(3))
            drag = wj * sum(li[f] * dv[f] for f in range(3)) - wi * sum(
                lj[f] * dv[f] for f in range(3)
            )
            q2 = q * q
            q3 = q2 * q
            on_d = q * (q * drag - 8.0 * (cs * along))
            on_l = (cs * q2) * 2.0
            gx = [on_d * d[f] + on_l * diff[f] for f in range(3)]
            gv = [q3 * lj[f] for f in range(3)]
            return gx + gv + [q3 * wj]

        return terms

    own = [(columns, f) for f in range(6)] + [(lam_columns, f) for f in range(3)]
    own += [(press_columns, f) for f in range(2)]
    pair_sums(table_ref, own, sums, 7, 2, body, tiles=(2 * half, 2 * half + 2))

    def finish(t):
        s = row_sums(sums, t, 7)
        w = press[2 * half + t][1:2]
        rows = [(3.0 * particle_mass) * s[f] for f in range(3)]
        scale = viscosity * particle_mass
        for f in range(3):
            mine = lam[2 * half + t][f : f + 1]
            rows.append(scale * (w * s[3 + f] - mine * s[6]))
        out[t] = stack_rows(rows)

    each_tile(finish, tiles=2)


def last_grad_kernel(table_ref, order_ref, bias_ref, merged, places, state, *refs):
    grads, partials, carried = refs[:4], refs[4:6], refs[6]
    lam_out, carried_out, region, merged_g, columns, sums = refs[7:]
    fill_region(region, grads, 8)
    merge_region(merged_g, region, order_ref, table_ref[0, COUNTS_AT + 4], 8)
    each_tile(
        lambda t: spread_columns(columns, t, ((grads[0][t], (0,)),)), unroll=True
    )

    def body(column, t):
        xi, gi = column[:3], column[3]

        def terms(block):
            d, q = separation(xi, merged, bias_ref, t, block)
            weight = (gi + merged_g[block, 0:1, :]) * (q * q)
            return [weight * d[f] for f in range(3)]

        return terms

    own = [(places, f) for f in range(3)] + [(columns, 0)]
    pair_sums(table_ref, own, sums, 3, 4, body)

    def finish(t):
        live = state[t][6:7] > 0.5
        s = row_sums(sums, t, 3)
        part = partials[t // 2][t % 2]
        old = carried[t]
        new_pos, new_vel = [], []
        for f in range(3):
            extra = part[f : f + 1] + (6.0 * particle_mass) * s[f]
            gx = old[f : f + 1] + jnp.where(live, extra, 0.0)
            gv = old[3 + f : 4 + f] + jnp.where(live, part[3 + f : 4 + f], 0.0)
            new_pos.append(gx)
            new_vel.append(gv + time_step * gx)
        lam_out[t] = stack_rows([jnp.where(live, time_step * v, 0.0) for v in new_vel], LAM_ROWS)
        carried_out[t] = stack_rows(new_pos + new_vel)

    each_tile(finish, unroll=True)


def tiles_of(rows, tiles=4):
    return jax.ShapeDtypeStruct((tiles, rows, 2 * LANES), jnp.float32)


TILES = tiles_of(FEATS)
MERGED = jax.ShapeDtypeStruct((BLOCKS + PAD, FEATS, LANES), jnp.float32)
TABLE = jax.ShapeDtypeStruct((1, LANES), jnp.int32)


def wide(count, tiles=4):
    return jax.ShapeDtypeStruct((count, tiles, 2 * LANES, LANES), jnp.float32)


def vmem_like(shape):
    return pltpu.VMEM(shape.shape, shape.dtype)


def packed_region(pack):
    return pltpu.VMEM((-(-BLOCKS // pack), FEATS, LANES), jnp.float32)


def run_kernel(kernel, name, scalars, arrays, out_shape, scratch, cycles, scalar_outputs=0):
    smem = pl.BlockSpec(memory_space=pltpu.SMEM)
    vmem = pl.BlockSpec(memory_space=pltpu.VMEM)
    result = pl.pallas_call(
        kernel,
        name=name,
        out_shape=out_shape,
        in_specs=[smem] * len(scalars) + [vmem] * len(arrays),
        out_specs=[smem] * scalar_outputs + [vmem] * (len(out_shape) - scalar_outputs),
        scratch_shapes=scratch,
        compiler_params=pltpu.CompilerParams(vmem_limit_bytes=VMEM_LIMIT),
        cost_estimate=pl.CostEstimate(
            flops=cycles * 65536, bytes_accessed=1 << 18, transcendentals=0
        ),
    )(*scalars, *arrays)
    return result


def per_device(exchange, positions, velocities, occupancy, cot_positions, cot_velocities):
    slots = positions.shape[3]
    assert positions.shape[1:] == (2, 2, 2 * LANES)
    at_low = exchange.at_low()
    flags = jnp.stack([lax.axis_index("gy") % 2 == 1, exchange.at_odd(), at_low]).astype(jnp.int32)
    shift = jnp.where(at_low, 4.0, -4.0).astype(jnp.float32).reshape(1)
    parts = run_kernel(
        pack_kernel,
        "pack",
        (flags, occupancy),
        (positions, velocities, cot_positions, cot_velocities),
        [tiles_of(2 * FEATS, 2)] * 2,
        [],
        500,
    )
    parts = exchange.place(parts)
    state, carried, lam, rank = run_kernel(
        prepare_kernel,
        "prepare",
        (flags,),
        tuple(parts),
        [TILES, TILES, tiles_of(LAM_ROWS), jax.ShapeDtypeStruct((4, 1, slots), jnp.int32)],
        [],
        1000,
    )

    pieces = exchange.halo(state)
    own, x_low, x_high, far = [piece[:, 2:7:4] for piece in pieces]
    around = jnp.stack([x_low, own, x_high])
    around = jnp.concatenate([around, far[:, None]], axis=1)
    present = around[:, :, 1] > 0.5
    key = jnp.where(present, around[:, :, 0], BEYOND).reshape(-1)
    place = lax.broadcasted_iota(jnp.int32, key.shape, 0)
    order = lax.sort((key, place), dimension=0, num_keys=1)[1]
    counts, order, bias = run_kernel(
        plan_kernel,
        "plan",
        (flags,),
        (order.reshape(BLOCKS, 1, LANES),) + pieces,
        [
            jax.ShapeDtypeStruct((8,), jnp.int32),
            jax.ShapeDtypeStruct((BLOCKS + PAD, 1, LANES), jnp.int32),
            jax.ShapeDtypeStruct((4, BLOCKS + PAD, 1, LANES), jnp.float32),
        ],
        [],
        500,
        scalar_outputs=1,
    )

    def spread(value, features, name):
        return run_kernel(
            functools.partial(spread_kernel, features), name, (), (value,), [wide(features)], [], 2000
        )[0]

    saved = []
    columns = spread(state, 6, "spread_state")
    for step in range(STEPS):
        if step > 0:
            pieces, columns = exchange.halo(state, beside=spread(state, 6, "spread_state"))
        own_press, merged, table = run_kernel(
            density_kernel,
            "density",
            (counts, shift),
            (order, bias, columns) + pieces,
            [tiles_of(PRESS_ROWS), MERGED, TABLE],
            [
                packed_region(1),
                vmem_like(wide(1)),
                pltpu.SMEM(TABLE.shape, jnp.int32),
                pltpu.SemaphoreType.DMA,
            ],
            8000,
        )
        press, press_columns = exchange.halo(
            own_press, beside=spread(own_press, 2, "spread_press")
        )
        if step + 1 < STEPS:
            new_state, merged_p = run_kernel(
                accel_kernel,
                "accel",
                (table,),
                (order, bias, merged, columns, press_columns, state) + press,
                [TILES, MERGED],
                [packed_region(4), vmem_like(wide(7))],
                10000,
            )
        else:
            new_state = state
            (merged_p,) = run_kernel(
                functools.partial(merge_kernel, 4),
                "merge",
                (table,),
                (order,) + press,
                [MERGED],
                [packed_region(4)],
                2000,
            )
        saved.append((state, own_press, table, merged, merged_p, columns, press_columns))
        state = new_state

    for step in reversed(range(STEPS)):
        state, own_press, table, merged, merged_p, columns, press_columns = saved[step]
        lam_pieces, lam_columns = exchange.halo(lam, beside=spread(lam, 3, "spread_lam"))
        own_grad, merged_l = run_kernel(
            density_grad_kernel,
            "density_grad",
            (table,),
            (order, bias, merged, columns, lam_columns, state, own_press) + lam_pieces,
            [tiles_of(1), MERGED],
            [packed_region(2), vmem_like(wide(2))],
            10000,
        )
        halves = [
            run_kernel(
                functools.partial(main_grad_kernel, half),
                "main_grad_%d" % half,
                (table,),
                (bias, merged, merged_p, merged_l, columns, lam_columns, press_columns)
                + (own_press, lam),
                [tiles_of(FEATS, 2)],
                [vmem_like(wide(7, 2))],
                10000,
            )[0]
            for half in range(2)
        ]
        grad_pieces, halves[0] = exchange.halo(own_grad, beside=halves[0])
        lam, carried = run_kernel(
            last_grad_kernel,
            "last_grad",
            (table,),
            (order, bias, merged, columns, state) + grad_pieces + tuple(halves) + (carried,),
            [tiles_of(LAM_ROWS), TILES],
            [packed_region(8), vmem_like(MERGED), vmem_like(wide(1)), vmem_like(wide(3))],
            8000,
        )

    parts = run_kernel(
        restore_kernel, "restore", (flags,), (rank, carried), [tiles_of(FEATS, 2)] * 2, [], 500
    )
    parts = exchange.unplace(parts)
    swap = lax.axis_index("gy") % 2 == 1
    grads = jnp.stack([jnp.where(swap, parts[1], parts[0]), jnp.where(swap, parts[0], parts[1])])
    grads = jnp.moveaxis(grads, 2, 0)
    return (grads[:3], grads[3:6])


def solution(mesh):
    spec = P(None, "gx", "gy", None)
    exchange = Exchange(mesh)
    return jax.shard_map(
        functools.partial(per_device, exchange),
        mesh=mesh,
        in_specs=(spec, spec, P("gx", "gy"), spec, spec),
        out_specs=(spec, spec),
        check_vma=False,
    )
```

```python
import functools

import jax
import jax.numpy as jnp
from jax import lax
from jax.experimental import pallas as pl
from jax.experimental.pallas import tpu as pltpu
from jax.sharding import PartitionSpec as P

STEPS = 4
time_step = 0.05
stiffness = 4.0
rest_density = 1.0
particle_mass = 0.15
viscosity = 0.5


FAR = 1.0e4
BEYOND = 1.0e5
ROWS = 16
LANES = 128
FEATS = 8
LANE_BITS = LANES.bit_length() - 1
PUSH = 12.0
PRESS_ROWS = 2
COUNTS_AT = 64
LAM_ROWS = 4
VMEM_LIMIT = 12 << 20
BLOCKS = 30
PAD = 4
MERGE = 4
REACH = 1.001
NEVER = 1.0e30


def closed_ring(count):
    assert count % 2 == 0
    levels = count // 2
    up = []
    for level in range(levels):
        three = [(2 * level, 0), (2 * level, 1), (2 * level + 1, 1)]
        up += three if level % 2 == 0 else three[::-1]
    down = [(2 * level + 1, 0) for level in range(levels)][::-1]
    return down[-1:] + up + down[:-1]


class Exchange:
    def __init__(self, mesh):
        self.count_x = mesh.shape["gx"]
        self.count_y = mesh.shape["gy"]
        assert self.count_y == 4
        self.ring = closed_ring(self.count_x)

    def device(self, column, half):
        a, line = self.ring[column % len(self.ring)]
        return a * self.count_y + line * 2 + half

    def permute(self, value, pairs):
        return lax.ppermute(value, ("gx", "gy"), pairs)

    def at_odd(self):
        a, b = lax.axis_index("gx"), lax.axis_index("gy")
        odd = jnp.bool_(False)
        for column, (level, line) in enumerate(self.ring):
            if column % 2 == 1:
                odd = odd | ((a == level) & (b // 2 == line))
        return odd

    def at_low(self):
        return lax.axis_index("gy") % 2 == 0

    def from_ring(self, value, step):
        pairs = [
            (self.device(column + step, half), self.device(column, half))
            for column in range(len(self.ring))
            for half in range(2)
        ]
        return self.permute(value, pairs)

    def from_other_half(self, value):
        pairs = [
            (self.device(column, 1 - half), self.device(column, half))
            for column in range(len(self.ring))
            for half in range(2)
        ]
        return self.permute(value, pairs)

    def routes(self, flip):
        return [
            (a * self.count_y + b, self.device(2 * a + (b + flip) % 2, b // 2))
            for a in range(self.count_x)
            for b in range(self.count_y)
        ]

    def place(self, parts):
        return [self.permute(part, self.routes(flip)) for flip, part in enumerate(parts)]

    def unplace(self, parts):
        return [
            self.permute(part, [(target, source) for source, target in self.routes(flip)])
            for flip, part in enumerate(parts)
        ]

    def halo(self, own, beside=None):
        x_low = self.from_ring(own, -1)
        x_high = self.from_ring(own, 1)
        if beside is not None:
            x_low, x_high, beside = lax.optimization_barrier((x_low, x_high, beside))
        at_low = self.at_low()
        edges = jnp.stack([jnp.where(at_low, part[3], part[0]) for part in (x_low, own, x_high)])
        pieces = (own, x_low, x_high, self.from_other_half(edges))
        return pieces if beside is None else (pieces, beside)


def fill_region(region, pieces, pack, shift_ref=None):
    own, x_low, x_high, far = pieces
    kept = FEATS // pack
    row = lax.broadcasted_iota(jnp.int32, (FEATS, 2 * LANES), 0)
    for rx in range(3):
        for ry in range(5):
            block = far[rx] if ry == 4 else (x_low, own, x_high)[rx][ry]
            if shift_ref is not None:
                if rx != 1:
                    block = jnp.where(row == 0, block + (rx - 1.0), block)
                if ry == 4:
                    block = jnp.where(row == 1, block + shift_ref[0], block)
            for lb in range(2):
                at = (rx * 5 + ry) * 2 + lb
                inside = (at % pack) * kept
                region[at // pack, inside : inside + kept] = block[
                    :kept, lb * LANES : (lb + 1) * LANES
                ]


def each_tile(work, tiles=4, unroll=False):
    if unroll:
        for t in range(tiles):
            work(t)
        return

    def step(t, carry):
        work(t)
        return carry

    lax.fori_loop(0, tiles, step, 0)


def spread_columns(columns, t, values):
    at = 0
    for block, chosen in values:
        padded = jnp.concatenate(
            [block, jnp.zeros((LANES - block.shape[0], 2 * LANES), jnp.float32)], axis=0
        )
        turned = padded.T
        for index, feature in enumerate(chosen):
            columns[at + index, t] = jnp.broadcast_to(
                turned[:, feature : feature + 1], (2 * LANES, LANES)
            )
        at += len(chosen)


def take_lanes(sources, row, pack=1):
    shape = (FEATS, LANES)
    lane = jnp.broadcast_to(row & (LANES - 1), shape)
    block = jnp.broadcast_to(row >> LANE_BITS, shape)
    vector = block // pack if pack > 1 else block
    picked = jnp.zeros(shape, jnp.float32)
    for at, source in enumerate(sources):
        picked = jnp.where(vector == at, jnp.take_along_axis(source, lane, axis=1), picked)
    if pack == 1:
        return picked
    inside = block & (pack - 1)
    result = picked
    for at in range(1, pack):
        shifted = pltpu.roll(picked, FEATS - at * (FEATS // pack), 0)
        result = jnp.where(inside == at, shifted, result)
    return result


def merge_region(merged, region, order_ref, total, pack):
    for at in range(BLOCKS + PAD):
        merged[at] = jnp.zeros((FEATS, LANES), jnp.float32)
    used = (total + (LANES - 1)) >> LANE_BITS

    def step(index, carry):
        for near in range(MERGE):
            at = index * MERGE + near
            sources = [region[s] for s in range(-(-BLOCKS // pack))]
            merged[at] = take_lanes(sources, order_ref[at], pack)
        return carry

    lax.fori_loop(0, (used + (MERGE - 1)) // MERGE, step, 0)


def block_ranges(table, merged, own, counts_ref):
    depth = merged[:BLOCKS, 2, :]
    rank = lax.broadcasted_iota(jnp.int32, (BLOCKS, LANES), 0) * LANES
    rank = rank + lax.broadcasted_iota(jnp.int32, (BLOCKS, LANES), 1)
    held = rank < counts_ref[4]
    least = jnp.min(jnp.where(held, depth, BEYOND), axis=1, keepdims=True)
    most = jnp.max(jnp.where(held, depth, -BEYOND), axis=1, keepdims=True)
    rows, limits = [], []
    for t in range(4):
        for lb in range(2):
            rows.append(own[t][2:3, lb * LANES : (lb + 1) * LANES])
            lane = lax.broadcasted_iota(jnp.int32, (1, LANES), 1) + lb * LANES
            limits.append((lane < counts_ref[t]).astype(jnp.float32))
    mine = jnp.concatenate(rows, axis=0)
    inside = jnp.concatenate(limits, axis=0) > 0.5
    low = jnp.where(inside, mine, BEYOND)
    high = jnp.where(inside, mine, -BEYOND)
    reach = 1
    while reach < ROWS:
        low = jnp.minimum(low, pltpu.roll(low, LANES - reach, 1))
        high = jnp.maximum(high, pltpu.roll(high, LANES - reach, 1))
        reach *= 2
    low = low - REACH
    high = high + REACH
    first = jnp.full((FEATS, LANES), BLOCKS, jnp.int32)
    past = jnp.zeros((FEATS, LANES), jnp.int32)
    for at in range(BLOCKS):
        near = (jnp.broadcast_to(most[at : at + 1], (FEATS, LANES)) >= low) & (
            jnp.broadcast_to(least[at : at + 1], (FEATS, LANES)) <= high
        )
        first = jnp.where(near, jnp.minimum(first, at), first)
        past = jnp.where(near, at + 1, past)
    length = jnp.maximum(past - first, 0)
    word = jnp.minimum(first, BLOCKS - 1)
    for together in range(2, 5):
        trips = jnp.zeros((FEATS, LANES), jnp.int32)
        for least_length in range(1, BLOCKS + 1, together):
            trips = jnp.where(length >= least_length, trips + 1, trips)
        word = word | (trips << (8 * (together - 1)))
    per_line = LANES // ROWS
    lane = lax.broadcasted_iota(jnp.int32, (FEATS, LANES), 1)
    line = lax.broadcasted_iota(jnp.int32, (FEATS, LANES), 0)
    word = jnp.take_along_axis(word, (lane & (per_line - 1)) * ROWS, axis=1)
    word = jnp.where(lane // per_line == line, word, 0)
    for shift in (4, 2, 1):
        word = word + pltpu.roll(word, shift, 0)
    for index in range(5):
        word = jnp.where(lane == COUNTS_AT + index, counts_ref[index], word)
    table[...] = word[0:1]


def pair_sums(table_ref, columns, sums_ref, outputs, together, body, tiles=(0, 4)):
    row_bits = ROWS.bit_length() - 1
    per_tile = 2 * LANES // ROWS

    def tile_loop(t, carry):
        groups = (table_ref[0, COUNTS_AT + t] + (ROWS - 1)) >> row_bits

        def group_loop(g, carry):
            start = pl.multiple_of(g << row_bits, ROWS)
            terms_of = body([ref[f, t, pl.ds(start, ROWS), :] for ref, f in columns], t)
            word = table_ref[0, t * per_tile + g]
            first = word & 31
            trips = (word >> (8 * (together - 1))) & 31

            def block_loop(index, totals):
                totals = list(totals)
                for near in range(together):
                    terms = terms_of(first + index * together + near)
                    totals = [a + b for a, b in zip(totals, terms)]
                return tuple(totals)

            zero = jnp.zeros((ROWS, LANES), jnp.float32)
            totals = lax.fori_loop(0, trips, block_loop, (zero,) * outputs)
            for index, total in enumerate(totals):
                sums_ref[index, t - tiles[0], pl.ds(start, ROWS), :] = total
            return carry

        return lax.fori_loop(0, groups, group_loop, carry)

    lax.fori_loop(*tiles, tile_loop, 0)


def row_sums(sums_ref, t, outputs):
    return [jnp.sum(sums_ref[index, t].T, axis=0, keepdims=True) for index in range(outputs)]


def separation(xi, merged, bias_ref, t, block):
    d = [merged[block, f : f + 1, :] - xi[f] for f in range(3)]
    bias = bias_ref[t, block]
    q = jnp.maximum(bias - d[0] * d[0] - d[1] * d[1] - d[2] * d[2], 0.0)
    return d, q


def stack_rows(rows, height=FEATS):
    width = rows[0].shape[1]
    rows = list(rows) + [jnp.zeros((1, width), jnp.float32)] * (height - len(rows))
    return jnp.concatenate(rows, axis=0)


def pack_kernel(flag_ref, held_ref, *refs):
    inputs, parts, held, sems = refs[:4], refs[4:6], refs[6:10], refs[10]
    copies = [
        pltpu.make_async_copy(source, target, sems.at[index])
        for index, (source, target) in enumerate(zip(inputs, held))
    ]
    for copy in copies:
        copy.start()
    for copy in copies:
        copy.wait()
    pos, vel, cot_pos, cot_vel = held
    lane = lax.broadcasted_iota(jnp.int32, (1, 2 * LANES), 1)
    none = jnp.zeros((1, 2 * LANES), jnp.float32)
    swap = flag_ref[0] == 1
    for ty in range(2):
        columns = []
        for tx in range(2):
            live = lane < held_ref[tx, ty]
            rows = [jnp.where(live, pos[f, tx, ty : ty + 1], FAR) for f in range(3)]
            rows += [vel[f, tx, ty : ty + 1] for f in range(3)]
            rows += [jnp.where(live, 1.0, 0.0), none]
            rows += [cot_pos[f, tx, ty : ty + 1] for f in range(3)]
            rows += [cot_vel[f, tx, ty : ty + 1] for f in range(3)]
            columns.append(jnp.concatenate(rows + [none, none], axis=0))
        parts[0][ty] = jnp.where(swap, columns[1], columns[0])
        parts[1][ty] = jnp.where(swap, columns[0], columns[1])


def spread_row(row):
    padded = jnp.concatenate([row, jnp.zeros((LANES - 1, 2 * LANES), jnp.float32)], axis=0)
    return jnp.broadcast_to(padded.T[:, 0:1], (2 * LANES, LANES))


def prepare_kernel(flag_ref, first, second, state, carried, lam, rank_ref):
    shape = (2 * LANES, LANES)
    slot = lax.broadcasted_iota(jnp.int32, shape, 0)
    lane = lax.broadcasted_iota(jnp.int32, shape, 1)
    swap = flag_ref[1] == 1
    for t in range(4):
        near, other = (first, second) if t < 2 else (second, first)
        value = jnp.where(swap, other[t % 2], near[t % 2])
        key = jnp.where(value[6:7] > 0.5, value[2:3], BEYOND)
        keys = spread_row(key)
        ranks = []
        for lb in range(2):
            mine = key[:, lb * LANES : (lb + 1) * LANES]
            ahead = (keys < mine) | ((keys == mine) & (slot < lane + lb * LANES))
            ranks.append(jnp.sum(jnp.where(ahead, 1.0, 0.0), axis=0, keepdims=True))
        rank = jnp.concatenate(ranks, axis=1)
        rank_ref[t] = rank.astype(jnp.int32)
        went = spread_row(rank)
        turned = [[], []]
        for lb in range(2):
            hit = went == (lane + lb * LANES).astype(jnp.float32)
            source = jnp.sum(
                jnp.where(hit, slot.astype(jnp.float32), 0.0), axis=0, keepdims=True
            ).astype(jnp.int32)
            for part in range(2):
                rows = value[part * FEATS : (part + 1) * FEATS]
                turned[part].append(take_lanes([rows[:, :LANES], rows[:, LANES:]], source))
        own, cots = [jnp.concatenate(halves, axis=1) for halves in turned]
        row = lax.broadcasted_iota(jnp.int32, own.shape, 0)
        state[t] = jnp.where(row == 1, own + float(t), own)
        grad_pos = [cots[f : f + 1] for f in range(3)]
        grad_vel = [cots[3 + f : 4 + f] + time_step * cots[f : f + 1] for f in range(3)]
        carried[t] = stack_rows(grad_pos + grad_vel)
        lam[t] = stack_rows([time_step * own[6:7] * g for g in grad_vel], LAM_ROWS)


def restore_kernel(flag_ref, rank_ref, carried, *parts):
    swap = flag_ref[1] == 1
    tiles = []
    for t in range(4):
        value = carried[t]
        halves = [
            take_lanes(
                [value[:, :LANES], value[:, LANES:]], rank_ref[t, :, lb * LANES : (lb + 1) * LANES]
            )
            for lb in range(2)
        ]
        value = jnp.concatenate(halves, axis=1)
        rows = [value[f : f + 1] for f in range(3)]
        rows += [value[3 + f : 4 + f] - time_step * value[f : f + 1] for f in range(3)]
        tiles.append(stack_rows(rows))
    for ty in range(2):
        parts[0][ty] = jnp.where(swap, tiles[2 + ty], tiles[ty])
        parts[1][ty] = jnp.where(swap, tiles[ty], tiles[2 + ty])


def plan_kernel(flag_ref, order, *refs):
    pieces, (counts, padded, bias) = refs[:4], refs[4:]
    total = jnp.float32(0)
    for kind, piece in enumerate(pieces):
        for t in range(piece.shape[0]):
            held = jnp.sum(piece[t][6:7])
            total = total + held
            if kind == 0:
                counts[t] = held.astype(jnp.int32)
    total = total.astype(jnp.int32)
    counts[4] = total
    far_row = jnp.where(flag_ref[2] == 1, 4, -1)
    lane = lax.broadcasted_iota(jnp.int32, (1, LANES), 1)
    for at in range(BLOCKS + PAD):
        if at >= BLOCKS:
            padded[at] = jnp.zeros((1, LANES), jnp.int32)
            for t in range(4):
                bias[t, at] = jnp.full((1, LANES), -NEVER, jnp.float32)
            continue
        places = order[at]
        padded[at] = places
        tile = places >> (LANE_BITS + 1)
        row_y = jnp.where(tile >= 10, tile - 10, jnp.where(tile >= 5, tile - 5, tile))
        row_y = jnp.where(row_y == 4, far_row, row_y)
        held = lane + at * LANES < total
        for t in range(4):
            near = (row_y >= t - 1) & (row_y <= t + 1) & held
            bias[t, at] = jnp.where(near, 1.0, -NEVER)


def spread_kernel(features, block, columns):
    each_tile(lambda t: spread_columns(columns, t, ((block[t], tuple(range(features))),)))


def merge_kernel(pack, table_ref, order_ref, *refs):
    pieces, (merged, region) = refs[:4], refs[4:]
    fill_region(region, pieces, pack)
    merge_region(merged, region, order_ref, table_ref[0, COUNTS_AT + 4], pack)


def density_kernel(counts_ref, shift_ref, order_ref, bias_ref, *refs):
    columns, pieces = refs[0], refs[1:5]
    out, merged, table, region, sums, table_ref = refs[5:]
    fill_region(region, pieces, 1, shift_ref)
    merge_region(merged, region, order_ref, counts_ref[4], 1)
    block_ranges(table, merged, pieces[0], counts_ref)
    words = table[...]
    for index in range(COUNTS_AT):
        table_ref[0, index] = words[0, index]
    for index in range(5):
        table_ref[0, COUNTS_AT + index] = counts_ref[index]

    def body(column, t):
        def terms(block):
            d, q = separation(column, merged, bias_ref, t, block)
            return [q * q * q]

        return terms

    own = [(columns, f) for f in range(3)]
    pair_sums(table_ref, own, sums, 1, 4, body)

    def finish(t):
        live = pieces[0][t][6:7] > 0.5
        density = particle_mass * row_sums(sums, t, 1)[0]
        padded = jnp.where(live, density, 1.0)
        inverse = jnp.where(live, 1.0 / padded, 0.0)
        coefficient = jnp.where(
            live, (PUSH * stiffness) * (density / rest_density - 1.0) / (padded * padded), 0.0
        )
        out[t] = stack_rows([coefficient, inverse], PRESS_ROWS)

    each_tile(finish, unroll=True)


def accel_kernel(table_ref, order_ref, bias_ref, merged, columns, press_columns, state, *refs):
    press, (out, merged_p, region, sums) = refs[:4], refs[4:]
    fill_region(region, press, 4)
    merge_region(merged_p, region, order_ref, table_ref[0, COUNTS_AT + 4], 4)

    def body(column, t):
        xi, vi, ci = column[:3], column[3:6], column[6]

        def terms(block):
            d, q = separation(xi, merged, bias_ref, t, block)
            q2 = q * q
            visc = q2 * q * merged_p[block, 1:2, :]
            push = (ci + merged_p[block, 0:1, :]) * q2
            dv = [merged[block, 3 + f : 4 + f, :] - vi[f] for f in range(3)]
            return [visc * dv[f] - push * d[f] for f in range(3)]

        return terms

    own = [(columns, f) for f in range(6)] + [(press_columns, 0)]
    pair_sums(table_ref, own, sums, 3, 3, body)

    def finish(t):
        own = state[t]
        live = own[6:7] > 0.5
        s = row_sums(sums, t, 3)
        new_pos, new_vel = [], []
        for f in range(3):
            vel = own[3 + f : 4 + f]
            accel = (particle_mass * viscosity) * s[f]
            vel = jnp.where(live, vel + time_step * accel, vel)
            new_vel.append(vel)
            new_pos.append(
                jnp.where(live, own[f : f + 1] + time_step * vel, own[f : f + 1])
            )
        out[t] = stack_rows(new_pos + new_vel + [own[6:7]])

    each_tile(finish, unroll=True)


def density_grad_kernel(
    table_ref, order_ref, bias_ref, merged, columns, lam_columns, state, press, *refs
):
    lam, (out, merged_l, region, sums) = refs[:4], refs[4:]
    fill_region(region, lam, 2)
    merge_region(merged_l, region, order_ref, table_ref[0, COUNTS_AT + 4], 2)

    def body(column, t):
        xi, vi, li = column[:3], column[3:6], column[6:]

        def terms(block):
            d, q = separation(xi, merged, bias_ref, t, block)
            lj = [merged_l[block, f : f + 1, :] for f in range(3)]
            q2 = q * q
            along = sum((li[f] - lj[f]) * d[f] for f in range(3))
            moved = sum(lj[f] * (vi[f] - merged[block, 3 + f : 4 + f, :]) for f in range(3))
            return [q2 * along, q2 * q * moved]

        return terms

    own = [(columns, f) for f in range(6)] + [(lam_columns, f) for f in range(3)]
    pair_sums(table_ref, own, sums, 2, 3, body)

    def finish(t):
        live = state[t][6:7] > 0.5
        s = row_sums(sums, t, 2)
        c = press[t][0:1] * (1.0 / PUSH)
        w = press[t][1:2]
        grad_c = (-6.0 * particle_mass) * s[0]
        grad_w = (viscosity * particle_mass) * s[1]
        grad = grad_c * (stiffness * w * w - 2.0 * c * w) - grad_w * w * w
        out[t] = jnp.where(live, grad, 0.0)

    each_tile(finish, unroll=True)


def main_grad_kernel(half, table_ref, bias_ref, merged, merged_p, merged_l, *refs):
    columns, lam_columns, press_columns, out, sums = refs

    def body(column, t):
        xi, vi, li = column[:3], column[3:6], column[6:9]
        ci, wi = column[9:]

        def terms(block):
            d, q = separation(xi, merged, bias_ref, t, block)
            lj = [merged_l[block, f : f + 1, :] for f in range(3)]
            wj = merged_p[block, 1:2, :]
            cs = ci + merged_p[block, 0:1, :]
            diff = [li[f] - lj[f] for f in range(3)]
            drags = [wj * li[f] - wi * lj[f] for f in range(3)]
            drag = sum(
                drags[f] * (merged[block, 3 + f : 4 + f, :] - vi[f]) for f in range(3)
            )
            along = sum(diff[f] * d[f] for f in range(3))
            q2 = q * q
            q3 = q2 * q
            on_d = q * (q * drag - (8.0 / PUSH) * (cs * along))
            on_l = (cs * q2) * (2.0 / PUSH)
            gx = [on_d * d[f] + on_l * diff[f] for f in range(3)]
            gv = [q3 * drags[f] for f in range(3)]
            return gx + gv

        return terms

    own = [(columns, f) for f in range(6)] + [(lam_columns, f) for f in range(3)]
    own += [(press_columns, f) for f in range(2)]
    pair_sums(table_ref, own, sums, 6, 2, body, tiles=(2 * half, 2 * half + 2))

    def finish(t):
        s = row_sums(sums, t, 6)
        rows = [(3.0 * particle_mass) * s[f] for f in range(3)]
        rows += [(-viscosity * particle_mass) * s[3 + f] for f in range(3)]
        out[t] = stack_rows(rows)

    each_tile(finish, tiles=2)


def last_grad_kernel(table_ref, order_ref, bias_ref, merged, places, state, *refs):
    grads, partials, carried = refs[:4], refs[4:6], refs[6]
    lam_out, carried_out, region, merged_g, columns, sums = refs[7:]
    fill_region(region, grads, 8)
    merge_region(merged_g, region, order_ref, table_ref[0, COUNTS_AT + 4], 8)
    each_tile(
        lambda t: spread_columns(columns, t, ((grads[0][t], (0,)),)), unroll=True
    )

    def body(column, t):
        xi, gi = column[:3], column[3]

        def terms(block):
            d, q = separation(xi, merged, bias_ref, t, block)
            weight = (gi + merged_g[block, 0:1, :]) * (q * q)
            return [weight * d[f] for f in range(3)]

        return terms

    own = [(places, f) for f in range(3)] + [(columns, 0)]
    pair_sums(table_ref, own, sums, 3, 4, body)

    def finish(t):
        live = state[t][6:7] > 0.5
        s = row_sums(sums, t, 3)
        part = partials[t // 2][t % 2]
        old = carried[t]
        new_pos, new_vel = [], []
        for f in range(3):
            extra = part[f : f + 1] + (6.0 * particle_mass) * s[f]
            gx = old[f : f + 1] + jnp.where(live, extra, 0.0)
            gv = old[3 + f : 4 + f] + jnp.where(live, part[3 + f : 4 + f], 0.0)
            new_pos.append(gx)
            new_vel.append(gv + time_step * gx)
        lam_out[t] = stack_rows([jnp.where(live, time_step * v, 0.0) for v in new_vel], LAM_ROWS)
        carried_out[t] = stack_rows(new_pos + new_vel)

    each_tile(finish, unroll=True)


def tiles_of(rows, tiles=4):
    return jax.ShapeDtypeStruct((tiles, rows, 2 * LANES), jnp.float32)


TILES = tiles_of(FEATS)
MERGED = jax.ShapeDtypeStruct((BLOCKS + PAD, FEATS, LANES), jnp.float32)
TABLE = jax.ShapeDtypeStruct((1, LANES), jnp.int32)


def wide(count, tiles=4):
    return jax.ShapeDtypeStruct((count, tiles, 2 * LANES, LANES), jnp.float32)


def vmem_like(shape):
    return pltpu.VMEM(shape.shape, shape.dtype)


def packed_region(pack):
    return pltpu.VMEM((-(-BLOCKS // pack), FEATS, LANES), jnp.float32)


def run_kernel(kernel, name, scalars, arrays, out_shape, scratch, cycles, scalar_outputs=0, anywhere=False):
    smem = pl.BlockSpec(memory_space=pltpu.SMEM)
    vmem = pl.BlockSpec(memory_space=pltpu.VMEM)
    result = pl.pallas_call(
        kernel,
        name=name,
        out_shape=out_shape,
        in_specs=[smem] * len(scalars)
        + [pl.BlockSpec(memory_space=pl.ANY) if anywhere else vmem] * len(arrays),
        out_specs=[smem] * scalar_outputs + [vmem] * (len(out_shape) - scalar_outputs),
        scratch_shapes=scratch,
        compiler_params=pltpu.CompilerParams(vmem_limit_bytes=VMEM_LIMIT),
        cost_estimate=pl.CostEstimate(
            flops=cycles * 65536, bytes_accessed=1 << 18, transcendentals=0
        ),
    )(*scalars, *arrays)
    return result


def per_device(exchange, positions, velocities, occupancy, cot_positions, cot_velocities):
    slots = positions.shape[3]
    assert positions.shape[1:] == (2, 2, 2 * LANES)
    at_low = exchange.at_low()
    flags = jnp.stack([lax.axis_index("gy") % 2 == 1, exchange.at_odd(), at_low]).astype(jnp.int32)
    shift = jnp.where(at_low, 4.0, -4.0).astype(jnp.float32).reshape(1)
    parts = run_kernel(
        pack_kernel,
        "pack",
        (flags, occupancy),
        (positions, velocities, cot_positions, cot_velocities),
        [tiles_of(2 * FEATS, 2)] * 2,
        [pltpu.VMEM(positions.shape, jnp.float32)] * 4 + [pltpu.SemaphoreType.DMA((4,))],
        500,
        anywhere=True,
    )
    parts = exchange.place(parts)
    state, carried, lam, rank = run_kernel(
        prepare_kernel,
        "prepare",
        (flags,),
        tuple(parts),
        [TILES, TILES, tiles_of(LAM_ROWS), jax.ShapeDtypeStruct((4, 1, slots), jnp.int32)],
        [],
        1000,
    )

    pieces = exchange.halo(state)
    own, x_low, x_high, far = [piece[:, 2:7:4] for piece in pieces]
    around = jnp.stack([x_low, own, x_high])
    around = jnp.concatenate([around, far[:, None]], axis=1)
    present = around[:, :, 1] > 0.5
    place_bits = (BLOCKS * LANES - 1).bit_length()
    deepest = (1 << (31 - place_bits)) - 1
    depth = jnp.clip(around[:, :, 0] * float((deepest + 1) // 16), 0.0, deepest - 1.0)
    depth = jnp.where(present, depth.astype(jnp.int32), deepest).reshape(-1)
    depth = jnp.minimum(depth, jnp.where(present.reshape(-1), deepest - 1, deepest))
    place = lax.broadcasted_iota(jnp.int32, depth.shape, 0)
    order = lax.sort((depth << place_bits) | place, is_stable=False) & ((1 << place_bits) - 1)
    counts, order, bias = run_kernel(
        plan_kernel,
        "plan",
        (flags,),
        (order.reshape(BLOCKS, 1, LANES),) + pieces,
        [
            jax.ShapeDtypeStruct((8,), jnp.int32),
            jax.ShapeDtypeStruct((BLOCKS + PAD, 1, LANES), jnp.int32),
            jax.ShapeDtypeStruct((4, BLOCKS + PAD, 1, LANES), jnp.float32),
        ],
        [],
        500,
        scalar_outputs=1,
    )

    def spread(value, features, name):
        return run_kernel(
            functools.partial(spread_kernel, features), name, (), (value,), [wide(features)], [], 2000
        )[0]

    saved = []
    columns = spread(state, 6, "spread_state")
    for step in range(STEPS):
        if step > 0:
            pieces, columns = exchange.halo(state, beside=spread(state, 6, "spread_state"))
        own_press, merged, table = run_kernel(
            density_kernel,
            "density",
            (counts, shift),
            (order, bias, columns) + pieces,
            [tiles_of(PRESS_ROWS), MERGED, TABLE],
            [
                packed_region(1),
                vmem_like(wide(1)),
                pltpu.SMEM(TABLE.shape, jnp.int32),
            ],
            8000,
        )
        press, press_columns = exchange.halo(
            own_press, beside=spread(own_press, 2, "spread_press")
        )
        if step + 1 < STEPS:
            new_state, merged_p = run_kernel(
                accel_kernel,
                "accel",
                (table,),
                (order, bias, merged, columns, press_columns, state) + press,
                [TILES, MERGED],
                [packed_region(4), vmem_like(wide(3))],
                10000,
            )
        else:
            new_state = state
            (merged_p,) = run_kernel(
                functools.partial(merge_kernel, 4),
                "merge",
                (table,),
                (order,) + press,
                [MERGED],
                [packed_region(4)],
                2000,
            )
        saved.append((state, own_press, table, merged, merged_p, columns, press_columns))
        state = new_state

    for step in reversed(range(STEPS)):
        state, own_press, table, merged, merged_p, columns, press_columns = saved[step]
        lam_pieces, lam_columns = exchange.halo(lam, beside=spread(lam, 3, "spread_lam"))
        own_grad, merged_l = run_kernel(
            density_grad_kernel,
            "density_grad",
            (table,),
            (order, bias, merged, columns, lam_columns, state, own_press) + lam_pieces,
            [tiles_of(1), MERGED],
            [packed_region(2), vmem_like(wide(2))],
            10000,
        )
        halves = [
            run_kernel(
                functools.partial(main_grad_kernel, half),
                "main_grad_%d" % half,
                (table,),
                (bias, merged, merged_p, merged_l, columns, lam_columns, press_columns),
                [tiles_of(FEATS, 2)],
                [vmem_like(wide(6, 2))],
                10000,
            )[0]
            for half in range(2)
        ]
        grad_pieces, halves[0] = exchange.halo(own_grad, beside=halves[0])
        lam, carried = run_kernel(
            last_grad_kernel,
            "last_grad",
            (table,),
            (order, bias, merged, columns, state) + grad_pieces + tuple(halves) + (carried,),
            [tiles_of(LAM_ROWS), TILES],
            [packed_region(8), vmem_like(MERGED), vmem_like(wide(1)), vmem_like(wide(3))],
            8000,
        )

    parts = run_kernel(
        restore_kernel, "restore", (flags,), (rank, carried), [tiles_of(FEATS, 2)] * 2, [], 500
    )
    parts = exchange.unplace(parts)
    swap = lax.axis_index("gy") % 2 == 1
    grads = jnp.stack([jnp.where(swap, parts[1], parts[0]), jnp.where(swap, parts[0], parts[1])])
    grads = jnp.moveaxis(grads, 2, 0)
    return (grads[:3], grads[3:6])


def solution(mesh):
    spec = P(None, "gx", "gy", None)
    exchange = Exchange(mesh)
    return jax.shard_map(
        functools.partial(per_device, exchange),
        mesh=mesh,
        in_specs=(spec, spec, P("gx", "gy"), spec, spec),
        out_specs=(spec, spec),
        check_vma=False,
    )
```

```python
import functools

import jax
import jax.numpy as jnp
from jax import lax
from jax.experimental import pallas as pl
from jax.experimental.pallas import tpu as pltpu
from jax.sharding import PartitionSpec as P

STEPS = 4
time_step = 0.05
stiffness = 4.0
rest_density = 1.0
particle_mass = 0.15
viscosity = 0.5


FAR = 1.0e4
BEYOND = 1.0e5
ROWS = 16
LANES = 128
FEATS = 8
LANE_BITS = LANES.bit_length() - 1
PUSH = 12.0
PRESS_ROWS = 2
COUNTS_AT = 64
LAM_ROWS = 4
VMEM_LIMIT = 12 << 20
BLOCKS = 30
PAD = 4
MERGE = 4
REACH = 1.001
NEVER = 1.0e30


def closed_ring(count):
    assert count % 2 == 0
    levels = count // 2
    up = []
    for level in range(levels):
        three = [(2 * level, 0), (2 * level, 1), (2 * level + 1, 1)]
        up += three if level % 2 == 0 else three[::-1]
    down = [(2 * level + 1, 0) for level in range(levels)][::-1]
    return down[-1:] + up + down[:-1]


class Exchange:
    def __init__(self, mesh):
        self.count_x = mesh.shape["gx"]
        self.count_y = mesh.shape["gy"]
        assert self.count_y == 4
        self.ring = closed_ring(self.count_x)

    def device(self, column, half):
        a, line = self.ring[column % len(self.ring)]
        return a * self.count_y + line * 2 + half

    def permute(self, value, pairs):
        return lax.ppermute(value, ("gx", "gy"), pairs)

    def at_odd(self):
        a, b = lax.axis_index("gx"), lax.axis_index("gy")
        odd = jnp.bool_(False)
        for column, (level, line) in enumerate(self.ring):
            if column % 2 == 1:
                odd = odd | ((a == level) & (b // 2 == line))
        return odd

    def at_low(self):
        return lax.axis_index("gy") % 2 == 0

    def from_ring(self, value, step):
        pairs = [
            (self.device(column + step, half), self.device(column, half))
            for column in range(len(self.ring))
            for half in range(2)
        ]
        return self.permute(value, pairs)

    def from_other_half(self, value):
        pairs = [
            (self.device(column, 1 - half), self.device(column, half))
            for column in range(len(self.ring))
            for half in range(2)
        ]
        return self.permute(value, pairs)

    def routes(self, flip):
        return [
            (a * self.count_y + b, self.device(2 * a + (b + flip) % 2, b // 2))
            for a in range(self.count_x)
            for b in range(self.count_y)
        ]

    def place(self, parts):
        return [self.permute(part, self.routes(flip)) for flip, part in enumerate(parts)]

    def unplace(self, parts):
        return [
            self.permute(part, [(target, source) for source, target in self.routes(flip)])
            for flip, part in enumerate(parts)
        ]

    def halo(self, own, beside=None):
        x_low = self.from_ring(own, -1)
        x_high = self.from_ring(own, 1)
        if beside is not None:
            x_low, x_high, beside = lax.optimization_barrier((x_low, x_high, beside))
        at_low = self.at_low()
        edges = jnp.stack([jnp.where(at_low, part[3], part[0]) for part in (x_low, own, x_high)])
        pieces = (own, x_low, x_high, self.from_other_half(edges))
        return pieces if beside is None else (pieces, beside)


def fill_region(region, pieces, pack, shift_ref=None):
    own, x_low, x_high, far = pieces
    kept = FEATS // pack
    row = lax.broadcasted_iota(jnp.int32, (FEATS, 2 * LANES), 0)
    for rx in range(3):
        for ry in range(5):
            block = far[rx] if ry == 4 else (x_low, own, x_high)[rx][ry]
            if shift_ref is not None:
                if rx != 1:
                    block = jnp.where(row == 0, block + (rx - 1.0), block)
                if ry == 4:
                    block = jnp.where(row == 1, block + shift_ref[0], block)
            for lb in range(2):
                at = (rx * 5 + ry) * 2 + lb
                inside = (at % pack) * kept
                region[at // pack, inside : inside + kept] = block[
                    :kept, lb * LANES : (lb + 1) * LANES
                ]


def each_tile(work, tiles=4, unroll=False):
    if unroll:
        for t in range(tiles):
            work(t)
        return

    def step(t, carry):
        work(t)
        return carry

    lax.fori_loop(0, tiles, step, 0)


def spread_columns(columns, t, values):
    at = 0
    for block, chosen in values:
        padded = jnp.concatenate(
            [block, jnp.zeros((LANES - block.shape[0], 2 * LANES), jnp.float32)], axis=0
        )
        turned = padded.T
        for index, feature in enumerate(chosen):
            columns[at + index, t] = jnp.broadcast_to(
                turned[:, feature : feature + 1], (2 * LANES, LANES)
            )
        at += len(chosen)


def take_lanes(sources, row, pack=1):
    shape = (FEATS, LANES)
    lane = jnp.broadcast_to(row & (LANES - 1), shape)
    block = jnp.broadcast_to(row >> LANE_BITS, shape)
    vector = block // pack if pack > 1 else block
    picked = jnp.zeros(shape, jnp.float32)
    for at, source in enumerate(sources):
        picked = jnp.where(vector == at, jnp.take_along_axis(source, lane, axis=1), picked)
    if pack == 1:
        return picked
    inside = block & (pack - 1)
    result = picked
    for at in range(1, pack):
        shifted = pltpu.roll(picked, FEATS - at * (FEATS // pack), 0)
        result = jnp.where(inside == at, shifted, result)
    return result


def merge_region(merged, region, order_ref, total, pack):
    for at in range(BLOCKS + PAD):
        merged[at] = jnp.zeros((FEATS, LANES), jnp.float32)
    used = (total + (LANES - 1)) >> LANE_BITS

    def step(index, carry):
        for near in range(MERGE):
            at = index * MERGE + near
            sources = [region[s] for s in range(-(-BLOCKS // pack))]
            merged[at] = take_lanes(sources, order_ref[at], pack)
        return carry

    lax.fori_loop(0, (used + (MERGE - 1)) // MERGE, step, 0)


def block_ranges(table, merged, own, counts_ref):
    depth = merged[:BLOCKS, 2, :]
    rank = lax.broadcasted_iota(jnp.int32, (BLOCKS, LANES), 0) * LANES
    rank = rank + lax.broadcasted_iota(jnp.int32, (BLOCKS, LANES), 1)
    held = rank < counts_ref[4]
    least = jnp.min(jnp.where(held, depth, BEYOND), axis=1, keepdims=True)
    most = jnp.max(jnp.where(held, depth, -BEYOND), axis=1, keepdims=True)
    rows, limits = [], []
    for t in range(4):
        for lb in range(2):
            rows.append(own[t][2:3, lb * LANES : (lb + 1) * LANES])
            lane = lax.broadcasted_iota(jnp.int32, (1, LANES), 1) + lb * LANES
            limits.append((lane < counts_ref[t]).astype(jnp.float32))
    mine = jnp.concatenate(rows, axis=0)
    inside = jnp.concatenate(limits, axis=0) > 0.5
    low = jnp.where(inside, mine, BEYOND)
    high = jnp.where(inside, mine, -BEYOND)
    reach = 1
    while reach < ROWS:
        low = jnp.minimum(low, pltpu.roll(low, LANES - reach, 1))
        high = jnp.maximum(high, pltpu.roll(high, LANES - reach, 1))
        reach *= 2
    low = low - REACH
    high = high + REACH
    first = jnp.full((FEATS, LANES), BLOCKS, jnp.int32)
    past = jnp.zeros((FEATS, LANES), jnp.int32)
    for at in range(BLOCKS):
        near = (jnp.broadcast_to(most[at : at + 1], (FEATS, LANES)) >= low) & (
            jnp.broadcast_to(least[at : at + 1], (FEATS, LANES)) <= high
        )
        first = jnp.where(near, jnp.minimum(first, at), first)
        past = jnp.where(near, at + 1, past)
    length = jnp.maximum(past - first, 0)
    word = jnp.minimum(first, BLOCKS - 1)
    for together in range(2, 5):
        trips = jnp.zeros((FEATS, LANES), jnp.int32)
        for least_length in range(1, BLOCKS + 1, together):
            trips = jnp.where(length >= least_length, trips + 1, trips)
        word = word | (trips << (8 * (together - 1)))
    per_line = LANES // ROWS
    lane = lax.broadcasted_iota(jnp.int32, (FEATS, LANES), 1)
    line = lax.broadcasted_iota(jnp.int32, (FEATS, LANES), 0)
    word = jnp.take_along_axis(word, (lane & (per_line - 1)) * ROWS, axis=1)
    word = jnp.where(lane // per_line == line, word, 0)
    for shift in (4, 2, 1):
        word = word + pltpu.roll(word, shift, 0)
    for index in range(5):
        word = jnp.where(lane == COUNTS_AT + index, counts_ref[index], word)
    table[...] = word[0:1]


def pair_sums(table_ref, columns, sums_ref, outputs, together, body, tiles=(0, 4)):
    row_bits = ROWS.bit_length() - 1
    per_tile = 2 * LANES // ROWS

    def tile_loop(t, carry):
        groups = (table_ref[0, COUNTS_AT + t] + (ROWS - 1)) >> row_bits

        def group_loop(g, carry):
            start = pl.multiple_of(g << row_bits, ROWS)
            terms_of = body([ref[f, t, pl.ds(start, ROWS), :] for ref, f in columns], t)
            word = table_ref[0, t * per_tile + g]
            first = word & 31
            trips = (word >> (8 * (together - 1))) & 31

            def block_loop(index, totals):
                totals = list(totals)
                for near in range(together):
                    terms = terms_of(first + index * together + near)
                    totals = [a + b for a, b in zip(totals, terms)]
                return tuple(totals)

            zero = jnp.zeros((ROWS, LANES), jnp.float32)
            totals = lax.fori_loop(0, trips, block_loop, (zero,) * outputs)
            for index, total in enumerate(totals):
                sums_ref[index, t - tiles[0], pl.ds(start, ROWS), :] = total
            return carry

        return lax.fori_loop(0, groups, group_loop, carry)

    lax.fori_loop(*tiles, tile_loop, 0)


def row_sums(sums_ref, t, outputs):
    return [jnp.sum(sums_ref[index, t].T, axis=0, keepdims=True) for index in range(outputs)]


def separation(xi, merged, bias_ref, t, block):
    d = [merged[block, f : f + 1, :] - xi[f] for f in range(3)]
    bias = bias_ref[t, block]
    q = jnp.maximum(bias - d[0] * d[0] - d[1] * d[1] - d[2] * d[2], 0.0)
    return d, q


def stack_rows(rows, height=FEATS):
    width = rows[0].shape[1]
    rows = list(rows) + [jnp.zeros((1, width), jnp.float32)] * (height - len(rows))
    return jnp.concatenate(rows, axis=0)


def pack_kernel(flag_ref, held_ref, *refs):
    inputs, parts, held, sems = refs[:4], refs[4:6], refs[6:10], refs[10]
    copies = [
        pltpu.make_async_copy(source, target, sems.at[index])
        for index, (source, target) in enumerate(zip(inputs, held))
    ]
    for copy in copies:
        copy.start()
    for copy in copies:
        copy.wait()
    pos, vel, cot_pos, cot_vel = held
    lane = lax.broadcasted_iota(jnp.int32, (1, 2 * LANES), 1)
    none = jnp.zeros((1, 2 * LANES), jnp.float32)
    swap = flag_ref[0] == 1
    for ty in range(2):
        columns = []
        for tx in range(2):
            live = lane < held_ref[tx, ty]
            rows = [jnp.where(live, pos[f, tx, ty : ty + 1], FAR) for f in range(3)]
            rows += [vel[f, tx, ty : ty + 1] for f in range(3)]
            rows += [jnp.where(live, 1.0, 0.0), none]
            rows += [cot_pos[f, tx, ty : ty + 1] for f in range(3)]
            rows += [cot_vel[f, tx, ty : ty + 1] for f in range(3)]
            columns.append(jnp.concatenate(rows + [none, none], axis=0))
        parts[0][ty] = jnp.where(swap, columns[1], columns[0])
        parts[1][ty] = jnp.where(swap, columns[0], columns[1])


def spread_row(row):
    padded = jnp.concatenate([row, jnp.zeros((LANES - 1, 2 * LANES), jnp.float32)], axis=0)
    return jnp.broadcast_to(padded.T[:, 0:1], (2 * LANES, LANES))


def prepare_kernel(flag_ref, first, second, state, carried, lam, rank_ref):
    shape = (2 * LANES, LANES)
    slot = lax.broadcasted_iota(jnp.int32, shape, 0)
    lane = lax.broadcasted_iota(jnp.int32, shape, 1)
    swap = flag_ref[1] == 1
    for t in range(4):
        near, other = (first, second) if t < 2 else (second, first)
        value = jnp.where(swap, other[t % 2], near[t % 2])
        key = jnp.where(value[6:7] > 0.5, value[2:3], BEYOND)
        keys = spread_row(key)
        ranks = []
        for lb in range(2):
            mine = key[:, lb * LANES : (lb + 1) * LANES]
            ahead = (keys < mine) | ((keys == mine) & (slot < lane + lb * LANES))
            ranks.append(jnp.sum(jnp.where(ahead, 1.0, 0.0), axis=0, keepdims=True))
        rank = jnp.concatenate(ranks, axis=1)
        rank_ref[t] = rank.astype(jnp.int32)
        went = spread_row(rank)
        turned = [[], []]
        for lb in range(2):
            hit = went == (lane + lb * LANES).astype(jnp.float32)
            source = jnp.sum(
                jnp.where(hit, slot.astype(jnp.float32), 0.0), axis=0, keepdims=True
            ).astype(jnp.int32)
            for part in range(2):
                rows = value[part * FEATS : (part + 1) * FEATS]
                turned[part].append(take_lanes([rows[:, :LANES], rows[:, LANES:]], source))
        own, cots = [jnp.concatenate(halves, axis=1) for halves in turned]
        row = lax.broadcasted_iota(jnp.int32, own.shape, 0)
        state[t] = jnp.where(row == 1, own + float(t), own)
        grad_pos = [cots[f : f + 1] for f in range(3)]
        grad_vel = [cots[3 + f : 4 + f] + time_step * cots[f : f + 1] for f in range(3)]
        carried[t] = stack_rows(grad_pos + grad_vel)
        lam[t] = stack_rows([time_step * own[6:7] * g for g in grad_vel], LAM_ROWS)


def restore_kernel(flag_ref, rank_ref, carried, *parts):
    swap = flag_ref[1] == 1
    tiles = []
    for t in range(4):
        value = carried[t]
        halves = [
            take_lanes(
                [value[:, :LANES], value[:, LANES:]], rank_ref[t, :, lb * LANES : (lb + 1) * LANES]
            )
            for lb in range(2)
        ]
        value = jnp.concatenate(halves, axis=1)
        rows = [value[f : f + 1] for f in range(3)]
        rows += [value[3 + f : 4 + f] - time_step * value[f : f + 1] for f in range(3)]
        tiles.append(stack_rows(rows))
    for ty in range(2):
        parts[0][ty] = jnp.where(swap, tiles[2 + ty], tiles[ty])
        parts[1][ty] = jnp.where(swap, tiles[ty], tiles[2 + ty])


def plan_kernel(flag_ref, order, *refs):
    pieces, (counts, padded, bias) = refs[:4], refs[4:]
    rows = []
    for kind, piece in enumerate(pieces):
        for t in range(piece.shape[0]):
            rows.append(piece[t][6:7])
            if kind == 0:
                counts[t] = jnp.sum(rows[-1]).astype(jnp.int32)
    total = jnp.sum(sum(rows)).astype(jnp.int32)
    counts[4] = total
    far_row = jnp.where(flag_ref[2] == 1, 4, -1)
    lane = lax.broadcasted_iota(jnp.int32, (1, LANES), 1)
    for at in range(BLOCKS + PAD):
        if at >= BLOCKS:
            padded[at] = jnp.zeros((1, LANES), jnp.int32)
            for t in range(4):
                bias[t, at] = jnp.full((1, LANES), -NEVER, jnp.float32)
            continue
        places = order[at]
        padded[at] = places
        tile = places >> (LANE_BITS + 1)
        row_y = jnp.where(tile >= 10, tile - 10, jnp.where(tile >= 5, tile - 5, tile))
        row_y = jnp.where(row_y == 4, far_row, row_y)
        held = lane + at * LANES < total
        for t in range(4):
            near = (row_y >= t - 1) & (row_y <= t + 1) & held
            bias[t, at] = jnp.where(near, 1.0, -NEVER)


def spread_kernel(features, block, columns):
    each_tile(lambda t: spread_columns(columns, t, ((block[t], tuple(range(features))),)))


def fetch_table(table, table_ref, sem):
    copy = pltpu.make_async_copy(table, table_ref, sem)
    copy.start()
    return copy, table[...][0, COUNTS_AT + 4]


def merge_kernel(pack, table_ref, order_ref, *refs):
    pieces, (merged, region) = refs[:4], refs[4:]
    fill_region(region, pieces, pack)
    merge_region(merged, region, order_ref, table_ref[0, COUNTS_AT + 4], pack)


def density_kernel(counts_ref, shift_ref, order_ref, bias_ref, *refs):
    columns, pieces = refs[0], refs[1:5]
    out, merged, table, region, sums, table_ref = refs[5:]
    fill_region(region, pieces, 1, shift_ref)
    merge_region(merged, region, order_ref, counts_ref[4], 1)
    block_ranges(table, merged, pieces[0], counts_ref)
    words = table[...]
    for index in range(COUNTS_AT):
        table_ref[0, index] = words[0, index]
    for index in range(5):
        table_ref[0, COUNTS_AT + index] = counts_ref[index]

    def body(column, t):
        def terms(block):
            d, q = separation(column, merged, bias_ref, t, block)
            return [q * q * q]

        return terms

    own = [(columns, f) for f in range(3)]
    pair_sums(table_ref, own, sums, 1, 4, body)

    def finish(t):
        live = pieces[0][t][6:7] > 0.5
        density = particle_mass * row_sums(sums, t, 1)[0]
        padded = jnp.where(live, density, 1.0)
        inverse = jnp.where(live, 1.0 / padded, 0.0)
        coefficient = jnp.where(
            live, (PUSH * stiffness) * (density / rest_density - 1.0) / (padded * padded), 0.0
        )
        out[t] = stack_rows([coefficient, inverse], PRESS_ROWS)

    each_tile(finish, unroll=True)


def accel_kernel(table, order_ref, bias_ref, merged, columns, press_columns, state, *refs):
    press, (out, merged_p, region, sums, table_ref, sem) = refs[:4], refs[4:]
    copy, total = fetch_table(table, table_ref, sem)
    fill_region(region, press, 4)
    merge_region(merged_p, region, order_ref, total, 4)
    copy.wait()

    def body(column, t):
        xi, vi, ci = column[:3], column[3:6], column[6]

        def terms(block):
            d, q = separation(xi, merged, bias_ref, t, block)
            q2 = q * q
            visc = q2 * q * merged_p[block, 1:2, :]
            push = (ci + merged_p[block, 0:1, :]) * q2
            dv = [merged[block, 3 + f : 4 + f, :] - vi[f] for f in range(3)]
            return [visc * dv[f] - push * d[f] for f in range(3)]

        return terms

    own = [(columns, f) for f in range(6)] + [(press_columns, 0)]
    pair_sums(table_ref, own, sums, 3, 3, body)

    def finish(t):
        own = state[t]
        live = own[6:7] > 0.5
        s = row_sums(sums, t, 3)
        new_pos, new_vel = [], []
        for f in range(3):
            vel = own[3 + f : 4 + f]
            accel = (particle_mass * viscosity) * s[f]
            vel = jnp.where(live, vel + time_step * accel, vel)
            new_vel.append(vel)
            new_pos.append(
                jnp.where(live, own[f : f + 1] + time_step * vel, own[f : f + 1])
            )
        out[t] = stack_rows(new_pos + new_vel + [own[6:7]])

    each_tile(finish, unroll=True)


def density_grad_kernel(
    table, order_ref, bias_ref, merged, columns, lam_columns, state, press, *refs
):
    lam, (out, merged_l, region, sums, table_ref, sem) = refs[:4], refs[4:]
    copy, total = fetch_table(table, table_ref, sem)
    fill_region(region, lam, 2)
    merge_region(merged_l, region, order_ref, total, 2)
    copy.wait()

    def body(column, t):
        xi, vi, li = column[:3], column[3:6], column[6:]

        def terms(block):
            d, q = separation(xi, merged, bias_ref, t, block)
            lj = [merged_l[block, f : f + 1, :] for f in range(3)]
            q2 = q * q
            along = sum((li[f] - lj[f]) * d[f] for f in range(3))
            moved = sum(lj[f] * (vi[f] - merged[block, 3 + f : 4 + f, :]) for f in range(3))
            return [q2 * along, q2 * q * moved]

        return terms

    own = [(columns, f) for f in range(6)] + [(lam_columns, f) for f in range(3)]
    pair_sums(table_ref, own, sums, 2, 3, body)

    def finish(t):
        live = state[t][6:7] > 0.5
        s = row_sums(sums, t, 2)
        c = press[t][0:1] * (1.0 / PUSH)
        w = press[t][1:2]
        grad_c = (-6.0 * particle_mass) * s[0]
        grad_w = (viscosity * particle_mass) * s[1]
        grad = grad_c * (stiffness * w * w - 2.0 * c * w) - grad_w * w * w
        out[t] = jnp.where(live, grad, 0.0)

    each_tile(finish, unroll=True)


def main_grad_kernel(half, table_ref, bias_ref, merged, merged_p, merged_l, *refs):
    columns, lam_columns, press_columns, out, sums = refs

    def body(column, t):
        xi, vi, li = column[:3], column[3:6], column[6:9]
        ci, wi = column[9:]

        def terms(block):
            d, q = separation(xi, merged, bias_ref, t, block)
            lj = [merged_l[block, f : f + 1, :] for f in range(3)]
            wj = merged_p[block, 1:2, :]
            cs = ci + merged_p[block, 0:1, :]
            diff = [li[f] - lj[f] for f in range(3)]
            drags = [wj * li[f] - wi * lj[f] for f in range(3)]
            drag = sum(
                drags[f] * (merged[block, 3 + f : 4 + f, :] - vi[f]) for f in range(3)
            )
            along = sum(diff[f] * d[f] for f in range(3))
            q2 = q * q
            q3 = q2 * q
            on_d = q * (q * drag - (8.0 / PUSH) * (cs * along))
            on_l = (cs * q2) * (2.0 / PUSH)
            gx = [on_d * d[f] + on_l * diff[f] for f in range(3)]
            gv = [q3 * drags[f] for f in range(3)]
            return gx + gv

        return terms

    own = [(columns, f) for f in range(6)] + [(lam_columns, f) for f in range(3)]
    own += [(press_columns, f) for f in range(2)]
    pair_sums(table_ref, own, sums, 6, 2, body, tiles=(2 * half, 2 * half + 2))

    def finish(t):
        s = row_sums(sums, t, 6)
        rows = [(3.0 * particle_mass) * s[f] for f in range(3)]
        rows += [(-viscosity * particle_mass) * s[3 + f] for f in range(3)]
        out[t] = stack_rows(rows)

    each_tile(finish, tiles=2)


def last_grad_kernel(table, order_ref, bias_ref, merged, places, state, *refs):
    grads, partials, carried = refs[:4], refs[4:6], refs[6]
    lam_out, carried_out, region, merged_g, columns, sums, table_ref, sem = refs[7:]
    copy, total = fetch_table(table, table_ref, sem)
    fill_region(region, grads, 8)
    merge_region(merged_g, region, order_ref, total, 8)
    each_tile(
        lambda t: spread_columns(columns, t, ((grads[0][t], (0,)),)), unroll=True
    )
    copy.wait()

    def body(column, t):
        xi, gi = column[:3], column[3]

        def terms(block):
            d, q = separation(xi, merged, bias_ref, t, block)
            weight = (gi + merged_g[block, 0:1, :]) * (q * q)
            return [weight * d[f] for f in range(3)]

        return terms

    own = [(places, f) for f in range(3)] + [(columns, 0)]
    pair_sums(table_ref, own, sums, 3, 4, body)

    def finish(t):
        live = state[t][6:7] > 0.5
        s = row_sums(sums, t, 3)
        part = partials[t // 2][t % 2]
        old = carried[t]
        new_pos, new_vel = [], []
        for f in range(3):
            extra = part[f : f + 1] + (6.0 * particle_mass) * s[f]
            gx = old[f : f + 1] + jnp.where(live, extra, 0.0)
            gv = old[3 + f : 4 + f] + jnp.where(live, part[3 + f : 4 + f], 0.0)
            new_pos.append(gx)
            new_vel.append(gv + time_step * gx)
        lam_out[t] = stack_rows([jnp.where(live, time_step * v, 0.0) for v in new_vel], LAM_ROWS)
        carried_out[t] = stack_rows(new_pos + new_vel)

    each_tile(finish, unroll=True)


def tiles_of(rows, tiles=4):
    return jax.ShapeDtypeStruct((tiles, rows, 2 * LANES), jnp.float32)


TILES = tiles_of(FEATS)
MERGED = jax.ShapeDtypeStruct((BLOCKS + PAD, FEATS, LANES), jnp.float32)
TABLE = jax.ShapeDtypeStruct((1, LANES), jnp.int32)
TABLE_COPY = [pltpu.SMEM(TABLE.shape, jnp.int32), pltpu.SemaphoreType.DMA]


def wide(count, tiles=4):
    return jax.ShapeDtypeStruct((count, tiles, 2 * LANES, LANES), jnp.float32)


def vmem_like(shape):
    return pltpu.VMEM(shape.shape, shape.dtype)


def packed_region(pack):
    return pltpu.VMEM((-(-BLOCKS // pack), FEATS, LANES), jnp.float32)


def run_kernel(kernel, name, scalars, arrays, out_shape, scratch, cycles, scalar_outputs=0, anywhere=False):
    smem = pl.BlockSpec(memory_space=pltpu.SMEM)
    vmem = pl.BlockSpec(memory_space=pltpu.VMEM)
    result = pl.pallas_call(
        kernel,
        name=name,
        out_shape=out_shape,
        in_specs=[smem] * len(scalars)
        + [pl.BlockSpec(memory_space=pltpu.HBM) if anywhere else vmem] * len(arrays),
        out_specs=[smem] * scalar_outputs + [vmem] * (len(out_shape) - scalar_outputs),
        scratch_shapes=scratch,
        compiler_params=pltpu.CompilerParams(
            vmem_limit_bytes=(60 << 20) if anywhere else VMEM_LIMIT
        ),
        cost_estimate=pl.CostEstimate(
            flops=cycles * 65536, bytes_accessed=1 << 18, transcendentals=0
        ),
    )(*scalars, *arrays)
    return result


def per_device(exchange, positions, velocities, occupancy, cot_positions, cot_velocities):
    slots = positions.shape[3]
    assert positions.shape[1:] == (2, 2, 2 * LANES)
    at_low = exchange.at_low()
    flags = jnp.stack([lax.axis_index("gy") % 2 == 1, exchange.at_odd(), at_low]).astype(jnp.int32)
    shift = jnp.where(at_low, 4.0, -4.0).astype(jnp.float32).reshape(1)
    parts = run_kernel(
        pack_kernel,
        "pack",
        (flags, occupancy),
        (positions, velocities, cot_positions, cot_velocities),
        [tiles_of(2 * FEATS, 2)] * 2,
        [pltpu.VMEM(positions.shape, jnp.float32)] * 4 + [pltpu.SemaphoreType.DMA((4,))],
        500,
        anywhere=True,
    )
    parts = exchange.place(parts)
    state, carried, lam, rank = run_kernel(
        prepare_kernel,
        "prepare",
        (flags,),
        tuple(parts),
        [TILES, TILES, tiles_of(LAM_ROWS), jax.ShapeDtypeStruct((4, 1, slots), jnp.int32)],
        [],
        1000,
    )

    pieces = exchange.halo(state)
    own, x_low, x_high, far = [piece[:, 2:7:4] for piece in pieces]
    around = jnp.stack([x_low, own, x_high])
    around = jnp.concatenate([around, far[:, None]], axis=1)
    present = around[:, :, 1] > 0.5
    place_bits = (BLOCKS * LANES - 1).bit_length()
    deepest = (1 << (31 - place_bits)) - 1
    depth = jnp.clip(around[:, :, 0] * float((deepest + 1) // 16), 0.0, deepest - 1.0)
    depth = jnp.where(present, depth.astype(jnp.int32), deepest).reshape(-1)
    depth = jnp.minimum(depth, jnp.where(present.reshape(-1), deepest - 1, deepest))
    place = lax.broadcasted_iota(jnp.int32, depth.shape, 0)
    order = lax.sort((depth << place_bits) | place, is_stable=False) & ((1 << place_bits) - 1)
    counts, order, bias = run_kernel(
        plan_kernel,
        "plan",
        (flags,),
        (order.reshape(BLOCKS, 1, LANES),) + pieces,
        [
            jax.ShapeDtypeStruct((8,), jnp.int32),
            jax.ShapeDtypeStruct((BLOCKS + PAD, 1, LANES), jnp.int32),
            jax.ShapeDtypeStruct((4, BLOCKS + PAD, 1, LANES), jnp.float32),
        ],
        [],
        500,
        scalar_outputs=1,
    )

    def spread(value, features, name):
        return run_kernel(
            functools.partial(spread_kernel, features), name, (), (value,), [wide(features)], [], 2000
        )[0]

    saved = []
    columns = spread(state, 6, "spread_state")
    for step in range(STEPS):
        if step > 0:
            pieces, columns = exchange.halo(state, beside=spread(state, 6, "spread_state"))
        own_press, merged, table = run_kernel(
            density_kernel,
            "density",
            (counts, shift),
            (order, bias, columns) + pieces,
            [tiles_of(PRESS_ROWS), MERGED, TABLE],
            [
                packed_region(1),
                vmem_like(wide(1)),
                pltpu.SMEM(TABLE.shape, jnp.int32),
            ],
            8000,
        )
        press, press_columns = exchange.halo(
            own_press, beside=spread(own_press, 2, "spread_press")
        )
        if step + 1 < STEPS:
            new_state, merged_p = run_kernel(
                accel_kernel,
                "accel",
                (),
                (table, order, bias, merged, columns, press_columns, state) + press,
                [TILES, MERGED],
                [packed_region(4), vmem_like(wide(3))] + TABLE_COPY,
                10000,
            )
        else:
            new_state = state
            (merged_p,) = run_kernel(
                functools.partial(merge_kernel, 4),
                "merge",
                (table,),
                (order,) + press,
                [MERGED],
                [packed_region(4)],
                2000,
            )
        saved.append((state, own_press, table, merged, merged_p, columns, press_columns))
        state = new_state

    for step in reversed(range(STEPS)):
        state, own_press, table, merged, merged_p, columns, press_columns = saved[step]
        lam_pieces, lam_columns = exchange.halo(lam, beside=spread(lam, 3, "spread_lam"))
        own_grad, merged_l = run_kernel(
            density_grad_kernel,
            "density_grad",
            (),
            (table, order, bias, merged, columns, lam_columns, state, own_press) + lam_pieces,
            [tiles_of(1), MERGED],
            [packed_region(2), vmem_like(wide(2))] + TABLE_COPY,
            10000,
        )
        halves = [
            run_kernel(
                functools.partial(main_grad_kernel, half),
                "main_grad_%d" % half,
                (table,),
                (bias, merged, merged_p, merged_l, columns, lam_columns, press_columns),
                [tiles_of(FEATS, 2)],
                [vmem_like(wide(6, 2))],
                10000,
            )[0]
            for half in range(2)
        ]
        grad_pieces, halves[0] = exchange.halo(own_grad, beside=halves[0])
        lam, carried = run_kernel(
            last_grad_kernel,
            "last_grad",
            (),
            (table, order, bias, merged, columns, state) + grad_pieces + tuple(halves) + (carried,),
            [tiles_of(LAM_ROWS), TILES],
            [packed_region(8), vmem_like(MERGED), vmem_like(wide(1)), vmem_like(wide(3))]
            + TABLE_COPY,
            8000,
        )

    parts = run_kernel(
        restore_kernel, "restore", (flags,), (rank, carried), [tiles_of(FEATS, 2)] * 2, [], 500
    )
    parts = exchange.unplace(parts)
    swap = lax.axis_index("gy") % 2 == 1
    grads = jnp.stack([jnp.where(swap, parts[1], parts[0]), jnp.where(swap, parts[0], parts[1])])
    grads = jnp.moveaxis(grads, 2, 0)
    return (grads[:3], grads[3:6])


def solution(mesh):
    spec = P(None, "gx", "gy", None)
    exchange = Exchange(mesh)
    return jax.shard_map(
        functools.partial(per_device, exchange),
        mesh=mesh,
        in_specs=(spec, spec, P("gx", "gy"), spec, spec),
        out_specs=(spec, spec),
        check_vma=False,
    )
```

```python
import functools

import jax
import jax.numpy as jnp
from jax import lax
from jax.experimental import pallas as pl
from jax.experimental.pallas import tpu as pltpu
from jax.sharding import PartitionSpec as P

STEPS = 4
time_step = 0.05
stiffness = 4.0
rest_density = 1.0
particle_mass = 0.15
viscosity = 0.5


FAR = 1.0e4
BEYOND = 1.0e5
ROWS = 16
LANES = 128
FEATS = 8
LANE_BITS = LANES.bit_length() - 1
PUSH = 12.0
PRESS_ROWS = 2
COUNTS_AT = 64
LAM_ROWS = 4
VMEM_LIMIT = 12 << 20
BLOCKS = 30
PAD = 4
MERGE = 4
REACH = 1.001
NEVER = 1.0e30


def closed_ring(count):
    assert count % 2 == 0
    levels = count // 2
    up = []
    for level in range(levels):
        three = [(2 * level, 0), (2 * level, 1), (2 * level + 1, 1)]
        up += three if level % 2 == 0 else three[::-1]
    down = [(2 * level + 1, 0) for level in range(levels)][::-1]
    return down[-1:] + up + down[:-1]


class Exchange:
    def __init__(self, mesh):
        self.count_x = mesh.shape["gx"]
        self.count_y = mesh.shape["gy"]
        assert self.count_y == 4
        self.ring = closed_ring(self.count_x)

    def device(self, column, half):
        a, line = self.ring[column % len(self.ring)]
        return a * self.count_y + line * 2 + half

    def permute(self, value, pairs):
        return lax.ppermute(value, ("gx", "gy"), pairs)

    def at_odd(self):
        a, b = lax.axis_index("gx"), lax.axis_index("gy")
        odd = jnp.bool_(False)
        for column, (level, line) in enumerate(self.ring):
            if column % 2 == 1:
                odd = odd | ((a == level) & (b // 2 == line))
        return odd

    def at_low(self):
        return lax.axis_index("gy") % 2 == 0

    def from_ring(self, value, step):
        pairs = [
            (self.device(column + step, half), self.device(column, half))
            for column in range(len(self.ring))
            for half in range(2)
        ]
        return self.permute(value, pairs)

    def from_other_half(self, value):
        pairs = [
            (self.device(column, 1 - half), self.device(column, half))
            for column in range(len(self.ring))
            for half in range(2)
        ]
        return self.permute(value, pairs)

    def routes(self, flip):
        return [
            (a * self.count_y + b, self.device(2 * a + (b + flip) % 2, b // 2))
            for a in range(self.count_x)
            for b in range(self.count_y)
        ]

    def place(self, parts):
        return [self.permute(part, self.routes(flip)) for flip, part in enumerate(parts)]

    def unplace(self, parts):
        return [
            self.permute(part, [(target, source) for source, target in self.routes(flip)])
            for flip, part in enumerate(parts)
        ]

    def halo(self, own, beside=None):
        x_low = self.from_ring(own, -1)
        x_high = self.from_ring(own, 1)
        if beside is not None:
            x_low, x_high, beside = lax.optimization_barrier((x_low, x_high, beside))
        at_low = self.at_low()
        edges = jnp.stack([jnp.where(at_low, part[3], part[0]) for part in (x_low, own, x_high)])
        pieces = (own, x_low, x_high, self.from_other_half(edges))
        return pieces if beside is None else (pieces, beside)


def fill_region(region, pieces, pack, shift=None):
    own, x_low, x_high, far = pieces
    kept = FEATS // pack
    row = lax.broadcasted_iota(jnp.int32, (FEATS, 2 * LANES), 0)
    for rx in range(3):
        for ry in range(5):
            block = far[rx] if ry == 4 else (x_low, own, x_high)[rx][ry]
            if shift is not None:
                if rx != 1:
                    block = jnp.where(row == 0, block + (rx - 1.0), block)
                if ry == 4:
                    block = jnp.where(row == 1, block + shift, block)
            for lb in range(2):
                at = (rx * 5 + ry) * 2 + lb
                inside = (at % pack) * kept
                region[at // pack, inside : inside + kept] = block[
                    :kept, lb * LANES : (lb + 1) * LANES
                ]


def each_tile(work, tiles=4, unroll=False):
    if unroll:
        for t in range(tiles):
            work(t)
        return

    def step(t, carry):
        work(t)
        return carry

    lax.fori_loop(0, tiles, step, 0)


def spread_columns(columns, t, values):
    at = 0
    for block, chosen in values:
        padded = jnp.concatenate(
            [block, jnp.zeros((LANES - block.shape[0], 2 * LANES), jnp.float32)], axis=0
        )
        turned = padded.T
        for index, feature in enumerate(chosen):
            columns[at + index, t] = jnp.broadcast_to(
                turned[:, feature : feature + 1], (2 * LANES, LANES)
            )
        at += len(chosen)


def take_lanes(sources, row, pack=1):
    shape = (FEATS, LANES)
    lane = jnp.broadcast_to(row & (LANES - 1), shape)
    block = jnp.broadcast_to(row >> LANE_BITS, shape)
    vector = block // pack if pack > 1 else block
    picked = jnp.zeros(shape, jnp.float32)
    for at, source in enumerate(sources):
        picked = jnp.where(vector == at, jnp.take_along_axis(source, lane, axis=1), picked)
    if pack == 1:
        return picked
    inside = block & (pack - 1)
    result = picked
    for at in range(1, pack):
        shifted = pltpu.roll(picked, FEATS - at * (FEATS // pack), 0)
        result = jnp.where(inside == at, shifted, result)
    return result


def merge_region(merged, region, order_ref, total, pack):
    for at in range(BLOCKS + PAD):
        merged[at] = jnp.zeros((FEATS, LANES), jnp.float32)
    used = (total + (LANES - 1)) >> LANE_BITS

    def step(index, carry):
        for near in range(MERGE):
            at = index * MERGE + near
            sources = [region[s] for s in range(-(-BLOCKS // pack))]
            merged[at] = take_lanes(sources, order_ref[at], pack)
        return carry

    lax.fori_loop(0, (used + (MERGE - 1)) // MERGE, step, 0)


def block_ranges(table, merged, own, counts_ref):
    depth = merged[:BLOCKS, 2, :]
    rank = lax.broadcasted_iota(jnp.int32, (BLOCKS, LANES), 0) * LANES
    rank = rank + lax.broadcasted_iota(jnp.int32, (BLOCKS, LANES), 1)
    held = rank < counts_ref[4]
    least = jnp.min(jnp.where(held, depth, BEYOND), axis=1, keepdims=True)
    most = jnp.max(jnp.where(held, depth, -BEYOND), axis=1, keepdims=True)
    rows, limits = [], []
    for t in range(4):
        for lb in range(2):
            rows.append(own[t][2:3, lb * LANES : (lb + 1) * LANES])
            lane = lax.broadcasted_iota(jnp.int32, (1, LANES), 1) + lb * LANES
            limits.append((lane < counts_ref[t]).astype(jnp.float32))
    mine = jnp.concatenate(rows, axis=0)
    inside = jnp.concatenate(limits, axis=0) > 0.5
    low = jnp.where(inside, mine, BEYOND)
    high = jnp.where(inside, mine, -BEYOND)
    reach = 1
    while reach < ROWS:
        low = jnp.minimum(low, pltpu.roll(low, LANES - reach, 1))
        high = jnp.maximum(high, pltpu.roll(high, LANES - reach, 1))
        reach *= 2
    low = low - REACH
    high = high + REACH
    first = jnp.full((FEATS, LANES), BLOCKS, jnp.int32)
    past = jnp.zeros((FEATS, LANES), jnp.int32)
    for at in range(BLOCKS):
        near = (jnp.broadcast_to(most[at : at + 1], (FEATS, LANES)) >= low) & (
            jnp.broadcast_to(least[at : at + 1], (FEATS, LANES)) <= high
        )
        first = jnp.where(near, jnp.minimum(first, at), first)
        past = jnp.where(near, at + 1, past)
    length = jnp.maximum(past - first, 0)
    word = jnp.minimum(first, BLOCKS - 1)
    for together in range(2, 5):
        trips = jnp.zeros((FEATS, LANES), jnp.int32)
        for least_length in range(1, BLOCKS + 1, together):
            trips = jnp.where(length >= least_length, trips + 1, trips)
        word = word | (trips << (8 * (together - 1)))
    per_line = LANES // ROWS
    lane = lax.broadcasted_iota(jnp.int32, (FEATS, LANES), 1)
    line = lax.broadcasted_iota(jnp.int32, (FEATS, LANES), 0)
    word = jnp.take_along_axis(word, (lane & (per_line - 1)) * ROWS, axis=1)
    word = jnp.where(lane // per_line == line, word, 0)
    for shift in (4, 2, 1):
        word = word + pltpu.roll(word, shift, 0)
    for index in range(5):
        word = jnp.where(lane == COUNTS_AT + index, counts_ref[index], word)
    table[...] = word[0:1]


def first_share(groups):
    return (groups * 5 + 7) >> 3


def pair_sums(table_ref, columns, sums_ref, outputs, together, body, share=None):
    row_bits = ROWS.bit_length() - 1
    per_tile = 2 * LANES // ROWS

    def tile_loop(t, carry):
        groups = (table_ref[0, COUNTS_AT + t] + (ROWS - 1)) >> row_bits

        def group_loop(g, carry):
            start = pl.multiple_of(g << row_bits, ROWS)
            terms_of = body([ref[f, t, pl.ds(start, ROWS), :] for ref, f in columns], t)
            word = table_ref[0, t * per_tile + g]
            first = word & 31
            trips = (word >> (8 * (together - 1))) & 31

            def block_loop(index, totals):
                totals = list(totals)
                for near in range(together):
                    terms = terms_of(first + index * together + near)
                    totals = [a + b for a, b in zip(totals, terms)]
                return tuple(totals)

            zero = jnp.zeros((ROWS, LANES), jnp.float32)
            totals = lax.fori_loop(0, trips, block_loop, (zero,) * outputs)
            for index, total in enumerate(totals):
                sums_ref[index, t, pl.ds(start, ROWS), :] = total
            return carry

        begin = first_share(groups) if share == 1 else 0
        end = first_share(groups) if share == 0 else groups
        return lax.fori_loop(begin, end, group_loop, carry)

    lax.fori_loop(0, 4, tile_loop, 0)


def row_sums(sums_ref, t, outputs):
    return [jnp.sum(sums_ref[index, t].T, axis=0, keepdims=True) for index in range(outputs)]


def separation(xi, merged, bias_ref, t, block):
    d = [merged[block, f : f + 1, :] - xi[f] for f in range(3)]
    bias = bias_ref[t, block]
    q = jnp.maximum(bias - d[0] * d[0] - d[1] * d[1] - d[2] * d[2], 0.0)
    return d, q


def stack_rows(rows, height=FEATS):
    width = rows[0].shape[1]
    rows = list(rows) + [jnp.zeros((1, width), jnp.float32)] * (height - len(rows))
    return jnp.concatenate(rows, axis=0)


def pack_kernel(exchange, held_ref, *refs):
    inputs, parts, held, sems = refs[:4], refs[4:6], refs[6:10], refs[10]
    copies = [
        pltpu.make_async_copy(source, target, sems.at[index])
        for index, (source, target) in enumerate(zip(inputs, held))
    ]
    for copy in copies:
        copy.start()
    for copy in copies:
        copy.wait()
    pos, vel, cot_pos, cot_vel = held
    lane = lax.broadcasted_iota(jnp.int32, (1, 2 * LANES), 1)
    none = jnp.zeros((1, 2 * LANES), jnp.float32)
    swap = lax.axis_index("gy") % 2 == 1
    for ty in range(2):
        columns = []
        for tx in range(2):
            live = lane < held_ref[tx, ty]
            rows = [jnp.where(live, pos[f, tx, ty : ty + 1], FAR) for f in range(3)]
            rows += [vel[f, tx, ty : ty + 1] for f in range(3)]
            rows += [jnp.where(live, 1.0, 0.0), none]
            rows += [cot_pos[f, tx, ty : ty + 1] for f in range(3)]
            rows += [cot_vel[f, tx, ty : ty + 1] for f in range(3)]
            columns.append(jnp.concatenate(rows + [none, none], axis=0))
        parts[0][ty] = jnp.where(swap, columns[1], columns[0])
        parts[1][ty] = jnp.where(swap, columns[0], columns[1])


def spread_row(row):
    padded = jnp.concatenate([row, jnp.zeros((LANES - 1, 2 * LANES), jnp.float32)], axis=0)
    return jnp.broadcast_to(padded.T[:, 0:1], (2 * LANES, LANES))


def prepare_kernel(exchange, first, second, state, carried, lam, rank_ref):
    shape = (2 * LANES, LANES)
    slot = lax.broadcasted_iota(jnp.int32, shape, 0)
    lane = lax.broadcasted_iota(jnp.int32, shape, 1)
    swap = exchange.at_odd()
    for t in range(4):
        near, other = (first, second) if t < 2 else (second, first)
        value = jnp.where(swap, other[t % 2], near[t % 2])
        key = jnp.where(value[6:7] > 0.5, value[2:3], BEYOND)
        keys = spread_row(key)
        ranks = []
        for lb in range(2):
            mine = key[:, lb * LANES : (lb + 1) * LANES]
            ahead = (keys < mine) | ((keys == mine) & (slot < lane + lb * LANES))
            ranks.append(jnp.sum(jnp.where(ahead, 1.0, 0.0), axis=0, keepdims=True))
        rank = jnp.concatenate(ranks, axis=1)
        rank_ref[t] = rank.astype(jnp.int32)
        went = spread_row(rank)
        turned = [[], []]
        for lb in range(2):
            hit = went == (lane + lb * LANES).astype(jnp.float32)
            source = jnp.sum(
                jnp.where(hit, slot.astype(jnp.float32), 0.0), axis=0, keepdims=True
            ).astype(jnp.int32)
            for part in range(2):
                rows = value[part * FEATS : (part + 1) * FEATS]
                turned[part].append(take_lanes([rows[:, :LANES], rows[:, LANES:]], source))
        own, cots = [jnp.concatenate(halves, axis=1) for halves in turned]
        row = lax.broadcasted_iota(jnp.int32, own.shape, 0)
        state[t] = jnp.where(row == 1, own + float(t), own)
        grad_pos = [cots[f : f + 1] for f in range(3)]
        grad_vel = [cots[3 + f : 4 + f] + time_step * cots[f : f + 1] for f in range(3)]
        carried[t] = stack_rows(grad_pos + grad_vel)
        lam[t] = stack_rows([time_step * own[6:7] * g for g in grad_vel], LAM_ROWS)


def restore_kernel(exchange, rank_ref, carried, *parts):
    swap = exchange.at_odd()
    tiles = []
    for t in range(4):
        value = carried[t]
        halves = [
            take_lanes(
                [value[:, :LANES], value[:, LANES:]], rank_ref[t, :, lb * LANES : (lb + 1) * LANES]
            )
            for lb in range(2)
        ]
        value = jnp.concatenate(halves, axis=1)
        rows = [value[f : f + 1] for f in range(3)]
        rows += [value[3 + f : 4 + f] - time_step * value[f : f + 1] for f in range(3)]
        tiles.append(stack_rows(rows))
    for ty in range(2):
        parts[0][ty] = jnp.where(swap, tiles[2 + ty], tiles[ty])
        parts[1][ty] = jnp.where(swap, tiles[ty], tiles[2 + ty])


def plan_kernel(exchange, order, *refs):
    pieces, (counts, padded, bias) = refs[:4], refs[4:]
    rows = []
    for kind, piece in enumerate(pieces):
        for t in range(piece.shape[0]):
            rows.append(piece[t][6:7])
            if kind == 0:
                counts[t] = jnp.sum(rows[-1]).astype(jnp.int32)
    total = jnp.sum(sum(rows)).astype(jnp.int32)
    counts[4] = total
    far_row = jnp.where(exchange.at_low(), 4, -1)
    lane = lax.broadcasted_iota(jnp.int32, (1, LANES), 1)
    for at in range(BLOCKS + PAD):
        if at >= BLOCKS:
            padded[at] = jnp.zeros((1, LANES), jnp.int32)
            for t in range(4):
                bias[t, at] = jnp.full((1, LANES), -NEVER, jnp.float32)
            continue
        places = order[at]
        padded[at] = places
        tile = places >> (LANE_BITS + 1)
        row_y = jnp.where(tile >= 10, tile - 10, jnp.where(tile >= 5, tile - 5, tile))
        row_y = jnp.where(row_y == 4, far_row, row_y)
        held = lane + at * LANES < total
        for t in range(4):
            near = (row_y >= t - 1) & (row_y <= t + 1) & held
            bias[t, at] = jnp.where(near, 1.0, -NEVER)


def spread_kernel(features, block, columns):
    each_tile(lambda t: spread_columns(columns, t, ((block[t], tuple(range(features))),)))


def fetch_table(table, table_ref, sem):
    copy = pltpu.make_async_copy(table, table_ref, sem)
    copy.start()
    return copy, table[...][0, COUNTS_AT + 4]


def merge_kernel(pack, table_ref, order_ref, *refs):
    pieces, (merged, region) = refs[:4], refs[4:]
    fill_region(region, pieces, pack)
    merge_region(merged, region, order_ref, table_ref[0, COUNTS_AT + 4], pack)


def density_kernel(exchange, counts_ref, order_ref, bias_ref, *refs):
    columns, pieces = refs[0], refs[1:5]
    out, merged, table, region, sums, table_ref = refs[5:]
    fill_region(region, pieces, 1, jnp.where(exchange.at_low(), 4.0, -4.0))
    merge_region(merged, region, order_ref, counts_ref[4], 1)
    block_ranges(table, merged, pieces[0], counts_ref)
    words = table[...]
    for index in range(COUNTS_AT):
        table_ref[0, index] = words[0, index]
    for index in range(5):
        table_ref[0, COUNTS_AT + index] = counts_ref[index]

    def body(column, t):
        def terms(block):
            d, q = separation(column, merged, bias_ref, t, block)
            return [q * q * q]

        return terms

    own = [(columns, f) for f in range(3)]
    pair_sums(table_ref, own, sums, 1, 4, body)

    def finish(t):
        live = pieces[0][t][6:7] > 0.5
        density = particle_mass * row_sums(sums, t, 1)[0]
        padded = jnp.where(live, density, 1.0)
        inverse = jnp.where(live, 1.0 / padded, 0.0)
        coefficient = jnp.where(
            live, (PUSH * stiffness) * (density / rest_density - 1.0) / (padded * padded), 0.0
        )
        out[t] = stack_rows([coefficient, inverse], PRESS_ROWS)

    each_tile(finish, unroll=True)


def accel_kernel(table, order_ref, bias_ref, merged, columns, press_columns, state, *refs):
    press, (out, merged_p, region, sums, table_ref, sem) = refs[:4], refs[4:]
    copy, total = fetch_table(table, table_ref, sem)
    fill_region(region, press, 4)
    merge_region(merged_p, region, order_ref, total, 4)
    copy.wait()

    def body(column, t):
        xi, vi, ci = column[:3], column[3:6], column[6]

        def terms(block):
            d, q = separation(xi, merged, bias_ref, t, block)
            q2 = q * q
            visc = q2 * q * merged_p[block, 1:2, :]
            push = (ci + merged_p[block, 0:1, :]) * q2
            dv = [merged[block, 3 + f : 4 + f, :] - vi[f] for f in range(3)]
            return [visc * dv[f] - push * d[f] for f in range(3)]

        return terms

    own = [(columns, f) for f in range(6)] + [(press_columns, 0)]
    pair_sums(table_ref, own, sums, 3, 3, body)

    def finish(t):
        own = state[t]
        live = own[6:7] > 0.5
        s = row_sums(sums, t, 3)
        new_pos, new_vel = [], []
        for f in range(3):
            vel = own[3 + f : 4 + f]
            accel = (particle_mass * viscosity) * s[f]
            vel = jnp.where(live, vel + time_step * accel, vel)
            new_vel.append(vel)
            new_pos.append(
                jnp.where(live, own[f : f + 1] + time_step * vel, own[f : f + 1])
            )
        out[t] = stack_rows(new_pos + new_vel + [own[6:7]])

    each_tile(finish, unroll=True)


def density_grad_kernel(
    table, order_ref, bias_ref, merged, columns, lam_columns, state, press, *refs
):
    lam, (out, merged_l, region, sums, table_ref, sem) = refs[:4], refs[4:]
    copy, total = fetch_table(table, table_ref, sem)
    fill_region(region, lam, 2)
    merge_region(merged_l, region, order_ref, total, 2)
    copy.wait()

    def body(column, t):
        xi, vi, li = column[:3], column[3:6], column[6:]

        def terms(block):
            d, q = separation(xi, merged, bias_ref, t, block)
            lj = [merged_l[block, f : f + 1, :] for f in range(3)]
            q2 = q * q
            along = sum((li[f] - lj[f]) * d[f] for f in range(3))
            moved = sum(lj[f] * (vi[f] - merged[block, 3 + f : 4 + f, :]) for f in range(3))
            return [q2 * along, q2 * q * moved]

        return terms

    own = [(columns, f) for f in range(6)] + [(lam_columns, f) for f in range(3)]
    pair_sums(table_ref, own, sums, 2, 3, body)

    def finish(t):
        live = state[t][6:7] > 0.5
        s = row_sums(sums, t, 2)
        c = press[t][0:1] * (1.0 / PUSH)
        w = press[t][1:2]
        grad_c = (-6.0 * particle_mass) * s[0]
        grad_w = (viscosity * particle_mass) * s[1]
        grad = grad_c * (stiffness * w * w - 2.0 * c * w) - grad_w * w * w
        out[t] = jnp.where(live, grad, 0.0)

    each_tile(finish, unroll=True)


def main_grad_kernel(share, table_ref, bias_ref, merged, merged_p, merged_l, *refs):
    columns, lam_columns, press_columns = refs[:3]
    sums = refs[3] if share == 0 else refs[5]

    def body(column, t):
        xi, vi, li = column[:3], column[3:6], column[6:9]
        ci, wi = column[9:]

        def terms(block):
            d, q = separation(xi, merged, bias_ref, t, block)
            lj = [merged_l[block, f : f + 1, :] for f in range(3)]
            wj = merged_p[block, 1:2, :]
            cs = ci + merged_p[block, 0:1, :]
            diff = [li[f] - lj[f] for f in range(3)]
            drags = [wj * li[f] - wi * lj[f] for f in range(3)]
            drag = sum(
                drags[f] * (merged[block, 3 + f : 4 + f, :] - vi[f]) for f in range(3)
            )
            along = sum(diff[f] * d[f] for f in range(3))
            q2 = q * q
            q3 = q2 * q
            on_d = q * (q * drag - (8.0 / PUSH) * (cs * along))
            on_l = (cs * q2) * (2.0 / PUSH)
            gx = [on_d * d[f] + on_l * diff[f] for f in range(3)]
            gv = [q3 * drags[f] for f in range(3)]
            return gx + gv

        return terms

    own = [(columns, f) for f in range(6)] + [(lam_columns, f) for f in range(3)]
    own += [(press_columns, f) for f in range(2)]
    pair_sums(table_ref, own, sums, 6, 2, body, share=share)

    if share == 0:
        return
    before, out = refs[3:5]
    slot = lax.broadcasted_iota(jnp.int32, (2 * LANES, LANES), 0)

    def finish(t):
        groups = (table_ref[0, COUNTS_AT + t] + (ROWS - 1)) // ROWS
        done = slot < first_share(groups) * ROWS
        s = [
            jnp.sum(jnp.where(done, before[f, t], sums[f, t]).T, axis=0, keepdims=True)
            for f in range(6)
        ]
        rows = [(3.0 * particle_mass) * s[f] for f in range(3)]
        rows += [(-viscosity * particle_mass) * s[3 + f] for f in range(3)]
        out[t] = stack_rows(rows)

    each_tile(finish)


def last_grad_kernel(table, order_ref, bias_ref, merged, places, state, *refs):
    grads, partial, carried = refs[:4], refs[4], refs[5]
    lam_out, carried_out, region, merged_g, columns, sums, table_ref, sem = refs[6:]
    copy, total = fetch_table(table, table_ref, sem)
    fill_region(region, grads, 8)
    merge_region(merged_g, region, order_ref, total, 8)
    each_tile(
        lambda t: spread_columns(columns, t, ((grads[0][t], (0,)),)), unroll=True
    )
    copy.wait()

    def body(column, t):
        xi, gi = column[:3], column[3]

        def terms(block):
            d, q = separation(xi, merged, bias_ref, t, block)
            weight = (gi + merged_g[block, 0:1, :]) * (q * q)
            return [weight * d[f] for f in range(3)]

        return terms

    own = [(places, f) for f in range(3)] + [(columns, 0)]
    pair_sums(table_ref, own, sums, 3, 4, body)

    def finish(t):
        live = state[t][6:7] > 0.5
        s = row_sums(sums, t, 3)
        part = partial[t]
        old = carried[t]
        new_pos, new_vel = [], []
        for f in range(3):
            extra = part[f : f + 1] + (6.0 * particle_mass) * s[f]
            gx = old[f : f + 1] + jnp.where(live, extra, 0.0)
            gv = old[3 + f : 4 + f] + jnp.where(live, part[3 + f : 4 + f], 0.0)
            new_pos.append(gx)
            new_vel.append(gv + time_step * gx)
        lam_out[t] = stack_rows([jnp.where(live, time_step * v, 0.0) for v in new_vel], LAM_ROWS)
        carried_out[t] = stack_rows(new_pos + new_vel)

    each_tile(finish, unroll=True)


def tiles_of(rows, tiles=4):
    return jax.ShapeDtypeStruct((tiles, rows, 2 * LANES), jnp.float32)


TILES = tiles_of(FEATS)
MERGED = jax.ShapeDtypeStruct((BLOCKS + PAD, FEATS, LANES), jnp.float32)
TABLE = jax.ShapeDtypeStruct((1, LANES), jnp.int32)
TABLE_COPY = [pltpu.SMEM(TABLE.shape, jnp.int32), pltpu.SemaphoreType.DMA]


def wide(count, tiles=4):
    return jax.ShapeDtypeStruct((count, tiles, 2 * LANES, LANES), jnp.float32)


def vmem_like(shape):
    return pltpu.VMEM(shape.shape, shape.dtype)


def packed_region(pack):
    return pltpu.VMEM((-(-BLOCKS // pack), FEATS, LANES), jnp.float32)


def run_kernel(kernel, name, scalars, arrays, out_shape, scratch, cycles, scalar_outputs=0, anywhere=False):
    smem = pl.BlockSpec(memory_space=pltpu.SMEM)
    vmem = pl.BlockSpec(memory_space=pltpu.VMEM)
    result = pl.pallas_call(
        kernel,
        name=name,
        out_shape=out_shape,
        in_specs=[smem] * len(scalars)
        + [pl.BlockSpec(memory_space=pltpu.HBM) if anywhere else vmem] * len(arrays),
        out_specs=[smem] * scalar_outputs + [vmem] * (len(out_shape) - scalar_outputs),
        scratch_shapes=scratch,
        compiler_params=pltpu.CompilerParams(
            vmem_limit_bytes=(60 << 20) if anywhere else VMEM_LIMIT
        ),
        cost_estimate=pl.CostEstimate(
            flops=cycles * 65536, bytes_accessed=1 << 18, transcendentals=0
        ),
    )(*scalars, *arrays)
    return result


def per_device(exchange, positions, velocities, occupancy, cot_positions, cot_velocities):
    slots = positions.shape[3]
    assert positions.shape[1:] == (2, 2, 2 * LANES)
    parts = run_kernel(
        functools.partial(pack_kernel, exchange),
        "pack",
        (occupancy,),
        (positions, velocities, cot_positions, cot_velocities),
        [tiles_of(2 * FEATS, 2)] * 2,
        [pltpu.VMEM(positions.shape, jnp.float32)] * 4 + [pltpu.SemaphoreType.DMA((4,))],
        500,
        anywhere=True,
    )
    parts = exchange.place(parts)
    state, carried, lam, rank = run_kernel(
        functools.partial(prepare_kernel, exchange),
        "prepare",
        (),
        tuple(parts),
        [TILES, TILES, tiles_of(LAM_ROWS), jax.ShapeDtypeStruct((4, 1, slots), jnp.int32)],
        [],
        1000,
    )

    pieces = exchange.halo(state)
    own, x_low, x_high, far = [piece[:, 2:7:4] for piece in pieces]
    around = jnp.stack([x_low, own, x_high])
    around = jnp.concatenate([around, far[:, None]], axis=1)
    present = around[:, :, 1] > 0.5
    place_bits = (BLOCKS * LANES - 1).bit_length()
    deepest = (1 << (31 - place_bits)) - 1
    depth = jnp.clip(around[:, :, 0] * float((deepest + 1) // 16), 0.0, deepest - 1.0)
    depth = jnp.where(present, depth.astype(jnp.int32), deepest).reshape(-1)
    depth = jnp.minimum(depth, jnp.where(present.reshape(-1), deepest - 1, deepest))
    place = lax.broadcasted_iota(jnp.int32, depth.shape, 0)
    order = lax.sort((depth << place_bits) | place, is_stable=False) & ((1 << place_bits) - 1)
    counts, order, bias = run_kernel(
        functools.partial(plan_kernel, exchange),
        "plan",
        (),
        (order.reshape(BLOCKS, 1, LANES),) + pieces,
        [
            jax.ShapeDtypeStruct((8,), jnp.int32),
            jax.ShapeDtypeStruct((BLOCKS + PAD, 1, LANES), jnp.int32),
            jax.ShapeDtypeStruct((4, BLOCKS + PAD, 1, LANES), jnp.float32),
        ],
        [],
        500,
        scalar_outputs=1,
    )

    def spread(value, features, name):
        return run_kernel(
            functools.partial(spread_kernel, features), name, (), (value,), [wide(features)], [], 2000
        )[0]

    saved = []
    columns = spread(state, 6, "spread_state")
    for step in range(STEPS):
        if step > 0:
            pieces, columns = exchange.halo(state, beside=spread(state, 6, "spread_state"))
        own_press, merged, table = run_kernel(
            functools.partial(density_kernel, exchange),
            "density",
            (counts,),
            (order, bias, columns) + pieces,
            [tiles_of(PRESS_ROWS), MERGED, TABLE],
            [
                packed_region(1),
                vmem_like(wide(1)),
                pltpu.SMEM(TABLE.shape, jnp.int32),
            ],
            8000,
        )
        press, press_columns = exchange.halo(
            own_press, beside=spread(own_press, 2, "spread_press")
        )
        if step + 1 < STEPS:
            new_state, merged_p = run_kernel(
                accel_kernel,
                "accel",
                (),
                (table, order, bias, merged, columns, press_columns, state) + press,
                [TILES, MERGED],
                [packed_region(4), vmem_like(wide(3))] + TABLE_COPY,
                10000,
            )
        else:
            new_state = state
            (merged_p,) = run_kernel(
                functools.partial(merge_kernel, 4),
                "merge",
                (table,),
                (order,) + press,
                [MERGED],
                [packed_region(4)],
                2000,
            )
        saved.append((state, own_press, table, merged, merged_p, columns, press_columns))
        state = new_state

    for step in reversed(range(STEPS)):
        state, own_press, table, merged, merged_p, columns, press_columns = saved[step]
        lam_pieces, lam_columns = exchange.halo(lam, beside=spread(lam, 3, "spread_lam"))
        own_grad, merged_l = run_kernel(
            density_grad_kernel,
            "density_grad",
            (),
            (table, order, bias, merged, columns, lam_columns, state, own_press) + lam_pieces,
            [tiles_of(1), MERGED],
            [packed_region(2), vmem_like(wide(2))] + TABLE_COPY,
            10000,
        )
        pairs = (bias, merged, merged_p, merged_l, columns, lam_columns, press_columns)
        (sums,) = run_kernel(
            functools.partial(main_grad_kernel, 0),
            "main_grad_0",
            (table,),
            pairs,
            [wide(6)],
            [],
            10000,
        )
        grad_pieces, sums = exchange.halo(own_grad, beside=sums)
        (partial,) = run_kernel(
            functools.partial(main_grad_kernel, 1),
            "main_grad_1",
            (table,),
            pairs + (sums,),
            [TILES],
            [vmem_like(wide(6))],
            10000,
        )
        lam, carried = run_kernel(
            last_grad_kernel,
            "last_grad",
            (),
            (table, order, bias, merged, columns, state) + grad_pieces + (partial, carried),
            [tiles_of(LAM_ROWS), TILES],
            [packed_region(8), vmem_like(MERGED), vmem_like(wide(1)), vmem_like(wide(3))]
            + TABLE_COPY,
            8000,
        )

    parts = run_kernel(
        functools.partial(restore_kernel, exchange),
        "restore",
        (),
        (rank, carried),
        [tiles_of(FEATS, 2)] * 2,
        [],
        500,
    )
    parts = exchange.unplace(parts)
    swap = lax.axis_index("gy") % 2 == 1
    grads = jnp.stack([jnp.where(swap, parts[1], parts[0]), jnp.where(swap, parts[0], parts[1])])
    grads = jnp.moveaxis(grads, 2, 0)
    return (grads[:3], grads[3:6])


def solution(mesh):
    spec = P(None, "gx", "gy", None)
    exchange = Exchange(mesh)
    return jax.shard_map(
        functools.partial(per_device, exchange),
        mesh=mesh,
        in_specs=(spec, spec, P("gx", "gy"), spec, spec),
        out_specs=(spec, spec),
        check_vma=False,
    )
```

```python
import functools

import jax
import jax.numpy as jnp
from jax import lax
from jax.experimental import pallas as pl
from jax.experimental.pallas import tpu as pltpu
from jax.sharding import PartitionSpec as P

STEPS = 4
time_step = 0.05
stiffness = 4.0
rest_density = 1.0
particle_mass = 0.15
viscosity = 0.5


FAR = 1.0e4
BEYOND = 1.0e5
ROWS = 16
LANES = 128
FEATS = 8
LANE_BITS = LANES.bit_length() - 1
PUSH = 12.0
PRESS_ROWS = 2
COUNTS_AT = 64
LAM_ROWS = 4
VMEM_LIMIT = 12 << 20
BLOCKS = 30
PAD = 4
MERGE = 4
REACH = 1.001
NEVER = 1.0e30


def closed_ring(count):
    assert count % 2 == 0
    levels = count // 2
    up = []
    for level in range(levels):
        three = [(2 * level, 0), (2 * level, 1), (2 * level + 1, 1)]
        up += three if level % 2 == 0 else three[::-1]
    down = [(2 * level + 1, 0) for level in range(levels)][::-1]
    return down[-1:] + up + down[:-1]


class Exchange:
    def __init__(self, mesh):
        self.count_x = mesh.shape["gx"]
        self.count_y = mesh.shape["gy"]
        assert self.count_y == 4
        self.ring = closed_ring(self.count_x)

    def device(self, column, half):
        a, line = self.ring[column % len(self.ring)]
        return a * self.count_y + line * 2 + half

    def permute(self, value, pairs):
        return lax.ppermute(value, ("gx", "gy"), pairs)

    def at_odd(self):
        a, b = lax.axis_index("gx"), lax.axis_index("gy")
        odd = jnp.bool_(False)
        for column, (level, line) in enumerate(self.ring):
            if column % 2 == 1:
                odd = odd | ((a == level) & (b // 2 == line))
        return odd

    def at_low(self):
        return lax.axis_index("gy") % 2 == 0

    def from_ring(self, value, step):
        pairs = [
            (self.device(column + step, half), self.device(column, half))
            for column in range(len(self.ring))
            for half in range(2)
        ]
        return self.permute(value, pairs)

    def from_other_half(self, value):
        pairs = [
            (self.device(column, 1 - half), self.device(column, half))
            for column in range(len(self.ring))
            for half in range(2)
        ]
        return self.permute(value, pairs)

    def routes(self, flip):
        return [
            (a * self.count_y + b, self.device(2 * a + (b + flip) % 2, b // 2))
            for a in range(self.count_x)
            for b in range(self.count_y)
        ]

    def place(self, parts):
        return [self.permute(part, self.routes(flip)) for flip, part in enumerate(parts)]

    def unplace(self, parts):
        return [
            self.permute(part, [(target, source) for source, target in self.routes(flip)])
            for flip, part in enumerate(parts)
        ]

    def halo(self, own, beside=None):
        x_low = self.from_ring(own, -1)
        x_high = self.from_ring(own, 1)
        if beside is not None:
            x_low, x_high, beside = lax.optimization_barrier((x_low, x_high, beside))
        at_low = self.at_low()
        edges = jnp.stack([jnp.where(at_low, part[3], part[0]) for part in (x_low, own, x_high)])
        pieces = (own, x_low, x_high, self.from_other_half(edges))
        return pieces if beside is None else (pieces, beside)


def fill_region(region, pieces, pack, shift=None):
    own, x_low, x_high, far = pieces
    kept = FEATS // pack
    row = lax.broadcasted_iota(jnp.int32, (FEATS, 2 * LANES), 0)
    for rx in range(3):
        for ry in range(5):
            block = far[rx] if ry == 4 else (x_low, own, x_high)[rx][ry]
            if shift is not None:
                if rx != 1:
                    block = jnp.where(row == 0, block + (rx - 1.0), block)
                if ry == 4:
                    block = jnp.where(row == 1, block + shift, block)
            for lb in range(2):
                at = (rx * 5 + ry) * 2 + lb
                inside = (at % pack) * kept
                region[at // pack, inside : inside + kept] = block[
                    :kept, lb * LANES : (lb + 1) * LANES
                ]


def each_tile(work, tiles=4, unroll=False):
    if unroll:
        for t in range(tiles):
            work(t)
        return

    def step(t, carry):
        work(t)
        return carry

    lax.fori_loop(0, tiles, step, 0)


def spread_columns(columns, t, values):
    at = 0
    for block, chosen in values:
        padded = jnp.concatenate(
            [block, jnp.zeros((LANES - block.shape[0], 2 * LANES), jnp.float32)], axis=0
        )
        turned = padded.T
        for index, feature in enumerate(chosen):
            columns[at + index, t] = jnp.broadcast_to(
                turned[:, feature : feature + 1], (2 * LANES, LANES)
            )
        at += len(chosen)


def take_lanes(sources, row, pack=1):
    shape = (FEATS, LANES)
    lane = jnp.broadcast_to(row & (LANES - 1), shape)
    block = jnp.broadcast_to(row >> LANE_BITS, shape)
    vector = block // pack if pack > 1 else block
    picked = jnp.zeros(shape, jnp.float32)
    for at, source in enumerate(sources):
        picked = jnp.where(vector == at, jnp.take_along_axis(source, lane, axis=1), picked)
    if pack == 1:
        return picked
    inside = block & (pack - 1)
    result = picked
    for at in range(1, pack):
        shifted = pltpu.roll(picked, FEATS - at * (FEATS // pack), 0)
        result = jnp.where(inside == at, shifted, result)
    return result


def merge_region(merged, region, order_ref, total, pack):
    for at in range(BLOCKS + PAD):
        merged[at] = jnp.zeros((FEATS, LANES), jnp.float32)
    used = (total + (LANES - 1)) >> LANE_BITS

    def step(index, carry):
        for near in range(MERGE):
            at = index * MERGE + near
            sources = [region[s] for s in range(-(-BLOCKS // pack))]
            merged[at] = take_lanes(sources, order_ref[at], pack)
        return carry

    lax.fori_loop(0, (used + (MERGE - 1)) // MERGE, step, 0)


def block_ranges(table, merged, own, counts_ref):
    depth = merged[:BLOCKS, 2, :]
    rank = lax.broadcasted_iota(jnp.int32, (BLOCKS, LANES), 0) * LANES
    rank = rank + lax.broadcasted_iota(jnp.int32, (BLOCKS, LANES), 1)
    held = rank < counts_ref[4]
    least = jnp.min(jnp.where(held, depth, BEYOND), axis=1, keepdims=True)
    most = jnp.max(jnp.where(held, depth, -BEYOND), axis=1, keepdims=True)
    rows, limits = [], []
    for t in range(4):
        for lb in range(2):
            rows.append(own[t][2:3, lb * LANES : (lb + 1) * LANES])
            lane = lax.broadcasted_iota(jnp.int32, (1, LANES), 1) + lb * LANES
            limits.append((lane < counts_ref[t]).astype(jnp.float32))
    mine = jnp.concatenate(rows, axis=0)
    inside = jnp.concatenate(limits, axis=0) > 0.5
    low = jnp.where(inside, mine, BEYOND)
    high = jnp.where(inside, mine, -BEYOND)
    reach = 1
    while reach < ROWS:
        low = jnp.minimum(low, pltpu.roll(low, LANES - reach, 1))
        high = jnp.maximum(high, pltpu.roll(high, LANES - reach, 1))
        reach *= 2
    low = low - REACH
    high = high + REACH
    first = jnp.full((FEATS, LANES), BLOCKS, jnp.int32)
    past = jnp.zeros((FEATS, LANES), jnp.int32)
    for at in range(BLOCKS):
        near = (jnp.broadcast_to(most[at : at + 1], (FEATS, LANES)) >= low) & (
            jnp.broadcast_to(least[at : at + 1], (FEATS, LANES)) <= high
        )
        first = jnp.where(near, jnp.minimum(first, at), first)
        past = jnp.where(near, at + 1, past)
    length = jnp.maximum(past - first, 0)
    word = jnp.minimum(first, BLOCKS - 1)
    for together in range(2, 5):
        trips = jnp.zeros((FEATS, LANES), jnp.int32)
        for least_length in range(1, BLOCKS + 1, together):
            trips = jnp.where(length >= least_length, trips + 1, trips)
        word = word | (trips << (8 * (together - 1)))
    per_line = LANES // ROWS
    lane = lax.broadcasted_iota(jnp.int32, (FEATS, LANES), 1)
    line = lax.broadcasted_iota(jnp.int32, (FEATS, LANES), 0)
    word = jnp.take_along_axis(word, (lane & (per_line - 1)) * ROWS, axis=1)
    word = jnp.where(lane // per_line == line, word, 0)
    for shift in (4, 2, 1):
        word = word + pltpu.roll(word, shift, 0)
    for index in range(5):
        word = jnp.where(lane == COUNTS_AT + index, counts_ref[index], word)
    table[...] = word[0:1]


def pair_sums(table_ref, columns, sums_ref, outputs, together, body, tiles=(0, 4)):
    row_bits = ROWS.bit_length() - 1
    per_tile = 2 * LANES // ROWS

    def tile_loop(t, carry):
        groups = (table_ref[0, COUNTS_AT + t] + (ROWS - 1)) >> row_bits

        def group_loop(g, carry):
            start = pl.multiple_of(g << row_bits, ROWS)
            terms_of = body([ref[f, t, pl.ds(start, ROWS), :] for ref, f in columns], t)
            word = table_ref[0, t * per_tile + g]
            first = word & 31
            trips = (word >> (8 * (together - 1))) & 31

            def block_loop(index, totals):
                totals = list(totals)
                for near in range(together):
                    terms = terms_of(first + index * together + near)
                    totals = [a + b for a, b in zip(totals, terms)]
                return tuple(totals)

            zero = jnp.zeros((ROWS, LANES), jnp.float32)
            totals = lax.fori_loop(0, trips, block_loop, (zero,) * outputs)
            for index, total in enumerate(totals):
                sums_ref[index, t - tiles[0], pl.ds(start, ROWS), :] = total
            return carry

        return lax.fori_loop(0, groups, group_loop, carry)

    lax.fori_loop(*tiles, tile_loop, 0)


def row_sums(sums_ref, t, outputs):
    return [jnp.sum(sums_ref[index, t].T, axis=0, keepdims=True) for index in range(outputs)]


def separation(xi, merged, bias_ref, t, block):
    d = [merged[block, f : f + 1, :] - xi[f] for f in range(3)]
    bias = bias_ref[t, block]
    q = jnp.maximum(bias - d[0] * d[0] - d[1] * d[1] - d[2] * d[2], 0.0)
    return d, q


def stack_rows(rows, height=FEATS):
    width = rows[0].shape[1]
    rows = list(rows) + [jnp.zeros((1, width), jnp.float32)] * (height - len(rows))
    return jnp.concatenate(rows, axis=0)


def pack_kernel(exchange, held_ref, *refs):
    inputs, parts, held, sems = refs[:4], refs[4:6], refs[6:10], refs[10]
    copies = [
        pltpu.make_async_copy(source, target, sems.at[index])
        for index, (source, target) in enumerate(zip(inputs, held))
    ]
    for copy in copies:
        copy.start()
    for copy in copies:
        copy.wait()
    pos, vel, cot_pos, cot_vel = held
    lane = lax.broadcasted_iota(jnp.int32, (1, 2 * LANES), 1)
    none = jnp.zeros((1, 2 * LANES), jnp.float32)
    swap = lax.axis_index("gy") % 2 == 1
    for ty in range(2):
        columns = []
        for tx in range(2):
            live = lane < held_ref[tx, ty]
            rows = [jnp.where(live, pos[f, tx, ty : ty + 1], FAR) for f in range(3)]
            rows += [vel[f, tx, ty : ty + 1] for f in range(3)]
            rows += [jnp.where(live, 1.0, 0.0), none]
            rows += [cot_pos[f, tx, ty : ty + 1] for f in range(3)]
            rows += [cot_vel[f, tx, ty : ty + 1] for f in range(3)]
            columns.append(jnp.concatenate(rows + [none, none], axis=0))
        parts[0][ty] = jnp.where(swap, columns[1], columns[0])
        parts[1][ty] = jnp.where(swap, columns[0], columns[1])


def spread_row(row):
    padded = jnp.concatenate([row, jnp.zeros((LANES - 1, 2 * LANES), jnp.float32)], axis=0)
    return jnp.broadcast_to(padded.T[:, 0:1], (2 * LANES, LANES))


def prepare_kernel(exchange, first, second, state, carried, lam, rank_ref):
    shape = (2 * LANES, LANES)
    slot = lax.broadcasted_iota(jnp.int32, shape, 0)
    lane = lax.broadcasted_iota(jnp.int32, shape, 1)
    swap = exchange.at_odd()
    for t in range(4):
        near, other = (first, second) if t < 2 else (second, first)
        value = jnp.where(swap, other[t % 2], near[t % 2])
        key = jnp.where(value[6:7] > 0.5, value[2:3], BEYOND)
        keys = spread_row(key)
        ranks = []
        for lb in range(2):
            mine = key[:, lb * LANES : (lb + 1) * LANES]
            ahead = (keys < mine) | ((keys == mine) & (slot < lane + lb * LANES))
            ranks.append(jnp.sum(jnp.where(ahead, 1.0, 0.0), axis=0, keepdims=True))
        rank = jnp.concatenate(ranks, axis=1)
        rank_ref[t] = rank.astype(jnp.int32)
        went = spread_row(rank)
        turned = [[], []]
        for lb in range(2):
            hit = went == (lane + lb * LANES).astype(jnp.float32)
            source = jnp.sum(
                jnp.where(hit, slot.astype(jnp.float32), 0.0), axis=0, keepdims=True
            ).astype(jnp.int32)
            for part in range(2):
                rows = value[part * FEATS : (part + 1) * FEATS]
                turned[part].append(take_lanes([rows[:, :LANES], rows[:, LANES:]], source))
        own, cots = [jnp.concatenate(halves, axis=1) for halves in turned]
        row = lax.broadcasted_iota(jnp.int32, own.shape, 0)
        state[t] = jnp.where(row == 1, own + float(t), own)
        grad_pos = [cots[f : f + 1] for f in range(3)]
        grad_vel = [cots[3 + f : 4 + f] + time_step * cots[f : f + 1] for f in range(3)]
        carried[t] = stack_rows(grad_pos + grad_vel)
        lam[t] = stack_rows([time_step * own[6:7] * g for g in grad_vel], LAM_ROWS)


def restore_kernel(exchange, rank_ref, carried, *parts):
    swap = exchange.at_odd()
    tiles = []
    for t in range(4):
        value = carried[t]
        halves = [
            take_lanes(
                [value[:, :LANES], value[:, LANES:]], rank_ref[t, :, lb * LANES : (lb + 1) * LANES]
            )
            for lb in range(2)
        ]
        value = jnp.concatenate(halves, axis=1)
        rows = [value[f : f + 1] for f in range(3)]
        rows += [value[3 + f : 4 + f] - time_step * value[f : f + 1] for f in range(3)]
        tiles.append(stack_rows(rows))
    for ty in range(2):
        parts[0][ty] = jnp.where(swap, tiles[2 + ty], tiles[ty])
        parts[1][ty] = jnp.where(swap, tiles[ty], tiles[2 + ty])


def plan_kernel(exchange, order, *refs):
    pieces, (counts, padded, bias) = refs[:4], refs[4:]
    rows = []
    for kind, piece in enumerate(pieces):
        for t in range(piece.shape[0]):
            rows.append(piece[t][6:7])
            if kind == 0:
                counts[t] = jnp.sum(rows[-1]).astype(jnp.int32)
    total = jnp.sum(sum(rows)).astype(jnp.int32)
    counts[4] = total
    far_row = jnp.where(exchange.at_low(), 4, -1)
    lane = lax.broadcasted_iota(jnp.int32, (1, LANES), 1)
    for at in range(BLOCKS + PAD):
        if at >= BLOCKS:
            padded[at] = jnp.zeros((1, LANES), jnp.int32)
            for t in range(4):
                bias[t, at] = jnp.full((1, LANES), -NEVER, jnp.float32)
            continue
        places = order[at]
        padded[at] = places
        tile = places >> (LANE_BITS + 1)
        row_y = jnp.where(tile >= 10, tile - 10, jnp.where(tile >= 5, tile - 5, tile))
        row_y = jnp.where(row_y == 4, far_row, row_y)
        held = lane + at * LANES < total
        for t in range(4):
            near = (row_y >= t - 1) & (row_y <= t + 1) & held
            bias[t, at] = jnp.where(near, 1.0, -NEVER)


def spread_kernel(features, block, columns):
    each_tile(lambda t: spread_columns(columns, t, ((block[t], tuple(range(features))),)))


def fetch_table(table, table_ref, sem):
    copy = pltpu.make_async_copy(table, table_ref, sem)
    copy.start()
    return copy, table[...][0, COUNTS_AT + 4]


def merge_kernel(pack, table_ref, order_ref, *refs):
    pieces, (merged, region) = refs[:4], refs[4:]
    fill_region(region, pieces, pack)
    merge_region(merged, region, order_ref, table_ref[0, COUNTS_AT + 4], pack)


def density_kernel(exchange, counts_ref, order_ref, bias_ref, *refs):
    columns, pieces = refs[0], refs[1:5]
    out, merged, table, region, sums, table_ref = refs[5:]
    fill_region(region, pieces, 1, jnp.where(exchange.at_low(), 4.0, -4.0))
    merge_region(merged, region, order_ref, counts_ref[4], 1)
    block_ranges(table, merged, pieces[0], counts_ref)
    words = table[...]
    for index in range(COUNTS_AT):
        table_ref[0, index] = words[0, index]
    for index in range(5):
        table_ref[0, COUNTS_AT + index] = counts_ref[index]

    def body(column, t):
        def terms(block):
            d, q = separation(column, merged, bias_ref, t, block)
            return [q * q * q]

        return terms

    own = [(columns, f) for f in range(3)]
    pair_sums(table_ref, own, sums, 1, 4, body)

    def finish(t):
        live = pieces[0][t][6:7] > 0.5
        density = particle_mass * row_sums(sums, t, 1)[0]
        padded = jnp.where(live, density, 1.0)
        inverse = jnp.where(live, 1.0 / padded, 0.0)
        coefficient = jnp.where(
            live, (PUSH * stiffness) * (density / rest_density - 1.0) / (padded * padded), 0.0
        )
        out[t] = stack_rows([coefficient, inverse], PRESS_ROWS)

    each_tile(finish, unroll=True)


def accel_kernel(table, order_ref, bias_ref, merged, columns, press_columns, state, *refs):
    press, (out, merged_p, region, sums, table_ref, sem) = refs[:4], refs[4:]
    copy, total = fetch_table(table, table_ref, sem)
    fill_region(region, press, 4)
    merge_region(merged_p, region, order_ref, total, 4)
    copy.wait()

    def body(column, t):
        xi, vi, ci = column[:3], column[3:6], column[6]

        def terms(block):
            d, q = separation(xi, merged, bias_ref, t, block)
            q2 = q * q
            visc = q2 * q * merged_p[block, 1:2, :]
            push = (ci + merged_p[block, 0:1, :]) * q2
            dv = [merged[block, 3 + f : 4 + f, :] - vi[f] for f in range(3)]
            return [visc * dv[f] - push * d[f] for f in range(3)]

        return terms

    own = [(columns, f) for f in range(6)] + [(press_columns, 0)]
    pair_sums(table_ref, own, sums, 3, 3, body)

    def finish(t):
        own = state[t]
        live = own[6:7] > 0.5
        s = row_sums(sums, t, 3)
        new_pos, new_vel = [], []
        for f in range(3):
            vel = own[3 + f : 4 + f]
            accel = (particle_mass * viscosity) * s[f]
            vel = jnp.where(live, vel + time_step * accel, vel)
            new_vel.append(vel)
            new_pos.append(
                jnp.where(live, own[f : f + 1] + time_step * vel, own[f : f + 1])
            )
        out[t] = stack_rows(new_pos + new_vel + [own[6:7]])

    each_tile(finish, unroll=True)


def density_grad_kernel(
    table, order_ref, bias_ref, merged, columns, lam_columns, state, press, *refs
):
    lam, (out, merged_l, region, sums, table_ref, sem) = refs[:4], refs[4:]
    copy, total = fetch_table(table, table_ref, sem)
    fill_region(region, lam, 2)
    merge_region(merged_l, region, order_ref, total, 2)
    copy.wait()

    def body(column, t):
        xi, vi, li = column[:3], column[3:6], column[6:]

        def terms(block):
            d, q = separation(xi, merged, bias_ref, t, block)
            lj = [merged_l[block, f : f + 1, :] for f in range(3)]
            q2 = q * q
            along = sum((li[f] - lj[f]) * d[f] for f in range(3))
            moved = sum(lj[f] * (vi[f] - merged[block, 3 + f : 4 + f, :]) for f in range(3))
            return [q2 * along, q2 * q * moved]

        return terms

    own = [(columns, f) for f in range(6)] + [(lam_columns, f) for f in range(3)]
    pair_sums(table_ref, own, sums, 2, 3, body)

    def finish(t):
        live = state[t][6:7] > 0.5
        s = row_sums(sums, t, 2)
        c = press[t][0:1] * (1.0 / PUSH)
        w = press[t][1:2]
        grad_c = (-6.0 * particle_mass) * s[0]
        grad_w = (viscosity * particle_mass) * s[1]
        grad = grad_c * (stiffness * w * w - 2.0 * c * w) - grad_w * w * w
        out[t] = jnp.where(live, grad, 0.0)

    each_tile(finish, unroll=True)


def main_grad_kernel(half, table_ref, bias_ref, merged, merged_p, merged_l, *refs):
    columns, lam_columns, press_columns, out, sums = refs

    def body(column, t):
        xi, vi, li = column[:3], column[3:6], column[6:9]
        ci, wi = column[9:]

        def terms(block):
            d, q = separation(xi, merged, bias_ref, t, block)
            lj = [merged_l[block, f : f + 1, :] for f in range(3)]
            wj = merged_p[block, 1:2, :]
            cs = ci + merged_p[block, 0:1, :]
            diff = [li[f] - lj[f] for f in range(3)]
            drags = [wj * li[f] - wi * lj[f] for f in range(3)]
            drag = sum(
                drags[f] * (merged[block, 3 + f : 4 + f, :] - vi[f]) for f in range(3)
            )
            along = sum(diff[f] * d[f] for f in range(3))
            q2 = q * q
            q3 = q2 * q
            on_d = q * (q * drag - (8.0 / PUSH) * (cs * along))
            on_l = (cs * q2) * (2.0 / PUSH)
            gx = [on_d * d[f] + on_l * diff[f] for f in range(3)]
            gv = [q3 * drags[f] for f in range(3)]
            return gx + gv

        return terms

    own = [(columns, f) for f in range(6)] + [(lam_columns, f) for f in range(3)]
    own += [(press_columns, f) for f in range(2)]
    pair_sums(table_ref, own, sums, 6, 2, body, tiles=(2 * half, 2 * half + 2))

    def finish(t):
        s = row_sums(sums, t, 6)
        rows = [(3.0 * particle_mass) * s[f] for f in range(3)]
        rows += [(-viscosity * particle_mass) * s[3 + f] for f in range(3)]
        out[t] = stack_rows(rows)

    each_tile(finish, tiles=2)


def last_grad_kernel(table, order_ref, bias_ref, merged, places, state, *refs):
    grads, partials, carried = refs[:4], refs[4:6], refs[6]
    lam_out, carried_out, region, merged_g, columns, sums, table_ref, sem = refs[7:]
    copy, total = fetch_table(table, table_ref, sem)
    fill_region(region, grads, 8)
    merge_region(merged_g, region, order_ref, total, 8)
    each_tile(
        lambda t: spread_columns(columns, t, ((grads[0][t], (0,)),)), unroll=True
    )
    copy.wait()

    def body(column, t):
        xi, gi = column[:3], column[3]

        def terms(block):
            d, q = separation(xi, merged, bias_ref, t, block)
            weight = (gi + merged_g[block, 0:1, :]) * (q * q)
            return [weight * d[f] for f in range(3)]

        return terms

    own = [(places, f) for f in range(3)] + [(columns, 0)]
    pair_sums(table_ref, own, sums, 3, 4, body)

    def finish(t):
        live = state[t][6:7] > 0.5
        s = row_sums(sums, t, 3)
        part = partials[t // 2][t % 2]
        old = carried[t]
        new_pos, new_vel = [], []
        for f in range(3):
            extra = part[f : f + 1] + (6.0 * particle_mass) * s[f]
            gx = old[f : f + 1] + jnp.where(live, extra, 0.0)
            gv = old[3 + f : 4 + f] + jnp.where(live, part[3 + f : 4 + f], 0.0)
            new_pos.append(gx)
            new_vel.append(gv + time_step * gx)
        lam_out[t] = stack_rows([jnp.where(live, time_step * v, 0.0) for v in new_vel], LAM_ROWS)
        carried_out[t] = stack_rows(new_pos + new_vel)

    each_tile(finish, unroll=True)


def tiles_of(rows, tiles=4):
    return jax.ShapeDtypeStruct((tiles, rows, 2 * LANES), jnp.float32)


TILES = tiles_of(FEATS)
MERGED = jax.ShapeDtypeStruct((BLOCKS + PAD, FEATS, LANES), jnp.float32)
TABLE = jax.ShapeDtypeStruct((1, LANES), jnp.int32)
TABLE_COPY = [pltpu.SMEM(TABLE.shape, jnp.int32), pltpu.SemaphoreType.DMA]


def wide(count, tiles=4):
    return jax.ShapeDtypeStruct((count, tiles, 2 * LANES, LANES), jnp.float32)


def vmem_like(shape):
    return pltpu.VMEM(shape.shape, shape.dtype)


def packed_region(pack):
    return pltpu.VMEM((-(-BLOCKS // pack), FEATS, LANES), jnp.float32)


def run_kernel(kernel, name, scalars, arrays, out_shape, scratch, cycles, scalar_outputs=0, anywhere=False):
    smem = pl.BlockSpec(memory_space=pltpu.SMEM)
    vmem = pl.BlockSpec(memory_space=pltpu.VMEM)
    result = pl.pallas_call(
        kernel,
        name=name,
        out_shape=out_shape,
        in_specs=[smem] * len(scalars)
        + [pl.BlockSpec(memory_space=pltpu.HBM) if anywhere else vmem] * len(arrays),
        out_specs=[smem] * scalar_outputs + [vmem] * (len(out_shape) - scalar_outputs),
        scratch_shapes=scratch,
        compiler_params=pltpu.CompilerParams(
            vmem_limit_bytes=(60 << 20) if anywhere else VMEM_LIMIT
        ),
        cost_estimate=pl.CostEstimate(
            flops=cycles * 65536, bytes_accessed=1 << 18, transcendentals=0
        ),
    )(*scalars, *arrays)
    return result


def per_device(exchange, positions, velocities, occupancy, cot_positions, cot_velocities):
    slots = positions.shape[3]
    assert positions.shape[1:] == (2, 2, 2 * LANES)
    parts = run_kernel(
        functools.partial(pack_kernel, exchange),
        "pack",
        (occupancy,),
        (positions, velocities, cot_positions, cot_velocities),
        [tiles_of(2 * FEATS, 2)] * 2,
        [pltpu.VMEM(positions.shape, jnp.float32)] * 4 + [pltpu.SemaphoreType.DMA((4,))],
        500,
        anywhere=True,
    )
    parts = exchange.place(parts)
    state, carried, lam, rank = run_kernel(
        functools.partial(prepare_kernel, exchange),
        "prepare",
        (),
        tuple(parts),
        [TILES, TILES, tiles_of(LAM_ROWS), jax.ShapeDtypeStruct((4, 1, slots), jnp.int32)],
        [],
        1000,
    )

    pieces = exchange.halo(state)
    own, x_low, x_high, far = [piece[:, 2:7:4] for piece in pieces]
    around = jnp.stack([x_low, own, x_high])
    around = jnp.concatenate([around, far[:, None]], axis=1)
    present = around[:, :, 1] > 0.5
    place_bits = (BLOCKS * LANES - 1).bit_length()
    deepest = (1 << (31 - place_bits)) - 1
    depth = jnp.clip(around[:, :, 0] * float((deepest + 1) // 16), 0.0, deepest - 1.0)
    depth = jnp.where(present, depth.astype(jnp.int32), deepest).reshape(-1)
    depth = jnp.minimum(depth, jnp.where(present.reshape(-1), deepest - 1, deepest))
    place = lax.broadcasted_iota(jnp.int32, depth.shape, 0)
    order = lax.sort((depth << place_bits) | place, is_stable=False) & ((1 << place_bits) - 1)
    counts, order, bias = run_kernel(
        functools.partial(plan_kernel, exchange),
        "plan",
        (),
        (order.reshape(BLOCKS, 1, LANES),) + pieces,
        [
            jax.ShapeDtypeStruct((8,), jnp.int32),
            jax.ShapeDtypeStruct((BLOCKS + PAD, 1, LANES), jnp.int32),
            jax.ShapeDtypeStruct((4, BLOCKS + PAD, 1, LANES), jnp.float32),
        ],
        [],
        500,
        scalar_outputs=1,
    )

    def spread(value, features, name):
        return run_kernel(
            functools.partial(spread_kernel, features), name, (), (value,), [wide(features)], [], 2000
        )[0]

    saved = []
    columns = spread(state, 6, "spread_state")
    for step in range(STEPS):
        if step > 0:
            pieces, columns = exchange.halo(state, beside=spread(state, 6, "spread_state"))
        own_press, merged, table = run_kernel(
            functools.partial(density_kernel, exchange),
            "density",
            (counts,),
            (order, bias, columns) + pieces,
            [tiles_of(PRESS_ROWS), MERGED, TABLE],
            [
                packed_region(1),
                vmem_like(wide(1)),
                pltpu.SMEM(TABLE.shape, jnp.int32),
            ],
            8000,
        )
        press, press_columns = exchange.halo(
            own_press, beside=spread(own_press, 2, "spread_press")
        )
        if step + 1 < STEPS:
            new_state, merged_p = run_kernel(
                accel_kernel,
                "accel",
                (),
                (table, order, bias, merged, columns, press_columns, state) + press,
                [TILES, MERGED],
                [packed_region(4), vmem_like(wide(3))] + TABLE_COPY,
                10000,
            )
        else:
            new_state = state
            (merged_p,) = run_kernel(
                functools.partial(merge_kernel, 4),
                "merge",
                (table,),
                (order,) + press,
                [MERGED],
                [packed_region(4)],
                2000,
            )
        saved.append((state, own_press, table, merged, merged_p, columns, press_columns))
        state = new_state

    for step in reversed(range(STEPS)):
        state, own_press, table, merged, merged_p, columns, press_columns = saved[step]
        lam_pieces, lam_columns = exchange.halo(lam, beside=spread(lam, 3, "spread_lam"))
        own_grad, merged_l = run_kernel(
            density_grad_kernel,
            "density_grad",
            (),
            (table, order, bias, merged, columns, lam_columns, state, own_press) + lam_pieces,
            [tiles_of(1), MERGED],
            [packed_region(2), vmem_like(wide(2))] + TABLE_COPY,
            10000,
        )
        halves = [
            run_kernel(
                functools.partial(main_grad_kernel, half),
                "main_grad_%d" % half,
                (table,),
                (bias, merged, merged_p, merged_l, columns, lam_columns, press_columns),
                [tiles_of(FEATS, 2)],
                [vmem_like(wide(6, 2))],
                10000,
            )[0]
            for half in range(2)
        ]
        grad_pieces, halves[0] = exchange.halo(own_grad, beside=halves[0])
        lam, carried = run_kernel(
            last_grad_kernel,
            "last_grad",
            (),
            (table, order, bias, merged, columns, state) + grad_pieces + tuple(halves) + (carried,),
            [tiles_of(LAM_ROWS), TILES],
            [packed_region(8), vmem_like(MERGED), vmem_like(wide(1)), vmem_like(wide(3))]
            + TABLE_COPY,
            8000,
        )

    parts = run_kernel(
        functools.partial(restore_kernel, exchange),
        "restore",
        (),
        (rank, carried),
        [tiles_of(FEATS, 2)] * 2,
        [],
        500,
    )
    parts = exchange.unplace(parts)
    swap = lax.axis_index("gy") % 2 == 1
    grads = jnp.stack([jnp.where(swap, parts[1], parts[0]), jnp.where(swap, parts[0], parts[1])])
    grads = jnp.moveaxis(grads, 2, 0)
    return (grads[:3], grads[3:6])


def solution(mesh):
    spec = P(None, "gx", "gy", None)
    exchange = Exchange(mesh)
    return jax.shard_map(
        functools.partial(per_device, exchange),
        mesh=mesh,
        in_specs=(spec, spec, P("gx", "gy"), spec, spec),
        out_specs=(spec, spec),
        check_vma=False,
    )
```
